32 devices in a mesh: batch: 4 (over x, core), seq: 8 (over z, y).
Axes of the slice: x: 2, y: 2, z: 4, core: 2. Of those that a mesh axis runs over, the one named last changes fastest.
Arguments:
- tokens: bfloat16 [16, 2048, 768], P('batch', 'seq'), may hold values from -6 to 6
- prompts: float32 [50, 768], replicated, may hold values from -6 to 6
- image_id: int32 [16, 2048], P('batch'), may hold values from 0 to 8, as said below
- prompt_slot: int32 [16, 2048], P('batch', 'seq'), may hold values from 0 to 50, as said below
- ln1_gain: float32 [768], replicated, may hold values from 0.5 to 1.5
- ln1_bias: float32 [768], replicated, may hold values from -1.8 to 1.8
- w_qkv: bfloat16 [768, 2304], replicated, may hold values from -0.21875 to 0.21875
- bias_qv: float32 [1536], replicated, may hold values from -1.8 to 1.8
- w_out: bfloat16 [768, 768], replicated, may hold values from -0.875 to 0.875
- bias_out: float32 [768], replicated, may hold values from -1.8 to 1.8
- ln2_gain: float32 [768], replicated, may hold values from 0.5 to 1.5
- ln2_bias: float32 [768], replicated, may hold values from -1.8 to 1.8
- w_up: bfloat16 [768, 3072], replicated, may hold values from -0.21875 to 0.21875
- bias_up: float32 [3072], replicated, may hold values from -1.8 to 1.8
- w_down: bfloat16 [3072, 768], replicated, may hold values from -0.109375 to 0.109375
- bias_down: float32 [768], replicated, may hold values from -1.8 to 1.8
- cotangent: bfloat16 [16, 2048, 768], P('batch', 'seq'), may hold values from -6 to 6
Outputs:
- output: bfloat16 [16, 2048, 768], P('batch', 'seq')
- token_gradient: bfloat16 [16, 2048, 768], P('batch', 'seq')
- prompt_gradient: float32 [50, 768], replicated
The draws below stay inside these ranges and needn't reach their ends.
Inputs may be any that keep to these rules, and one draw needn't show every extreme that they name: `image_id`: each row holds 8 runs of 247 consecutive positions with ids 0 to 7 in order; all other positions (padding, some before, between or after the runs) have id 8. `prompt_slot`: within each run of image_id, the first position is the class token, the next 50 carry slots 0 to 49 in order; class tokens, patches and padding carry 50.
All inputs are finite; a program needn't handle non-finite values.
Results may differ from the reference program's by a relative error of at most 0.012.
Values may be sent and summed in bfloat16 or wider, within the bound.
A program may use at most 384 MiB of HBM per device.

```python
import math
import jax
import jax.numpy as jnp
from jax import lax

MODEL_WIDTH = 768
ATTENTION_HEADS = 12
HEAD_FEATURES = 64
FF = 3072
PROMPTS = 50
IMAGES_PER_ROW = 8
ROW_LENGTH = 2048
IMAGE_TOKENS = 247
PACKED_ROWS = 16


def row_layout(key):
    padding_mask = ROW_LENGTH - IMAGES_PER_ROW * IMAGE_TOKENS
    cuts = jax.random.randint(jax.random.fold_in(key, 7), (PACKED_ROWS, IMAGES_PER_ROW), 0, padding_mask + 1)
    cuts = jnp.sort(cuts, axis=1)
    image_starts = jnp.arange(IMAGES_PER_ROW, dtype=jnp.int32)[None, :] * IMAGE_TOKENS + cuts
    image_offsets = jnp.arange(ROW_LENGTH, dtype=jnp.int32)[None, None, :] - image_starts[:, :, None]
    inside = ((image_offsets >= 0) & (image_offsets < IMAGE_TOKENS)).astype(jnp.int32)
    covered = jnp.sum(inside, axis=1)
    image = jnp.sum(inside * jnp.arange(IMAGES_PER_ROW, dtype=jnp.int32)[None, :, None], axis=1) + (1 - covered) * IMAGES_PER_ROW
    within = jnp.sum(inside * image_offsets, axis=1)
    is_prompt = (covered == 1) & (within >= 1) & (within <= PROMPTS)
    slots = jnp.where(is_prompt, within - 1, PROMPTS)
    return (image.astype(jnp.int32), slots.astype(jnp.int32))


def draw_image_id(key, part):
    return row_layout(key)[0]


def draw_prompt_slot(key, part):
    return row_layout(key)[1]


def shard_levels(rng, dims, shards, smallest, high):
    loudness = 1.0
    for position, shards_of in shards:
        heights = jax.random.uniform(jax.random.fold_in(jax.random.fold_in(rng, 6), position), (shards_of,), jnp.float32, smallest / len(shards), high / len(shards))
        loudness = loudness * jnp.repeat(jnp.exp(heights), dims[position] // shards_of).reshape((-1,) + (1,) * (len(dims) - 1 - position))
    return loudness


def scatter_about(rng, dims, deviation, bound, cuts=(), held_as=jnp.bfloat16):
    values = deviation * jax.random.normal(rng, dims, jnp.float32)
    if cuts:
        values = values * shard_levels(rng, dims, cuts, -0.22, 0.18)
    return jnp.clip(values, -bound, bound).astype(held_as)


def setup_inputs(seed: int = 0) -> dict:
    streams_of = jax.random.split(jax.random.key(seed), 18)
    return {
        "tokens": scatter_about(streams_of[0], (PACKED_ROWS, ROW_LENGTH, MODEL_WIDTH), 1.0, 6.0, ((0, 4), (1, 8))),
        "prompts": scatter_about(streams_of[1], (PROMPTS, MODEL_WIDTH), 1.0, 6.0, (), jnp.float32),
        "image_id": draw_image_id(jax.random.fold_in(streams_of[17], 71), 0),
        "prompt_slot": draw_prompt_slot(jax.random.fold_in(streams_of[17], 71), 0),
        "ln1_gain": jnp.clip(1.0 + 0.1 * jax.random.normal(streams_of[4], (MODEL_WIDTH,), jnp.float32), 0.5, 1.5),
        "ln1_bias": scatter_about(streams_of[5], (MODEL_WIDTH,), 0.3, 1.8, (), jnp.float32),
        "w_qkv": scatter_about(streams_of[6], (MODEL_WIDTH, 3 * MODEL_WIDTH), MODEL_WIDTH ** -0.5, 0.21875),
        "bias_qv": scatter_about(streams_of[7], (2 * MODEL_WIDTH,), 0.3, 1.8, (), jnp.float32),
        "w_out": scatter_about(streams_of[8], (MODEL_WIDTH, MODEL_WIDTH), (MODEL_WIDTH // 16) ** -0.5, 0.875),
        "bias_out": scatter_about(streams_of[9], (MODEL_WIDTH,), 0.3, 1.8, (), jnp.float32),
        "ln2_gain": jnp.clip(1.0 + 0.1 * jax.random.normal(streams_of[10], (MODEL_WIDTH,), jnp.float32), 0.5, 1.5),
        "ln2_bias": scatter_about(streams_of[11], (MODEL_WIDTH,), 0.3, 1.8, (), jnp.float32),
        "w_up": scatter_about(streams_of[12], (MODEL_WIDTH, FF), MODEL_WIDTH ** -0.5, 0.21875),
        "bias_up": scatter_about(streams_of[13], (FF,), 0.3, 1.8, (), jnp.float32),
        "w_down": scatter_about(streams_of[14], (FF, MODEL_WIDTH), FF ** -0.5, 0.109375),
        "bias_down": scatter_about(streams_of[15], (MODEL_WIDTH,), 0.3, 1.8, (), jnp.float32),
        "cotangent": scatter_about(streams_of[16], (PACKED_ROWS, ROW_LENGTH, MODEL_WIDTH), 1.0, 6.0, ((0, 4), (1, 8))),
    }


@jax.custom_vjp
def low(v):
    return lax.optimization_barrier(v.astype(jnp.bfloat16)).astype(jnp.float32)

@jax.custom_vjp
def low_back(v):
    return v

def low_keep(v):
    return (low(v), None)

def low_pass(kept, grad):
    return (grad,)

def back_keep(v):
    return (v, None)

def back_low(kept, grad):
    return (low(grad),)
low.defvjp(low_keep, low_pass)
low_back.defvjp(back_keep, back_low)
highest_precision = lax.Precision.HIGHEST

def layer_norm(value_rows, gain, shift_bias):
    mean = lax.optimization_barrier(jnp.mean(value_rows, axis=-1, keepdims=True))
    centered = value_rows - mean
    inverse = lax.rsqrt(lax.optimization_barrier(jnp.mean(centered * centered, axis=-1, keepdims=True)) + 1e-06)
    return centered * inverse * gain + shift_bias

def reference(tokens, prompts, image_id, prompt_slot, ln1_gain, ln1_bias, w_qkv, bias_qv, w_out, bias_out, ln2_gain, ln2_bias, w_up, bias_up, w_down, bias_down, cotangent):
    wqkv_f = w_qkv.astype(jnp.float32)
    wout_f = w_out.astype(jnp.float32)
    wup_f = w_up.astype(jnp.float32)
    wdown_f = w_down.astype(jnp.float32)
    bias_three = jnp.concatenate([bias_qv[:MODEL_WIDTH], jnp.zeros((MODEL_WIDTH,), jnp.float32), bias_qv[MODEL_WIDTH:]])
    scale = HEAD_FEATURES ** (-0.5)

    def layer(hidden_in, ids, slots, prompt_rows):
        token_count = hidden_in.shape[0]
        one_hot = (slots[..., None] == jnp.arange(PROMPTS, dtype=jnp.int32)).astype(jnp.float32)
        placed = jnp.einsum('gln,nd->gld', one_hot, prompt_rows, precision=highest_precision)
        inserted = jnp.where((slots < PROMPTS)[..., None], placed, hidden_in)
        normed1 = low(layer_norm(inserted, ln1_gain, ln1_bias))
        query_key_value = jnp.einsum('gld,de->gle', normed1, wqkv_f, precision=highest_precision) + bias_three
        query_key_value = low_back(low(query_key_value))
        query_rows = query_key_value[..., :MODEL_WIDTH].reshape(token_count, ROW_LENGTH, ATTENTION_HEADS, HEAD_FEATURES)
        key_rows = query_key_value[..., MODEL_WIDTH:2 * MODEL_WIDTH].reshape(token_count, ROW_LENGTH, ATTENTION_HEADS, HEAD_FEATURES)
        value_rows = query_key_value[..., 2 * MODEL_WIDTH:].reshape(token_count, ROW_LENGTH, ATTENTION_HEADS, HEAD_FEATURES)
        scores = low_back(jnp.einsum('gqhd,gkhd->ghqk', query_rows, key_rows, precision=highest_precision) * scale)
        same_image = (ids[:, :, None] == ids[:, None, :]) & (ids < IMAGES_PER_ROW)[:, :, None]
        permitted_mask = same_image | jnp.eye(ROW_LENGTH, dtype=bool)[None]
        scores = jnp.where(permitted_mask[:, None], scores, -1e+30)
        attention_weights = low(jax.nn.softmax(scores, axis=-1))
        attention_output = jnp.einsum('vbta,vabj->vtbj', attention_weights, value_rows, precision=highest_precision).reshape(token_count, ROW_LENGTH, MODEL_WIDTH)
        attention_output = low_back(low(attention_output))
        branch = low_back(jnp.einsum('gld,de->gle', attention_output, wout_f, precision=highest_precision) + bias_out)
        hidden1 = inserted + branch
        normed2 = low(layer_norm(hidden1, ln2_gain, ln2_bias))
        upper = low_back(jnp.einsum('gld,df->glf', normed2, wup_f, precision=highest_precision) + bias_up)
        activated = low(jax.nn.gelu(upper, approximate=False))
        feed = low_back(jnp.einsum('glf,fd->gld', activated, wdown_f, precision=highest_precision) + bias_down)
        return hidden1 + feed
    group = math.gcd(PACKED_ROWS, 2)
    blocks = PACKED_ROWS // group

    def split(array):
        return array.reshape((blocks, group) + array.shape[1:])

    def one_block(carry, block):
        tok_block, cot_block, id_block, slot_block = block
        valid = (id_block < IMAGES_PER_ROW).astype(jnp.float32)

        def forward(hidden_in, prompt_rows):
            return layer(hidden_in, id_block, slot_block, prompt_rows)
        result, pull = jax.vjp(jax.checkpoint(forward), tok_block.astype(jnp.float32), prompts)
        in_grad, prm_grad = pull(cot_block.astype(jnp.float32) * valid[..., None])
        return (carry + prm_grad, (result.astype(jnp.bfloat16), in_grad.astype(jnp.bfloat16)))
    start = jnp.zeros((PROMPTS, MODEL_WIDTH), jnp.float32)
    prompt_gradient, (output, token_gradient) = lax.scan(one_block, start, (split(tokens), split(cotangent), split(image_id), split(prompt_slot)))
    return (output.reshape(PACKED_ROWS, ROW_LENGTH, MODEL_WIDTH), token_gradient.reshape(PACKED_ROWS, ROW_LENGTH, MODEL_WIDTH), prompt_gradient)
```

```python
import functools

import jax
import jax.numpy as jnp
from jax import lax
from jax.experimental import pallas as pl
from jax.experimental.pallas import tpu as pltpu
from jax.sharding import PartitionSpec as P

ATTENTION_HEADS = 12
HEAD_FEATURES = 64
PROMPTS = 50
IMAGES_PER_ROW = 8
IMAGE_TOKENS = 247


def passed_along(block, axis, distance):
    devices = range(lax.axis_size(axis))
    route = [(i - distance, i) for i in devices if i - distance in devices]
    return lax.ppermute(block, axis, route)


def normalize(value_rows):
    mean = jnp.mean(value_rows, axis=-1, keepdims=True)
    centered = value_rows - mean
    inverse = lax.rsqrt(jnp.mean(centered * centered, axis=-1, keepdims=True) + 1e-06)
    return (centered * inverse, inverse)


def norm_back(grad_in, normal_draws, inverse, gain):
    scaled = grad_in * gain
    return inverse * (
        scaled
        - jnp.mean(scaled, axis=-1, keepdims=True)
        - normal_draws * jnp.mean(scaled * normal_draws, axis=-1, keepdims=True)
    )


def block_rows(rows, span):
    group = min(rows, max(1, 512 // span))
    while rows % group:
        group = group - 1
    return group


def masked_scores(query_rows, key_rows, query_ids, key_ids, own_pos, key_pos):
    scores = jnp.einsum(
        "gqhd,gkhd->ghqk", query_rows, key_rows, preferred_element_type=jnp.float32
    ) * HEAD_FEATURES ** (-0.5)
    same_image = (query_ids[:, :, None] == key_ids[:, None, :]) & (query_ids < IMAGES_PER_ROW)[
        :, :, None
    ]
    permitted_mask = same_image | (own_pos[:, None] == key_pos[None, :])[None]
    return jnp.where(permitted_mask[:, None], scores, -1e30)


def general_body(
    tokens,
    prompts,
    image_id,
    prompt_slot,
    ln1_gain,
    ln1_bias,
    w_qkv,
    bias_qv,
    w_out,
    bias_out,
    ln2_gain,
    ln2_bias,
    w_up,
    bias_up,
    w_down,
    bias_down,
    cotangent,
):
    rows, span, width = tokens.shape
    length = image_id.shape[1]
    start = lax.axis_index("seq") * span
    own_ids = lax.dynamic_slice_in_dim(image_id, start, span, 1)
    own_pos = start + jnp.arange(span, dtype=jnp.int32)
    valid = (own_ids < IMAGES_PER_ROW).astype(jnp.float32)
    one_hot = (prompt_slot[..., None] == jnp.arange(PROMPTS, dtype=jnp.int32)).astype(jnp.float32)
    placed = jnp.einsum("rsn,nd->rsd", one_hot, prompts, precision=lax.Precision.HIGHEST)
    is_prompt = (prompt_slot < PROMPTS)[..., None]
    inserted = jnp.where(is_prompt, placed, tokens.astype(jnp.float32))
    normal1, inverse1 = normalize(inserted)
    normed1 = (normal1 * ln1_gain + ln1_bias).astype(jnp.bfloat16)
    bias_three = jnp.concatenate(
        [bias_qv[:width], jnp.zeros((width,), jnp.float32), bias_qv[width:]]
    )
    query_key_value = (
        jnp.einsum("rsd,de->rse", normed1, w_qkv, preferred_element_type=jnp.float32) + bias_three
    ).astype(jnp.bfloat16)
    query_rows = query_key_value[..., :width]
    key_own = query_key_value[..., width : 2 * width]
    value_own = query_key_value[..., 2 * width :]
    reach = (IMAGE_TOKENS - 2 + span) // span
    offsets = list(range(-reach, reach + 1))
    key_parts = []
    value_parts = []
    for offset in offsets:
        if offset == 0:
            fetched_key, fetched_value = (key_own, value_own)
        else:
            fetched_key, fetched_value = passed_along((key_own, value_own), "seq", -offset)
        key_parts.append(fetched_key)
        value_parts.append(fetched_value)
    key_rows = jnp.concatenate(key_parts, axis=1)
    value_rows = jnp.concatenate(value_parts, axis=1)
    raw_pos = jnp.concatenate(
        [start + offset * span + jnp.arange(span, dtype=jnp.int32) for offset in offsets]
    )
    in_row = (raw_pos >= 0) & (raw_pos < length)
    taken = jnp.take(image_id, jnp.clip(raw_pos, 0, length - 1), axis=1)
    key_ids = jnp.where(in_row[None, :], taken, -1)
    key_pos = jnp.where(in_row, raw_pos, -1)
    key_count = key_rows.shape[1]
    group = block_rows(rows, span)

    def grouped(array):
        return array.reshape((rows // group, group) + array.shape[1:])

    query_heads = grouped(query_rows.reshape(rows, span, ATTENTION_HEADS, HEAD_FEATURES))
    key_heads = grouped(key_rows.reshape(rows, key_count, ATTENTION_HEADS, HEAD_FEATURES))
    value_heads = grouped(value_rows.reshape(rows, key_count, ATTENTION_HEADS, HEAD_FEATURES))
    query_ids = grouped(own_ids)
    grouped_key_ids = grouped(key_ids)

    def forward_block(inputs):
        query_blk, key_blk, value_blk, qid_blk, kid_blk = inputs
        scores = masked_scores(query_blk, key_blk, qid_blk, kid_blk, own_pos, key_pos)
        row_top = jnp.max(scores, axis=-1, keepdims=True)
        total = jnp.sum(jnp.exp(scores - row_top), axis=-1, keepdims=True)
        log_total = row_top + jnp.log(total)
        attention_weights = jnp.exp(scores - log_total).astype(jnp.bfloat16)
        attention_output = jnp.einsum(
            "vbta,vabj->vtbj", attention_weights, value_blk, preferred_element_type=jnp.float32
        )
        return (attention_output.astype(jnp.bfloat16), log_total[..., 0])

    attention_output, log_totals = lax.map(
        forward_block, (query_heads, key_heads, value_heads, query_ids, grouped_key_ids)
    )
    attention_output = attention_output.reshape(rows, span, width)
    hidden1 = (
        inserted
        + jnp.einsum("rsd,de->rse", attention_output, w_out, preferred_element_type=jnp.float32)
        + bias_out
    )
    normal2, inverse2 = normalize(hidden1)
    normed2 = (normal2 * ln2_gain + ln2_bias).astype(jnp.bfloat16)
    upper = jnp.einsum("rsd,df->rsf", normed2, w_up, preferred_element_type=jnp.float32) + bias_up
    activated, gelu_pull = jax.vjp(lambda inner: jax.nn.gelu(inner, approximate=False), upper)
    activated = activated.astype(jnp.bfloat16)
    output = (
        hidden1
        + jnp.einsum("rsf,fd->rsd", activated, w_down, preferred_element_type=jnp.float32)
        + bias_down
    ).astype(jnp.bfloat16)
    out_grad = cotangent.astype(jnp.float32) * valid[..., None]
    act_grad = jnp.einsum(
        "rsd,fd->rsf", out_grad.astype(jnp.bfloat16), w_down, preferred_element_type=jnp.float32
    )
    upper_grad = gelu_pull(act_grad)[0].astype(jnp.bfloat16)
    normed2_grad = jnp.einsum("rsf,df->rsd", upper_grad, w_up, preferred_element_type=jnp.float32)
    hidden1_grad = out_grad + norm_back(normed2_grad, normal2, inverse2, ln2_gain)
    attended_grad = jnp.einsum(
        "rse,de->rsd", hidden1_grad.astype(jnp.bfloat16), w_out, preferred_element_type=jnp.float32
    ).astype(jnp.bfloat16)
    attended_grad = grouped(attended_grad.reshape(rows, span, ATTENTION_HEADS, HEAD_FEATURES))

    def backward_block(inputs):
        query_blk, key_blk, value_blk, qid_blk, kid_blk, total_blk, grad_blk = inputs
        scores = masked_scores(query_blk, key_blk, qid_blk, kid_blk, own_pos, key_pos)
        attention_weights = jnp.exp(scores - total_blk[..., None])
        value_grad = jnp.einsum(
            "ghqk,gqhd->gkhd",
            attention_weights.astype(jnp.bfloat16),
            grad_blk,
            preferred_element_type=jnp.float32,
        )
        prob_grad = jnp.einsum(
            "gqhd,gkhd->ghqk", grad_blk, value_blk, preferred_element_type=jnp.float32
        )
        inner = jnp.sum(attention_weights * prob_grad, axis=-1, keepdims=True)
        score_grad = (attention_weights * (prob_grad - inner)).astype(jnp.bfloat16)
        query_grad = jnp.einsum(
            "vbta,vabj->vtbj", score_grad, key_blk, preferred_element_type=jnp.float32
        ) * HEAD_FEATURES ** (-0.5)
        key_grad = jnp.einsum(
            "ghqk,gqhd->gkhd", score_grad, query_blk, preferred_element_type=jnp.float32
        ) * HEAD_FEATURES ** (-0.5)
        return (query_grad, key_grad, value_grad)

    query_grad, key_grad, value_grad = lax.map(
        backward_block,
        (
            query_heads,
            key_heads,
            value_heads,
            query_ids,
            grouped_key_ids,
            log_totals,
            attended_grad,
        ),
    )
    query_grad = query_grad.reshape(rows, span, width)
    key_grad = key_grad.reshape(rows, key_count, width)
    value_grad = value_grad.reshape(rows, key_count, width)
    key_total = key_grad[:, reach * span : (reach + 1) * span]
    value_total = value_grad[:, reach * span : (reach + 1) * span]
    for offset in range(-reach, reach + 1):
        if offset != 0:
            first = (offset + reach) * span
            back_key, back_value = (
                passed_along(
                    key_grad[:, first : first + span].astype(jnp.bfloat16), "seq", offset
                ).astype(jnp.float32),
                passed_along(
                    value_grad[:, first : first + span].astype(jnp.bfloat16), "seq", offset
                ).astype(jnp.float32),
            )
            key_total = key_total + back_key
            value_total = value_total + back_value
    qkv_grad = jnp.concatenate([query_grad, key_total, value_total], axis=-1).astype(jnp.bfloat16)
    normed1_grad = jnp.einsum("rse,de->rsd", qkv_grad, w_qkv, preferred_element_type=jnp.float32)
    inserted_grad = hidden1_grad + norm_back(normed1_grad, normal1, inverse1, ln1_gain)
    token_gradient = jnp.where(is_prompt, 0.0, inserted_grad).astype(jnp.bfloat16)
    prompt_part = jnp.einsum("rsn,rsd->nd", one_hot, inserted_grad, precision=lax.Precision.HIGHEST)
    prompt_gradient = lax.psum(prompt_part, ("batch", "seq"))
    return (output, token_gradient, prompt_gradient)


HALO = 64
SLOTS = 320
KEYS = 256
PAIR = 2 * HEAD_FEATURES
SCALE = HEAD_FEATURES ** (-0.5)
ERFC_RATE = 0.39
ERFC_TERMS = (
    0.23532515356929604,
    0.09138882070894727,
    0.6495583974454544,
    -0.6353990518468564,
    0.8866636223583176,
    -0.22753694392981927,
)


def dot(a, b):
    return lax.dot_general(a, b, (((1,), (0,)), ((), ())), preferred_element_type=jnp.float32)


def dot_nt(a, b):
    return lax.dot_general(a, b, (((1,), (1,)), ((), ())), preferred_element_type=jnp.float32)


def dot_tn(a, b):
    return lax.dot_general(a, b, (((0,), (0,)), ((), ())), preferred_element_type=jnp.float32)


def gelu_parts(upper):
    size = jnp.abs(upper)
    t = 1.0 / (1.0 + (ERFC_RATE * 0.5**0.5) * size)
    tail = jnp.full_like(t, 0.5 * ERFC_TERMS[-1])
    for term in ERFC_TERMS[-2::-1]:
        tail = tail * t + 0.5 * term
    bell = jnp.exp(-0.5 * upper * upper)
    tail = tail * t * bell
    below = jnp.where(upper < 0, tail, 1.0 - tail)
    return upper * below, below + upper * (bell * 0.3989422804014327)


def slot_map(ids, index, span):
    lane = lax.broadcasted_iota(jnp.int32, ids.shape, 1)

    def first(image):
        return jnp.min(jnp.where(ids == image, lane, ids.shape[1] * 2), axis=1, keepdims=True)

    low = index * span
    start = first(index)
    end = start + IMAGE_TOKENS
    before = jnp.where(index == 0, low, jnp.maximum(first(index - 1) + IMAGE_TOKENS, low))
    after = jnp.where(
        index == IMAGES_PER_ROW - 1, low + span, jnp.minimum(first(index + 1), low + span)
    )
    spot = lax.broadcasted_iota(jnp.int32, (1, span + 2 * HALO), 1)
    place = low + jnp.where(
        spot < span, spot, jnp.where(spot < span + HALO, spot - span - HALO, spot - HALO)
    )
    lead = jnp.maximum(start - before, 0)
    slot = jnp.where((place >= end) & (place < after), IMAGE_TOKENS + lead + place - end, -1)
    slot = jnp.where((place >= before) & (place < start), IMAGE_TOKENS + place - before, slot)
    return jnp.where((place >= start) & (place < end), place - start, slot)


def row_kernel(
    ids, tok, tok_halo, cot, cot_halo, prom, g1, b1, w_qkv, b_qv, w_out, b_out, g2, b2, w_up, b_up, w_down, b_down,
    out, out_halo, tgr, tgr_halo, pgr,
    pick, ins, n1, inv1, wide, qkv, probs, turned, hid, n2, inv2, act, upg, og, grad,
):
    index = lax.axis_index("seq")
    span, width = tok.shape[1], tok.shape[2]
    ff = w_up.shape[1]
    bf = jnp.bfloat16
    slot = slot_map(ids[0], index, span)
    slots = lax.broadcasted_iota(jnp.int32, (SLOTS, span + 2 * HALO), 0)
    pick[...] = jnp.where(slots == slot, 1.0, 0.0).astype(bf)

    first_rows = lax.broadcasted_iota(jnp.int32, (64, 1), 0)
    is_prompt = (first_rows >= 1) & (first_rows <= PROMPTS)
    for r in range(0, SLOTS, 64):
        x = dot(pick[r : r + 64, :span], tok[0]) + dot(pick[r : r + 64, span:], tok_halo[0])
        if r == 0:
            x = jnp.where(is_prompt, prom[...], x)
        ins[r : r + 64] = x
        mean = jnp.mean(x, axis=-1, keepdims=True)
        c = x - mean
        inv = lax.rsqrt(jnp.mean(c * c, axis=-1, keepdims=True) + 1e-06)
        c = c * inv
        if r < KEYS:
            n1[r : r + 64] = c
            inv1[r : r + 64] = inv
        wide[r : r + 64] = (c * g1[...] + b1[...]).astype(bf)

    for c in range(0, width, 256):
        q = dot(wide[:KEYS], w_qkv[:, c : c + 256]) + b_qv[:, c : c + 256]
        qkv[:KEYS, c : c + 256] = (q * SCALE).astype(bf)
        k = dot(wide[:KEYS], w_qkv[:, width + c : width + c + 256])
        qkv[:KEYS, width + c : width + c + 256] = k.astype(bf)
        v = dot(wide[...], w_qkv[:, 2 * width + c : 2 * width + c + 256]) + b_qv[:, width + c : width + c + 256]
        qkv[:, 2 * width + c : 2 * width + c + 256] = v.astype(bf)

    lane = lax.broadcasted_iota(jnp.int32, (1, PAIR), 1)
    low_half = jnp.where(lane < HEAD_FEATURES, 1.0, 0.0).astype(bf)
    high_half = jnp.where(lane < HEAD_FEATURES, 0.0, 1.0).astype(bf)

    def both(x):
        return jnp.concatenate([x * low_half, x * high_half], axis=0)

    def own_halves(x):
        return x[:HEAD_FEATURES, :KEYS], x[HEAD_FEATURES:, KEYS:]

    tail_rows = lax.broadcasted_iota(jnp.int32, (16, 1), 0) + (KEYS - 16)
    for p in range(width // PAIR):
        at = p * PAIR
        qp = qkv[:KEYS, at : at + PAIR]
        kp = qkv[:KEYS, width + at : width + at + PAIR]
        vp = qkv[:KEYS, 2 * width + at : 2 * width + at + PAIR]
        st = dot_nt(kp, both(qp))
        upper, lower = st[: KEYS - 16], st[KEYS - 16 :]
        lower = jnp.where(tail_rows < IMAGE_TOKENS, lower, -1e30)
        top = jnp.maximum(jnp.max(upper, axis=0, keepdims=True), jnp.max(lower, axis=0, keepdims=True))
        upper = jnp.exp(upper - top)
        lower = jnp.exp(lower - top)
        total = jnp.sum(upper, axis=0, keepdims=True) + jnp.sum(lower, axis=0, keepdims=True)
        share = 1.0 / total
        probs[p, : KEYS - 16] = (upper * share).astype(bf)
        probs[p, KEYS - 16 :] = (lower * share).astype(bf)
        head0, head1 = own_halves(dot_tn(vp, probs[p]))
        turned[at : at + HEAD_FEATURES] = head0.astype(bf)
        turned[at + HEAD_FEATURES : at + PAIR] = head1.astype(bf)

    key_rows = lax.broadcasted_iota(jnp.int32, (KEYS, 1), 0)
    attended = turned[...].T
    wide[:KEYS] = jnp.where(key_rows < IMAGE_TOKENS, attended, qkv[:KEYS, 2 * width :])
    wide[KEYS:] = qkv[KEYS:, 2 * width :]
    for c in range(0, width, 256):
        hid[:, c : c + 256] = ins[:, c : c + 256] + dot(wide[...], w_out[:, c : c + 256]) + b_out[:, c : c + 256]

    for r in range(0, SLOTS, 64):
        x = hid[r : r + 64]
        mean = jnp.mean(x, axis=-1, keepdims=True)
        c = x - mean
        inv = lax.rsqrt(jnp.mean(c * c, axis=-1, keepdims=True) + 1e-06)
        c = c * inv
        if r < KEYS:
            n2[r : r + 64] = c
            inv2[r : r + 64] = inv
        wide[r : r + 64] = (c * g2[...] + b2[...]).astype(bf)
    for r in range(0, KEYS, 64):
        x = dot(pick[r : r + 64, :span], cot[0]) + dot(pick[r : r + 64, span:], cot_halo[0])
        if r + 64 == KEYS:
            x = jnp.where(first_rows < IMAGE_TOKENS - r, x, 0.0)
        og[r : r + 64] = x.astype(bf)

    for c in range(0, ff, 256):
        upper = dot(wide[...], w_up[:, c : c + 256]) + b_up[:, c : c + 256]
        act_grad = dot_nt(og[...], w_down[c : c + 256, :])
        value, slope = gelu_parts(upper)
        act[:, c : c + 256] = value.astype(bf)
        upg[:, c : c + 256] = (act_grad * slope[:KEYS]).astype(bf)
    for c in range(0, width, 256):
        y = hid[:, c : c + 256] + dot(act[...], w_down[:, c : c + 256]) + b_down[:, c : c + 256]
        wide[:, c : c + 256] = y.astype(bf)
        grad[:, c : c + 256] = dot_nt(upg[...], w_up[c : c + 256, :])
    out[0] = dot_tn(pick[:, :span], wide[...]).astype(bf)
    out_halo[0] = dot_tn(pick[:, span:], wide[...]).astype(bf)

    for r in range(0, KEYS, 64):
        e = grad[r : r + 64] * g2[...]
        n = n2[r : r + 64]
        mean = jnp.mean(e, axis=-1, keepdims=True)
        part = jnp.mean(e * n, axis=-1, keepdims=True)
        h = og[r : r + 64].astype(jnp.float32) + inv2[r : r + 64] * (e - mean - n * part)
        hid[r : r + 64] = h
        wide[r : r + 64] = h.astype(bf)
    for c in range(0, width, 256):
        og[:, c : c + 256] = dot_nt(wide[:KEYS], w_out[c : c + 256, :]).astype(bf)

    for p in range(width // PAIR):
        at = p * PAIR
        qp = qkv[:KEYS, at : at + PAIR]
        kp = qkv[:KEYS, width + at : width + at + PAIR]
        vp = qkv[:KEYS, 2 * width + at : 2 * width + at + PAIR]
        two_grads = both(og[:, at : at + PAIR])
        dp = dot_nt(vp, two_grads)
        pt = probs[p]
        pf = pt.astype(jnp.float32)
        inner = jnp.sum(pf * dp, axis=0, keepdims=True)
        ds = (pf * (dp - inner)).astype(bf)
        qkv[:KEYS, 2 * width + at : 2 * width + at + PAIR] = dot(pt, two_grads).astype(bf)
        head0, head1 = own_halves(dot_tn(kp, ds))
        qkv[:KEYS, width + at : width + at + PAIR] = dot(ds, both(qp)).astype(bf)
        turned[at : at + HEAD_FEATURES] = (head0 * SCALE).astype(bf)
        turned[at + HEAD_FEATURES : at + PAIR] = (head1 * SCALE).astype(bf)
    qkv[:KEYS, :width] = turned[...].T

    for c in range(0, width, 256):
        grad[:, c : c + 256] = dot_nt(qkv[:KEYS], w_qkv[c : c + 256, :])
    for r in range(0, KEYS, 64):
        e = grad[r : r + 64] * g1[...]
        n = n1[r : r + 64]
        mean = jnp.mean(e, axis=-1, keepdims=True)
        part = jnp.mean(e * n, axis=-1, keepdims=True)
        x = hid[r : r + 64] + inv1[r : r + 64] * (e - mean - n * part)
        if r == 0:
            @pl.when(pl.program_id(0) == 0)
            def _():
                pgr[...] = x

            @pl.when(pl.program_id(0) > 0)
            def _():
                pgr[...] += x
            x = jnp.where(is_prompt, 0.0, x)
        wide[r : r + 64] = x.astype(bf)
    tgr[0] = dot_tn(pick[:KEYS, :span], wide[:KEYS]).astype(bf)
    tgr_halo[0] = dot_tn(pick[:KEYS, span:], wide[:KEYS]).astype(bf)


def swapped(to_left, to_right):
    count = lax.axis_size("seq")
    from_right = lax.ppermute(to_left, "seq", [(i, i - 1) for i in range(1, count)])
    from_left = lax.ppermute(to_right, "seq", [(i, i + 1) for i in range(count - 1)])
    return from_left, from_right


def image_body(
    tokens, prompts, image_id, prompt_slot, ln1_gain, ln1_bias, w_qkv, bias_qv, w_out, bias_out,
    ln2_gain, ln2_bias, w_up, bias_up, w_down, bias_down, cotangent,
):
    rows, span, width = tokens.shape
    length = image_id.shape[1]
    ff = w_up.shape[1]
    f32, bf = jnp.float32, jnp.bfloat16

    def halo(x):
        return jnp.concatenate(swapped(x[:, :HALO], x[:, span - HALO :]), axis=1)

    prom = jnp.zeros((64, width), f32).at[1 : PROMPTS + 1].set(prompts)

    def per_row(*shape):
        return pl.BlockSpec((1,) + shape, lambda r: (r, 0, 0))

    def whole(*shape):
        return pl.BlockSpec(shape, lambda r: (0,) * len(shape), pipeline_mode=pl.Buffered(1))

    def line(x):
        return x.reshape(1, -1)

    out, out_halo, tgr, tgr_halo, pgr = pl.pallas_call(
        row_kernel,
        grid=(rows,),
        in_specs=[
            per_row(1, length), per_row(span, width), per_row(2 * HALO, width), per_row(span, width),
            per_row(2 * HALO, width), whole(64, width), whole(1, width), whole(1, width), whole(width, 3 * width),
            whole(1, 2 * width), whole(width, width), whole(1, width), whole(1, width), whole(1, width),
            whole(width, ff), whole(1, ff), whole(ff, width), whole(1, width),
        ],
        out_specs=[
            per_row(span, width), per_row(2 * HALO, width), per_row(span, width), per_row(2 * HALO, width),
            pl.BlockSpec((64, width), lambda r: (0, 0)),
        ],
        out_shape=[
            jax.ShapeDtypeStruct((rows, span, width), bf), jax.ShapeDtypeStruct((rows, 2 * HALO, width), bf),
            jax.ShapeDtypeStruct((rows, span, width), bf), jax.ShapeDtypeStruct((rows, 2 * HALO, width), bf),
            jax.ShapeDtypeStruct((64, width), f32),
        ],
        scratch_shapes=[
            pltpu.VMEM((SLOTS, span + 2 * HALO), bf), pltpu.VMEM((SLOTS, width), f32), pltpu.VMEM((KEYS, width), f32),
            pltpu.VMEM((KEYS, 1), f32), pltpu.VMEM((SLOTS, width), bf), pltpu.VMEM((SLOTS, 3 * width), bf),
            pltpu.VMEM((width // PAIR, KEYS, 2 * KEYS), bf), pltpu.VMEM((width, KEYS), bf),
            pltpu.VMEM((SLOTS, width), f32), pltpu.VMEM((KEYS, width), f32), pltpu.VMEM((KEYS, 1), f32),
            pltpu.VMEM((SLOTS, ff), bf), pltpu.VMEM((KEYS, ff), bf), pltpu.VMEM((KEYS, width), bf),
            pltpu.VMEM((KEYS, width), f32),
        ],
        compiler_params=pltpu.CompilerParams(vmem_limit_bytes=60 << 20, dimension_semantics=("arbitrary",)),
        name="layer_rows",
    )(
        image_id[:, None], tokens, halo(tokens), cotangent, halo(cotangent), prom, line(ln1_gain), line(ln1_bias),
        w_qkv, line(bias_qv), w_out, line(bias_out), line(ln2_gain), line(ln2_bias), w_up, line(bias_up), w_down,
        line(bias_down),
    )

    def home(own, sides):
        from_left, from_right = swapped(sides[:, :HALO], sides[:, HALO:])
        return own + jnp.concatenate(
            [from_left, jnp.zeros((rows, span - 2 * HALO, width), bf), from_right], axis=1
        )

    prompt_gradient = lax.psum(pgr[1 : PROMPTS + 1], ("batch", "seq"))
    return home(out, out_halo), home(tgr, tgr_halo), prompt_gradient


def body(tokens, prompts, image_id, *rest):
    if lax.axis_size("seq") == IMAGES_PER_ROW and tokens.shape[1] == KEYS:
        return image_body(tokens, prompts, image_id, *rest)
    return general_body(tokens, prompts, image_id, *rest)


def solution(mesh):
    in_specs = (
        P("batch", "seq", None),
        P(),
        P("batch", None),
        P("batch", "seq"),
        P(),
        P(),
        P(),
        P(),
        P(),
        P(),
        P(),
        P(),
        P(),
        P(),
        P(),
        P(),
        P("batch", "seq", None),
    )
    out_specs = (P("batch", "seq", None), P("batch", "seq", None), P())
    return jax.shard_map(body, mesh=mesh, in_specs=in_specs, out_specs=out_specs, check_vma=False)
```

```python
import functools

import jax
import jax.numpy as jnp
from jax import lax
from jax.experimental import pallas as pl
from jax.experimental.pallas import tpu as pltpu
from jax.sharding import PartitionSpec as P

ATTENTION_HEADS = 12
HEAD_FEATURES = 64
PROMPTS = 50
IMAGES_PER_ROW = 8
IMAGE_TOKENS = 247


def passed_along(block, axis, distance):
    devices = range(lax.axis_size(axis))
    route = [(i - distance, i) for i in devices if i - distance in devices]
    return lax.ppermute(block, axis, route)


def normalize(value_rows):
    mean = jnp.mean(value_rows, axis=-1, keepdims=True)
    centered = value_rows - mean
    inverse = lax.rsqrt(jnp.mean(centered * centered, axis=-1, keepdims=True) + 1e-06)
    return (centered * inverse, inverse)


def norm_back(grad_in, normal_draws, inverse, gain):
    scaled = grad_in * gain
    return inverse * (
        scaled
        - jnp.mean(scaled, axis=-1, keepdims=True)
        - normal_draws * jnp.mean(scaled * normal_draws, axis=-1, keepdims=True)
    )


def block_rows(rows, span):
    group = min(rows, max(1, 512 // span))
    while rows % group:
        group = group - 1
    return group


def masked_scores(query_rows, key_rows, query_ids, key_ids, own_pos, key_pos):
    scores = jnp.einsum(
        "gqhd,gkhd->ghqk", query_rows, key_rows, preferred_element_type=jnp.float32
    ) * HEAD_FEATURES ** (-0.5)
    same_image = (query_ids[:, :, None] == key_ids[:, None, :]) & (query_ids < IMAGES_PER_ROW)[
        :, :, None
    ]
    permitted_mask = same_image | (own_pos[:, None] == key_pos[None, :])[None]
    return jnp.where(permitted_mask[:, None], scores, -1e30)


def general_body(
    tokens,
    prompts,
    image_id,
    prompt_slot,
    ln1_gain,
    ln1_bias,
    w_qkv,
    bias_qv,
    w_out,
    bias_out,
    ln2_gain,
    ln2_bias,
    w_up,
    bias_up,
    w_down,
    bias_down,
    cotangent,
):
    rows, span, width = tokens.shape
    length = image_id.shape[1]
    start = lax.axis_index("seq") * span
    own_ids = lax.dynamic_slice_in_dim(image_id, start, span, 1)
    own_pos = start + jnp.arange(span, dtype=jnp.int32)
    valid = (own_ids < IMAGES_PER_ROW).astype(jnp.float32)
    one_hot = (prompt_slot[..., None] == jnp.arange(PROMPTS, dtype=jnp.int32)).astype(jnp.float32)
    placed = jnp.einsum("rsn,nd->rsd", one_hot, prompts, precision=lax.Precision.HIGHEST)
    is_prompt = (prompt_slot < PROMPTS)[..., None]
    inserted = jnp.where(is_prompt, placed, tokens.astype(jnp.float32))
    normal1, inverse1 = normalize(inserted)
    normed1 = (normal1 * ln1_gain + ln1_bias).astype(jnp.bfloat16)
    bias_three = jnp.concatenate(
        [bias_qv[:width], jnp.zeros((width,), jnp.float32), bias_qv[width:]]
    )
    query_key_value = (
        jnp.einsum("rsd,de->rse", normed1, w_qkv, preferred_element_type=jnp.float32) + bias_three
    ).astype(jnp.bfloat16)
    query_rows = query_key_value[..., :width]
    key_own = query_key_value[..., width : 2 * width]
    value_own = query_key_value[..., 2 * width :]
    reach = (IMAGE_TOKENS - 2 + span) // span
    offsets = list(range(-reach, reach + 1))
    key_parts = []
    value_parts = []
    for offset in offsets:
        if offset == 0:
            fetched_key, fetched_value = (key_own, value_own)
        else:
            fetched_key, fetched_value = passed_along((key_own, value_own), "seq", -offset)
        key_parts.append(fetched_key)
        value_parts.append(fetched_value)
    key_rows = jnp.concatenate(key_parts, axis=1)
    value_rows = jnp.concatenate(value_parts, axis=1)
    raw_pos = jnp.concatenate(
        [start + offset * span + jnp.arange(span, dtype=jnp.int32) for offset in offsets]
    )
    in_row = (raw_pos >= 0) & (raw_pos < length)
    taken = jnp.take(image_id, jnp.clip(raw_pos, 0, length - 1), axis=1)
    key_ids = jnp.where(in_row[None, :], taken, -1)
    key_pos = jnp.where(in_row, raw_pos, -1)
    key_count = key_rows.shape[1]
    group = block_rows(rows, span)

    def grouped(array):
        return array.reshape((rows // group, group) + array.shape[1:])

    query_heads = grouped(query_rows.reshape(rows, span, ATTENTION_HEADS, HEAD_FEATURES))
    key_heads = grouped(key_rows.reshape(rows, key_count, ATTENTION_HEADS, HEAD_FEATURES))
    value_heads = grouped(value_rows.reshape(rows, key_count, ATTENTION_HEADS, HEAD_FEATURES))
    query_ids = grouped(own_ids)
    grouped_key_ids = grouped(key_ids)

    def forward_block(inputs):
        query_blk, key_blk, value_blk, qid_blk, kid_blk = inputs
        scores = masked_scores(query_blk, key_blk, qid_blk, kid_blk, own_pos, key_pos)
        row_top = jnp.max(scores, axis=-1, keepdims=True)
        total = jnp.sum(jnp.exp(scores - row_top), axis=-1, keepdims=True)
        log_total = row_top + jnp.log(total)
        attention_weights = jnp.exp(scores - log_total).astype(jnp.bfloat16)
        attention_output = jnp.einsum(
            "vbta,vabj->vtbj", attention_weights, value_blk, preferred_element_type=jnp.float32
        )
        return (attention_output.astype(jnp.bfloat16), log_total[..., 0])

    attention_output, log_totals = lax.map(
        forward_block, (query_heads, key_heads, value_heads, query_ids, grouped_key_ids)
    )
    attention_output = attention_output.reshape(rows, span, width)
    hidden1 = (
        inserted
        + jnp.einsum("rsd,de->rse", attention_output, w_out, preferred_element_type=jnp.float32)
        + bias_out
    )
    normal2, inverse2 = normalize(hidden1)
    normed2 = (normal2 * ln2_gain + ln2_bias).astype(jnp.bfloat16)
    upper = jnp.einsum("rsd,df->rsf", normed2, w_up, preferred_element_type=jnp.float32) + bias_up
    activated, gelu_pull = jax.vjp(lambda inner: jax.nn.gelu(inner, approximate=False), upper)
    activated = activated.astype(jnp.bfloat16)
    output = (
        hidden1
        + jnp.einsum("rsf,fd->rsd", activated, w_down, preferred_element_type=jnp.float32)
        + bias_down
    ).astype(jnp.bfloat16)
    out_grad = cotangent.astype(jnp.float32) * valid[..., None]
    act_grad = jnp.einsum(
        "rsd,fd->rsf", out_grad.astype(jnp.bfloat16), w_down, preferred_element_type=jnp.float32
    )
    upper_grad = gelu_pull(act_grad)[0].astype(jnp.bfloat16)
    normed2_grad = jnp.einsum("rsf,df->rsd", upper_grad, w_up, preferred_element_type=jnp.float32)
    hidden1_grad = out_grad + norm_back(normed2_grad, normal2, inverse2, ln2_gain)
    attended_grad = jnp.einsum(
        "rse,de->rsd", hidden1_grad.astype(jnp.bfloat16), w_out, preferred_element_type=jnp.float32
    ).astype(jnp.bfloat16)
    attended_grad = grouped(attended_grad.reshape(rows, span, ATTENTION_HEADS, HEAD_FEATURES))

    def backward_block(inputs):
        query_blk, key_blk, value_blk, qid_blk, kid_blk, total_blk, grad_blk = inputs
        scores = masked_scores(query_blk, key_blk, qid_blk, kid_blk, own_pos, key_pos)
        attention_weights = jnp.exp(scores - total_blk[..., None])
        value_grad = jnp.einsum(
            "ghqk,gqhd->gkhd",
            attention_weights.astype(jnp.bfloat16),
            grad_blk,
            preferred_element_type=jnp.float32,
        )
        prob_grad = jnp.einsum(
            "gqhd,gkhd->ghqk", grad_blk, value_blk, preferred_element_type=jnp.float32
        )
        inner = jnp.sum(attention_weights * prob_grad, axis=-1, keepdims=True)
        score_grad = (attention_weights * (prob_grad - inner)).astype(jnp.bfloat16)
        query_grad = jnp.einsum(
            "vbta,vabj->vtbj", score_grad, key_blk, preferred_element_type=jnp.float32
        ) * HEAD_FEATURES ** (-0.5)
        key_grad = jnp.einsum(
            "ghqk,gqhd->gkhd", score_grad, query_blk, preferred_element_type=jnp.float32
        ) * HEAD_FEATURES ** (-0.5)
        return (query_grad, key_grad, value_grad)

    query_grad, key_grad, value_grad = lax.map(
        backward_block,
        (
            query_heads,
            key_heads,
            value_heads,
            query_ids,
            grouped_key_ids,
            log_totals,
            attended_grad,
        ),
    )
    query_grad = query_grad.reshape(rows, span, width)
    key_grad = key_grad.reshape(rows, key_count, width)
    value_grad = value_grad.reshape(rows, key_count, width)
    key_total = key_grad[:, reach * span : (reach + 1) * span]
    value_total = value_grad[:, reach * span : (reach + 1) * span]
    for offset in range(-reach, reach + 1):
        if offset != 0:
            first = (offset + reach) * span
            back_key, back_value = (
                passed_along(
                    key_grad[:, first : first + span].astype(jnp.bfloat16), "seq", offset
                ).astype(jnp.float32),
                passed_along(
                    value_grad[:, first : first + span].astype(jnp.bfloat16), "seq", offset
                ).astype(jnp.float32),
            )
            key_total = key_total + back_key
            value_total = value_total + back_value
    qkv_grad = jnp.concatenate([query_grad, key_total, value_total], axis=-1).astype(jnp.bfloat16)
    normed1_grad = jnp.einsum("rse,de->rsd", qkv_grad, w_qkv, preferred_element_type=jnp.float32)
    inserted_grad = hidden1_grad + norm_back(normed1_grad, normal1, inverse1, ln1_gain)
    token_gradient = jnp.where(is_prompt, 0.0, inserted_grad).astype(jnp.bfloat16)
    prompt_part = jnp.einsum("rsn,rsd->nd", one_hot, inserted_grad, precision=lax.Precision.HIGHEST)
    prompt_gradient = lax.psum(prompt_part, ("batch", "seq"))
    return (output, token_gradient, prompt_gradient)


MESH = pl.DeviceIdType.MESH
HALO = 64
SLOTS = 320
KEYS = 256
PAIR = 2 * HEAD_FEATURES
SCALE = HEAD_FEATURES ** (-0.5)
ERFC_RATE = 0.39
ERFC_TERMS = (
    0.23532515356929604,
    0.09138882070894727,
    0.6495583974454544,
    -0.6353990518468564,
    0.8866636223583176,
    -0.22753694392981927,
)


def dot(a, b):
    return lax.dot_general(a, b, (((1,), (0,)), ((), ())), preferred_element_type=jnp.float32)


def dot_nt(a, b):
    return lax.dot_general(a, b, (((1,), (1,)), ((), ())), preferred_element_type=jnp.float32)


def dot_tn(a, b):
    return lax.dot_general(a, b, (((0,), (0,)), ((), ())), preferred_element_type=jnp.float32)


def gelu_parts(upper):
    size = jnp.abs(upper)
    t = 1.0 / (1.0 + (ERFC_RATE * 0.5**0.5) * size)
    tail = jnp.full_like(t, 0.5 * ERFC_TERMS[-1])
    for term in ERFC_TERMS[-2::-1]:
        tail = tail * t + 0.5 * term
    bell = jnp.exp(-0.5 * upper * upper)
    tail = tail * t * bell
    below = jnp.where(upper < 0, tail, 1.0 - tail)
    return upper * below, below + upper * (bell * 0.3989422804014327)


def slot_map(ids, index, span):
    lane = lax.broadcasted_iota(jnp.int32, ids.shape, 1)

    def first(image):
        return jnp.min(jnp.where(ids == image, lane, ids.shape[1] * 2), axis=1, keepdims=True)

    low = index * span
    start = first(index)
    end = start + IMAGE_TOKENS
    before = jnp.where(index == 0, low, jnp.maximum(first(index - 1) + IMAGE_TOKENS, low))
    after = jnp.where(
        index == IMAGES_PER_ROW - 1, low + span, jnp.minimum(first(index + 1), low + span)
    )
    spot = lax.broadcasted_iota(jnp.int32, (1, span + 2 * HALO), 1)
    place = low + jnp.where(
        spot < span, spot, jnp.where(spot < span + HALO, spot - span - HALO, spot - HALO)
    )
    lead = jnp.maximum(start - before, 0)
    slot = jnp.where((place >= end) & (place < after), IMAGE_TOKENS + lead + place - end, -1)
    slot = jnp.where((place >= before) & (place < start), IMAGE_TOKENS + place - before, slot)
    return jnp.where((place >= start) & (place < end), place - start, slot)


def needed(tokens):
    return (tokens + 15) // 16 * 16


def sized(count, act):
    for size in range(16, HALO + 1, 16):
        pl.when(count == size)(functools.partial(act, size))


def row_kernel(
    ids, tok, cot, tok_all, cot_all, prompts, g1, b1, w_qkv_hbm, b_qv, w_out_hbm, b_out, g2, b2, w_up_hbm, b_up,
    w_down_hbm, b_down,
    out, tgr, pgr,
    w_qkv, w_out, w_up, w_down, w_sem,
    prom, pick, ins, n1, inv1, wide, qkv, probs, turned, hid, n2, inv2, act, upg, og, grad,
    halos, halo_send, halo_recv, sides, backs, side_send, side_recv,
    part, part_in, part_send, part_recv,
):
    index = lax.axis_index("seq")
    group = lax.axis_index("batch")
    row = pl.program_id(0)
    rows = tok_all.shape[0]
    span, width = tok.shape[1], tok.shape[2]
    ff = w_up.shape[1]
    bf = jnp.bfloat16
    last = IMAGES_PER_ROW - 1
    slack = span - IMAGE_TOKENS
    has_left, has_right = index > 0, index < last
    from_left = jnp.where(has_left, needed(slack * index), 0)
    from_right = jnp.where(has_right, needed(slack * (last - index)), 0)
    to_right = jnp.where(has_right, needed(slack * (index + 1)), 0)
    to_left = jnp.where(has_left, needed(slack * (IMAGES_PER_ROW - index)), 0)

    def weight(k):
        source = (w_qkv_hbm, w_out_hbm, w_up_hbm, w_down_hbm)[k]
        return pltpu.make_async_copy(source, (w_qkv, w_out, w_up, w_down)[k], w_sem.at[k])

    def arrived(k):
        pl.when(row == 0)(lambda: weight(k).wait())

    def seq_copy(source, target, send, recv, to):
        return pltpu.make_async_remote_copy(
            source, target, send, recv, device_id={"seq": to}, device_id_type=MESH
        )

    def halo_right(kind, r, size):
        source = (tok_all, cot_all)[kind].at[r, span - size :]
        target = halos.at[kind, r, HALO - size : HALO]
        return seq_copy(source, target, halo_send.at[kind, r, 0], halo_recv.at[kind, r, 0], index + 1)

    def halo_left(kind, r, size):
        source = (tok_all, cot_all)[kind].at[r, :size]
        target = halos.at[kind, r, HALO : HALO + size]
        return seq_copy(source, target, halo_send.at[kind, r, 1], halo_recv.at[kind, r, 1], index - 1)

    def halo_wait(kind, r):
        sized(from_left, lambda size: halo_right(kind, r, size).wait_recv())
        sized(from_right, lambda size: halo_left(kind, r, size).wait_recv())

    def side_left(kind, r, size):
        source = sides.at[kind, r, HALO - size : HALO]
        target = backs.at[kind, r, 2 * HALO - size :]
        return seq_copy(source, target, side_send.at[kind, r, 0], side_recv.at[kind, r, 0], index - 1)

    def side_right(kind, r, size):
        source = sides.at[kind, r, HALO : HALO + size]
        target = backs.at[kind, r, :size]
        return seq_copy(source, target, side_send.at[kind, r, 1], side_recv.at[kind, r, 1], index + 1)

    def side_start(kind, r):
        sized(from_left, lambda size: side_left(kind, r, size).start())
        sized(from_right, lambda size: side_right(kind, r, size).start())

    def side_merge(kind, r):
        sized(to_right, lambda size: side_left(kind, r, size).wait_recv())
        sized(to_left, lambda size: side_right(kind, r, size).wait_recv())
        result = (out, tgr)[kind]
        result[r, :HALO] = result[r, :HALO] + backs[kind, r, :HALO]
        result[r, span - HALO :] = result[r, span - HALO :] + backs[kind, r, HALO:]

    def flipped(place, step):
        return place + step - 2 * step * (place // step % 2)

    partners = tuple({"batch": flipped(group, k)} for k in (1, 2)) + tuple({"seq": flipped(index, k)} for k in (1, 2, 4))

    @pl.when(row == 0)
    def _():
        for k in range(4):
            weight(k).start()
        halos[...] = jnp.zeros_like(halos)
        backs[...] = jnp.zeros_like(backs)
        barrier = pltpu.get_barrier_semaphore()
        for device in partners:
            pl.semaphore_signal(barrier, inc=1, device_id=device, device_id_type=MESH)
        @pl.when(has_left)
        def _():
            pl.semaphore_signal(barrier, inc=1, device_id={"seq": index - 1}, device_id_type=MESH)
        @pl.when(has_right)
        def _():
            pl.semaphore_signal(barrier, inc=1, device_id={"seq": index + 1}, device_id_type=MESH)
        prom[...] = jnp.zeros_like(prom)
        prom[1 : PROMPTS + 1] = prompts[...]
        part[...] = jnp.zeros_like(part)
        pl.semaphore_wait(barrier, len(partners) + jnp.where(has_left, 1, 0) + jnp.where(has_right, 1, 0))
        for r in range(rows):
            for kind in range(2):
                sized(to_right, lambda size: halo_right(kind, r, size).start())
                sized(to_left, lambda size: halo_left(kind, r, size).start())

    slot = slot_map(ids[pl.ds(row, 1)], index, span)
    slots = lax.broadcasted_iota(jnp.int32, (SLOTS, span + 2 * HALO), 0)
    pick[...] = jnp.where(slots == slot, 1.0, 0.0).astype(bf)

    first_rows = lax.broadcasted_iota(jnp.int32, (64, 1), 0)
    is_prompt = (first_rows >= 1) & (first_rows <= PROMPTS)
    halo_wait(0, row)
    for r in range(0, SLOTS, 64):
        x = dot(pick[r : r + 64, :span], tok[0]) + dot(pick[r : r + 64, span:], halos[0, row])
        if r == 0:
            x = jnp.where(is_prompt, prom[...], x)
        ins[r : r + 64] = x
        mean = jnp.mean(x, axis=-1, keepdims=True)
        c = x - mean
        inv = lax.rsqrt(jnp.mean(c * c, axis=-1, keepdims=True) + 1e-06)
        c = c * inv
        if r < KEYS:
            n1[r : r + 64] = c
            inv1[r : r + 64] = inv
        wide[r : r + 64] = (c * g1[...][None] + b1[...][None]).astype(bf)

    arrived(0)
    for c in range(0, width, 256):
        q = dot(wide[:KEYS], w_qkv[:, c : c + 256]) + b_qv[c : c + 256][None]
        qkv[:KEYS, c : c + 256] = (q * SCALE).astype(bf)
        k = dot(wide[:KEYS], w_qkv[:, width + c : width + c + 256])
        qkv[:KEYS, width + c : width + c + 256] = k.astype(bf)
        v = dot(wide[...], w_qkv[:, 2 * width + c : 2 * width + c + 256]) + b_qv[width + c : width + c + 256][None]
        qkv[:, 2 * width + c : 2 * width + c + 256] = v.astype(bf)

    lane = lax.broadcasted_iota(jnp.int32, (1, PAIR), 1)
    low_half = jnp.where(lane < HEAD_FEATURES, 1.0, 0.0).astype(bf)
    high_half = jnp.where(lane < HEAD_FEATURES, 0.0, 1.0).astype(bf)

    def both(x):
        return jnp.concatenate([x * low_half, x * high_half], axis=0)

    def own_halves(x):
        return x[:HEAD_FEATURES, :KEYS], x[HEAD_FEATURES:, KEYS:]

    tail_rows = lax.broadcasted_iota(jnp.int32, (16, 1), 0) + (KEYS - 16)
    for p in range(width // PAIR):
        at = p * PAIR
        qp = qkv[:KEYS, at : at + PAIR]
        kp = qkv[:KEYS, width + at : width + at + PAIR]
        vp = qkv[:KEYS, 2 * width + at : 2 * width + at + PAIR]
        st = dot_nt(kp, both(qp))
        upper, lower = st[: KEYS - 16], st[KEYS - 16 :]
        lower = jnp.where(tail_rows < IMAGE_TOKENS, lower, -1e30)
        top = jnp.maximum(jnp.max(upper, axis=0, keepdims=True), jnp.max(lower, axis=0, keepdims=True))
        upper = jnp.exp(upper - top)
        lower = jnp.exp(lower - top)
        total = jnp.sum(upper, axis=0, keepdims=True) + jnp.sum(lower, axis=0, keepdims=True)
        share = 1.0 / total
        probs[p, : KEYS - 16] = (upper * share).astype(bf)
        probs[p, KEYS - 16 :] = (lower * share).astype(bf)
        head0, head1 = own_halves(dot_tn(vp, probs[p]))
        turned[at : at + HEAD_FEATURES] = head0.astype(bf)
        turned[at + HEAD_FEATURES : at + PAIR] = head1.astype(bf)

    key_rows = lax.broadcasted_iota(jnp.int32, (KEYS, 1), 0)
    attended = turned[...].T
    wide[:KEYS] = jnp.where(key_rows < IMAGE_TOKENS, attended, qkv[:KEYS, 2 * width :])
    wide[KEYS:] = qkv[KEYS:, 2 * width :]
    arrived(1)
    for c in range(0, width, 256):
        hid[:, c : c + 256] = ins[:, c : c + 256] + dot(wide[...], w_out[:, c : c + 256]) + b_out[c : c + 256][None]

    for r in range(0, SLOTS, 64):
        x = hid[r : r + 64]
        mean = jnp.mean(x, axis=-1, keepdims=True)
        c = x - mean
        inv = lax.rsqrt(jnp.mean(c * c, axis=-1, keepdims=True) + 1e-06)
        c = c * inv
        if r < KEYS:
            n2[r : r + 64] = c
            inv2[r : r + 64] = inv
        wide[r : r + 64] = (c * g2[...][None] + b2[...][None]).astype(bf)
    halo_wait(1, row)
    for r in range(0, KEYS, 64):
        x = dot(pick[r : r + 64, :span], cot[0]) + dot(pick[r : r + 64, span:], halos[1, row])
        if r + 64 == KEYS:
            x = jnp.where(first_rows < IMAGE_TOKENS - r, x, 0.0)
        og[r : r + 64] = x.astype(bf)

    arrived(2)
    arrived(3)
    for c in range(0, ff, 256):
        upper = dot(wide[...], w_up[:, c : c + 256]) + b_up[c : c + 256][None]
        act_grad = dot_nt(og[...], w_down[c : c + 256, :])
        value, slope = gelu_parts(upper)
        act[:, c : c + 256] = value.astype(bf)
        upg[:, c : c + 256] = (act_grad * slope[:KEYS]).astype(bf)
    for c in range(0, width, 256):
        y = hid[:, c : c + 256] + dot(act[...], w_down[:, c : c + 256]) + b_down[c : c + 256][None]
        wide[:, c : c + 256] = y.astype(bf)
        grad[:, c : c + 256] = dot_nt(upg[...], w_up[c : c + 256, :])
    out[row] = dot_tn(pick[:, :span], wide[...]).astype(bf)
    sides[0, row] = dot_tn(pick[:, span:], wide[...]).astype(bf)

    for r in range(0, KEYS, 64):
        e = grad[r : r + 64] * g2[...][None]
        n = n2[r : r + 64]
        mean = jnp.mean(e, axis=-1, keepdims=True)
        lean = jnp.mean(e * n, axis=-1, keepdims=True)
        h = og[r : r + 64].astype(jnp.float32) + inv2[r : r + 64] * (e - mean - n * lean)
        hid[r : r + 64] = h
        wide[r : r + 64] = h.astype(bf)
    for c in range(0, width, 256):
        og[:, c : c + 256] = dot_nt(wide[:KEYS], w_out[c : c + 256, :]).astype(bf)

    side_start(0, row)

    for p in range(width // PAIR):
        at = p * PAIR
        qp = qkv[:KEYS, at : at + PAIR]
        kp = qkv[:KEYS, width + at : width + at + PAIR]
        vp = qkv[:KEYS, 2 * width + at : 2 * width + at + PAIR]
        two_grads = both(og[:, at : at + PAIR])
        dp = dot_nt(vp, two_grads)
        pt = probs[p]
        pf = pt.astype(jnp.float32)
        inner = jnp.sum(pf * dp, axis=0, keepdims=True)
        ds = (pf * (dp - inner)).astype(bf)
        qkv[:KEYS, 2 * width + at : 2 * width + at + PAIR] = dot(pt, two_grads).astype(bf)
        head0, head1 = own_halves(dot_tn(kp, ds))
        qkv[:KEYS, width + at : width + at + PAIR] = dot(ds, both(qp)).astype(bf)
        turned[at : at + HEAD_FEATURES] = (head0 * SCALE).astype(bf)
        turned[at + HEAD_FEATURES : at + PAIR] = (head1 * SCALE).astype(bf)
    qkv[:KEYS, :width] = turned[...].T

    for c in range(0, width, 256):
        grad[:, c : c + 256] = dot_nt(qkv[:KEYS], w_qkv[c : c + 256, :])
    for r in range(0, KEYS, 64):
        e = grad[r : r + 64] * g1[...][None]
        n = n1[r : r + 64]
        mean = jnp.mean(e, axis=-1, keepdims=True)
        lean = jnp.mean(e * n, axis=-1, keepdims=True)
        x = hid[r : r + 64] + inv1[r : r + 64] * (e - mean - n * lean)
        if r == 0:
            part[...] += x
            x = jnp.where(is_prompt, 0.0, x)
        wide[r : r + 64] = x.astype(bf)
    tgr[row] = dot_tn(pick[:KEYS, :span], wide[:KEYS]).astype(bf)
    sides[1, row] = dot_tn(pick[:KEYS, span:], wide[:KEYS]).astype(bf)

    @pl.when(row > 0)
    def _():
        side_merge(0, row - 1)
        side_merge(1, row - 1)

    side_start(1, row)

    @pl.when(row == rows - 1)
    def _():
        def exchange(stage, source, target):
            partner = partners[(0, 1, 2, 3, 4, 2, 1, 0)[stage]]
            copy = pltpu.make_async_remote_copy(
                source, target, part_send.at[stage], part_recv.at[stage], device_id=partner, device_id_type=MESH
            )
            copy.start()
            copy.wait()

        def rows_at(first, size):
            return pl.ds(pl.multiple_of(first, 8), size)

        first = 0
        size = part.shape[0]
        kept = []
        base = 0
        for stage, bit in enumerate((group % 2, group // 2, index % 2)):
            size = size // 2
            kept.append((first, size, bit))
            landed = part_in.at[base : base + size]
            exchange(stage, part.at[rows_at(first + (1 - bit) * size, size)], landed)
            first = first + bit * size
            part[rows_at(first, size)] += landed[...]
            base += size
        for stage in (3, 4):
            landed = part_in.at[base : base + size]
            exchange(stage, part.at[rows_at(first, size)], landed)
            part[rows_at(first, size)] += landed[...]
            base += size
        for stage in (5, 6, 7):
            before, size, bit = kept[7 - stage]
            landed = part_in.at[base : base + size]
            exchange(stage, part.at[rows_at(before + bit * size, size)], landed)
            part[rows_at(before + (1 - bit) * size, size)] = landed[...]
            base += size
        pgr[...] = part[1 : PROMPTS + 1]
        side_merge(0, row)
        side_merge(1, row)
        for r in range(rows):
            for kind in range(2):
                sized(to_right, lambda size: halo_right(kind, r, size).wait_send())
                sized(to_left, lambda size: halo_left(kind, r, size).wait_send())
                sized(from_left, lambda size: side_left(kind, r, size).wait_send())
                sized(from_right, lambda size: side_right(kind, r, size).wait_send())


def image_body(
    tokens, prompts, image_id, prompt_slot, ln1_gain, ln1_bias, w_qkv, bias_qv, w_out, bias_out,
    ln2_gain, ln2_bias, w_up, bias_up, w_down, bias_down, cotangent,
):
    rows, span, width = tokens.shape
    ff = w_up.shape[1]
    f32, bf = jnp.float32, jnp.bfloat16
    dma = pltpu.SemaphoreType.DMA

    per_row = pl.BlockSpec((1, span, width), lambda r: (r, 0, 0))
    in_place = pl.BlockSpec(memory_space=pl.ANY)

    def whole(array):
        return pl.BlockSpec(array.shape, lambda r: (0,) * len(array.shape), pipeline_mode=pl.Buffered(1))

    return pl.pallas_call(
        row_kernel,
        grid=(rows,),
        in_specs=[
            whole(image_id), per_row, per_row, in_place, in_place, whole(prompts), whole(ln1_gain), whole(ln1_bias),
            in_place, whole(bias_qv), in_place, whole(bias_out), whole(ln2_gain), whole(ln2_bias), in_place,
            whole(bias_up), in_place, whole(bias_down),
        ],
        out_specs=[
            pl.BlockSpec((rows, span, width), lambda r: (0, 0, 0)), pl.BlockSpec((rows, span, width), lambda r: (0, 0, 0)),
            pl.BlockSpec((PROMPTS, width), lambda r: (0, 0)),
        ],
        out_shape=[
            jax.ShapeDtypeStruct((rows, span, width), bf), jax.ShapeDtypeStruct((rows, span, width), bf),
            jax.ShapeDtypeStruct((PROMPTS, width), f32),
        ],
        scratch_shapes=[
            pltpu.VMEM(w_qkv.shape, bf), pltpu.VMEM(w_out.shape, bf), pltpu.VMEM(w_up.shape, bf),
            pltpu.VMEM(w_down.shape, bf), dma((4,)),
            pltpu.VMEM((64, width), f32), pltpu.VMEM((SLOTS, span + 2 * HALO), bf), pltpu.VMEM((SLOTS, width), f32),
            pltpu.VMEM((KEYS, width), f32), pltpu.VMEM((KEYS, 1), f32), pltpu.VMEM((SLOTS, width), bf),
            pltpu.VMEM((SLOTS, 3 * width), bf), pltpu.VMEM((width // PAIR, KEYS, 2 * KEYS), bf),
            pltpu.VMEM((width, KEYS), bf), pltpu.VMEM((SLOTS, width), f32), pltpu.VMEM((KEYS, width), f32),
            pltpu.VMEM((KEYS, 1), f32), pltpu.VMEM((SLOTS, ff), bf), pltpu.VMEM((KEYS, ff), bf),
            pltpu.VMEM((KEYS, width), bf), pltpu.VMEM((KEYS, width), f32),
            pltpu.VMEM((2, rows, 2 * HALO, width), bf), dma((2, rows, 2)), dma((2, rows, 2)),
            pltpu.VMEM((2, rows, 2 * HALO, width), bf), pltpu.VMEM((2, rows, 2 * HALO, width), bf),
            dma((2, rows, 2)), dma((2, rows, 2)),
            pltpu.VMEM((64, width), f32), pltpu.VMEM((128, width), f32), dma((8,)), dma((8,)),
        ],
        compiler_params=pltpu.CompilerParams(
            vmem_limit_bytes=62 << 20, dimension_semantics=("arbitrary",), collective_id=0, has_side_effects=True
        ),
        name="layer_rows",
    )(
        image_id, tokens, cotangent, tokens, cotangent, prompts, ln1_gain, ln1_bias, w_qkv, bias_qv, w_out, bias_out,
        ln2_gain, ln2_bias, w_up, bias_up, w_down, bias_down,
    )


def body(tokens, prompts, image_id, *rest):
    if lax.axis_size("seq") == IMAGES_PER_ROW and lax.axis_size("batch") == 4 and tokens.shape[1] == KEYS:
        return image_body(tokens, prompts, image_id, *rest)
    return general_body(tokens, prompts, image_id, *rest)


def solution(mesh):
    in_specs = (
        P("batch", "seq", None),
        P(),
        P("batch", None),
        P("batch", "seq"),
        P(),
        P(),
        P(),
        P(),
        P(),
        P(),
        P(),
        P(),
        P(),
        P(),
        P(),
        P(),
        P("batch", "seq", None),
    )
    out_specs = (P("batch", "seq", None), P("batch", "seq", None), P())
    return jax.shard_map(body, mesh=mesh, in_specs=in_specs, out_specs=out_specs, check_vma=False)
```

```python
import functools

import jax
import jax.numpy as jnp
from jax import lax
from jax.experimental import pallas as pl
from jax.experimental.pallas import tpu as pltpu
from jax.sharding import PartitionSpec as P

ATTENTION_HEADS = 12
HEAD_FEATURES = 64
PROMPTS = 50
IMAGES_PER_ROW = 8
IMAGE_TOKENS = 247


def passed_along(block, axis, distance):
    devices = range(lax.axis_size(axis))
    route = [(i - distance, i) for i in devices if i - distance in devices]
    return lax.ppermute(block, axis, route)


def normalize(value_rows):
    mean = jnp.mean(value_rows, axis=-1, keepdims=True)
    centered = value_rows - mean
    inverse = lax.rsqrt(jnp.mean(centered * centered, axis=-1, keepdims=True) + 1e-06)
    return (centered * inverse, inverse)


def norm_back(grad_in, normal_draws, inverse, gain):
    scaled = grad_in * gain
    return inverse * (
        scaled
        - jnp.mean(scaled, axis=-1, keepdims=True)
        - normal_draws * jnp.mean(scaled * normal_draws, axis=-1, keepdims=True)
    )


def block_rows(rows, span):
    group = min(rows, max(1, 512 // span))
    while rows % group:
        group = group - 1
    return group


def masked_scores(query_rows, key_rows, query_ids, key_ids, own_pos, key_pos):
    scores = jnp.einsum(
        "gqhd,gkhd->ghqk", query_rows, key_rows, preferred_element_type=jnp.float32
    ) * HEAD_FEATURES ** (-0.5)
    same_image = (query_ids[:, :, None] == key_ids[:, None, :]) & (query_ids < IMAGES_PER_ROW)[
        :, :, None
    ]
    permitted_mask = same_image | (own_pos[:, None] == key_pos[None, :])[None]
    return jnp.where(permitted_mask[:, None], scores, -1e30)


def general_body(
    tokens,
    prompts,
    image_id,
    prompt_slot,
    ln1_gain,
    ln1_bias,
    w_qkv,
    bias_qv,
    w_out,
    bias_out,
    ln2_gain,
    ln2_bias,
    w_up,
    bias_up,
    w_down,
    bias_down,
    cotangent,
):
    rows, span, width = tokens.shape
    length = image_id.shape[1]
    start = lax.axis_index("seq") * span
    own_ids = lax.dynamic_slice_in_dim(image_id, start, span, 1)
    own_pos = start + jnp.arange(span, dtype=jnp.int32)
    valid = (own_ids < IMAGES_PER_ROW).astype(jnp.float32)
    one_hot = (prompt_slot[..., None] == jnp.arange(PROMPTS, dtype=jnp.int32)).astype(jnp.float32)
    placed = jnp.einsum("rsn,nd->rsd", one_hot, prompts, precision=lax.Precision.HIGHEST)
    is_prompt = (prompt_slot < PROMPTS)[..., None]
    inserted = jnp.where(is_prompt, placed, tokens.astype(jnp.float32))
    normal1, inverse1 = normalize(inserted)
    normed1 = (normal1 * ln1_gain + ln1_bias).astype(jnp.bfloat16)
    bias_three = jnp.concatenate(
        [bias_qv[:width], jnp.zeros((width,), jnp.float32), bias_qv[width:]]
    )
    query_key_value = (
        jnp.einsum("rsd,de->rse", normed1, w_qkv, preferred_element_type=jnp.float32) + bias_three
    ).astype(jnp.bfloat16)
    query_rows = query_key_value[..., :width]
    key_own = query_key_value[..., width : 2 * width]
    value_own = query_key_value[..., 2 * width :]
    reach = (IMAGE_TOKENS - 2 + span) // span
    offsets = list(range(-reach, reach + 1))
    key_parts = []
    value_parts = []
    for offset in offsets:
        if offset == 0:
            fetched_key, fetched_value = (key_own, value_own)
        else:
            fetched_key, fetched_value = passed_along((key_own, value_own), "seq", -offset)
        key_parts.append(fetched_key)
        value_parts.append(fetched_value)
    key_rows = jnp.concatenate(key_parts, axis=1)
    value_rows = jnp.concatenate(value_parts, axis=1)
    raw_pos = jnp.concatenate(
        [start + offset * span + jnp.arange(span, dtype=jnp.int32) for offset in offsets]
    )
    in_row = (raw_pos >= 0) & (raw_pos < length)
    taken = jnp.take(image_id, jnp.clip(raw_pos, 0, length - 1), axis=1)
    key_ids = jnp.where(in_row[None, :], taken, -1)
    key_pos = jnp.where(in_row, raw_pos, -1)
    key_count = key_rows.shape[1]
    group = block_rows(rows, span)

    def grouped(array):
        return array.reshape((rows // group, group) + array.shape[1:])

    query_heads = grouped(query_rows.reshape(rows, span, ATTENTION_HEADS, HEAD_FEATURES))
    key_heads = grouped(key_rows.reshape(rows, key_count, ATTENTION_HEADS, HEAD_FEATURES))
    value_heads = grouped(value_rows.reshape(rows, key_count, ATTENTION_HEADS, HEAD_FEATURES))
    query_ids = grouped(own_ids)
    grouped_key_ids = grouped(key_ids)

    def forward_block(inputs):
        query_blk, key_blk, value_blk, qid_blk, kid_blk = inputs
        scores = masked_scores(query_blk, key_blk, qid_blk, kid_blk, own_pos, key_pos)
        row_top = jnp.max(scores, axis=-1, keepdims=True)
        total = jnp.sum(jnp.exp(scores - row_top), axis=-1, keepdims=True)
        log_total = row_top + jnp.log(total)
        attention_weights = jnp.exp(scores - log_total).astype(jnp.bfloat16)
        attention_output = jnp.einsum(
            "vbta,vabj->vtbj", attention_weights, value_blk, preferred_element_type=jnp.float32
        )
        return (attention_output.astype(jnp.bfloat16), log_total[..., 0])

    attention_output, log_totals = lax.map(
        forward_block, (query_heads, key_heads, value_heads, query_ids, grouped_key_ids)
    )
    attention_output = attention_output.reshape(rows, span, width)
    hidden1 = (
        inserted
        + jnp.einsum("rsd,de->rse", attention_output, w_out, preferred_element_type=jnp.float32)
        + bias_out
    )
    normal2, inverse2 = normalize(hidden1)
    normed2 = (normal2 * ln2_gain + ln2_bias).astype(jnp.bfloat16)
    upper = jnp.einsum("rsd,df->rsf", normed2, w_up, preferred_element_type=jnp.float32) + bias_up
    activated, gelu_pull = jax.vjp(lambda inner: jax.nn.gelu(inner, approximate=False), upper)
    activated = activated.astype(jnp.bfloat16)
    output = (
        hidden1
        + jnp.einsum("rsf,fd->rsd", activated, w_down, preferred_element_type=jnp.float32)
        + bias_down
    ).astype(jnp.bfloat16)
    out_grad = cotangent.astype(jnp.float32) * valid[..., None]
    act_grad = jnp.einsum(
        "rsd,fd->rsf", out_grad.astype(jnp.bfloat16), w_down, preferred_element_type=jnp.float32
    )
    upper_grad = gelu_pull(act_grad)[0].astype(jnp.bfloat16)
    normed2_grad = jnp.einsum("rsf,df->rsd", upper_grad, w_up, preferred_element_type=jnp.float32)
    hidden1_grad = out_grad + norm_back(normed2_grad, normal2, inverse2, ln2_gain)
    attended_grad = jnp.einsum(
        "rse,de->rsd", hidden1_grad.astype(jnp.bfloat16), w_out, preferred_element_type=jnp.float32
    ).astype(jnp.bfloat16)
    attended_grad = grouped(attended_grad.reshape(rows, span, ATTENTION_HEADS, HEAD_FEATURES))

    def backward_block(inputs):
        query_blk, key_blk, value_blk, qid_blk, kid_blk, total_blk, grad_blk = inputs
        scores = masked_scores(query_blk, key_blk, qid_blk, kid_blk, own_pos, key_pos)
        attention_weights = jnp.exp(scores - total_blk[..., None])
        value_grad = jnp.einsum(
            "ghqk,gqhd->gkhd",
            attention_weights.astype(jnp.bfloat16),
            grad_blk,
            preferred_element_type=jnp.float32,
        )
        prob_grad = jnp.einsum(
            "gqhd,gkhd->ghqk", grad_blk, value_blk, preferred_element_type=jnp.float32
        )
        inner = jnp.sum(attention_weights * prob_grad, axis=-1, keepdims=True)
        score_grad = (attention_weights * (prob_grad - inner)).astype(jnp.bfloat16)
        query_grad = jnp.einsum(
            "vbta,vabj->vtbj", score_grad, key_blk, preferred_element_type=jnp.float32
        ) * HEAD_FEATURES ** (-0.5)
        key_grad = jnp.einsum(
            "ghqk,gqhd->gkhd", score_grad, query_blk, preferred_element_type=jnp.float32
        ) * HEAD_FEATURES ** (-0.5)
        return (query_grad, key_grad, value_grad)

    query_grad, key_grad, value_grad = lax.map(
        backward_block,
        (
            query_heads,
            key_heads,
            value_heads,
            query_ids,
            grouped_key_ids,
            log_totals,
            attended_grad,
        ),
    )
    query_grad = query_grad.reshape(rows, span, width)
    key_grad = key_grad.reshape(rows, key_count, width)
    value_grad = value_grad.reshape(rows, key_count, width)
    key_total = key_grad[:, reach * span : (reach + 1) * span]
    value_total = value_grad[:, reach * span : (reach + 1) * span]
    for offset in range(-reach, reach + 1):
        if offset != 0:
            first = (offset + reach) * span
            back_key, back_value = (
                passed_along(
                    key_grad[:, first : first + span].astype(jnp.bfloat16), "seq", offset
                ).astype(jnp.float32),
                passed_along(
                    value_grad[:, first : first + span].astype(jnp.bfloat16), "seq", offset
                ).astype(jnp.float32),
            )
            key_total = key_total + back_key
            value_total = value_total + back_value
    qkv_grad = jnp.concatenate([query_grad, key_total, value_total], axis=-1).astype(jnp.bfloat16)
    normed1_grad = jnp.einsum("rse,de->rsd", qkv_grad, w_qkv, preferred_element_type=jnp.float32)
    inserted_grad = hidden1_grad + norm_back(normed1_grad, normal1, inverse1, ln1_gain)
    token_gradient = jnp.where(is_prompt, 0.0, inserted_grad).astype(jnp.bfloat16)
    prompt_part = jnp.einsum("rsn,rsd->nd", one_hot, inserted_grad, precision=lax.Precision.HIGHEST)
    prompt_gradient = lax.psum(prompt_part, ("batch", "seq"))
    return (output, token_gradient, prompt_gradient)


MESH = pl.DeviceIdType.MESH
HALO = 64
SLOTS = 320
KEYS = 256
PAIR = 2 * HEAD_FEATURES
SCALE = HEAD_FEATURES ** (-0.5)
ERFC_RATE = 0.39
ERFC_TERMS = (
    0.23532515356929604,
    0.09138882070894727,
    0.6495583974454544,
    -0.6353990518468564,
    0.8866636223583176,
    -0.22753694392981927,
)


def dot(a, b):
    return lax.dot_general(a, b, (((1,), (0,)), ((), ())), preferred_element_type=jnp.float32)


def dot_nt(a, b):
    return lax.dot_general(a, b, (((1,), (1,)), ((), ())), preferred_element_type=jnp.float32)


def dot_tn(a, b):
    return lax.dot_general(a, b, (((0,), (0,)), ((), ())), preferred_element_type=jnp.float32)


def gelu_parts(upper):
    size = jnp.abs(upper)
    t = 1.0 / (1.0 + (ERFC_RATE * 0.5**0.5) * size)
    tail = jnp.full_like(t, 0.5 * ERFC_TERMS[-1])
    for term in ERFC_TERMS[-2::-1]:
        tail = tail * t + 0.5 * term
    bell = jnp.exp(-0.5 * upper * upper)
    tail = tail * t * bell
    below = jnp.where(upper < 0, tail, 1.0 - tail)
    return upper * below, below + upper * (bell * 0.3989422804014327)


def slot_map(ids, index, span):
    lane = lax.broadcasted_iota(jnp.int32, ids.shape, 1)

    def first(image):
        return jnp.min(jnp.where(ids == image, lane, ids.shape[1] * 2), axis=1, keepdims=True)

    low = index * span
    start = first(index)
    end = start + IMAGE_TOKENS
    before = jnp.where(index == 0, low, jnp.maximum(first(index - 1) + IMAGE_TOKENS, low))
    after = jnp.where(
        index == IMAGES_PER_ROW - 1, low + span, jnp.minimum(first(index + 1), low + span)
    )
    spot = lax.broadcasted_iota(jnp.int32, (1, span + 2 * HALO), 1)
    place = low + jnp.where(
        spot < span, spot, jnp.where(spot < span + HALO, spot - span - HALO, spot - HALO)
    )
    lead = jnp.maximum(start - before, 0)
    slot = jnp.where((place >= end) & (place < after), IMAGE_TOKENS + lead + place - end, -1)
    slot = jnp.where((place >= before) & (place < start), IMAGE_TOKENS + place - before, slot)
    return jnp.where((place >= start) & (place < end), place - start, slot)


def needed(tokens):
    return (tokens + 15) // 16 * 16


def sized(count, act):
    for size in range(16, HALO + 1, 16):
        pl.when(count == size)(functools.partial(act, size))


def row_kernel(
    ids, tok, cot, tok_all, cot_all, prompts, g1, b1, w_qkv_hbm, b_qv, w_out_hbm, b_out, g2, b2, w_up_hbm, b_up,
    w_down_hbm, b_down,
    out, tgr, pgr,
    w_qkv, w_out, w_up, w_down, w_sem,
    prom, pick, ins, n1, inv1, wide, qkv, probs, turned, hid, n2, inv2, act, upg, og, grad,
    halos, halo_send, halo_recv, sides, backs, side_send, side_recv,
    part, part_in, part_send, part_recv,
):
    index = lax.axis_index("seq")
    group = lax.axis_index("batch")
    row = pl.program_id(0)
    rows = tok_all.shape[0]
    span, width = tok.shape[1], tok.shape[2]
    ff = w_up.shape[1]
    bf = jnp.bfloat16
    last = IMAGES_PER_ROW - 1
    slack = span - IMAGE_TOKENS
    has_left, has_right = index > 0, index < last
    from_left = jnp.where(has_left, needed(slack * index), 0)
    from_right = jnp.where(has_right, needed(slack * (last - index)), 0)
    to_right = jnp.where(has_right, needed(slack * (index + 1)), 0)
    to_left = jnp.where(has_left, needed(slack * (IMAGES_PER_ROW - index)), 0)

    def weight(k):
        source = (w_qkv_hbm, w_out_hbm, w_up_hbm, w_down_hbm)[k]
        return pltpu.make_async_copy(source, (w_qkv, w_out, w_up, w_down)[k], w_sem.at[k])

    def arrived(k):
        pl.when(row == 0)(lambda: weight(k).wait())

    def seq_copy(source, target, send, recv, to):
        return pltpu.make_async_remote_copy(
            source, target, send, recv, device_id={"seq": to}, device_id_type=MESH
        )

    def halo_right(kind, r, size):
        source = (tok_all, cot_all)[kind].at[r, span - size :]
        target = halos.at[kind, r, HALO - size : HALO]
        return seq_copy(source, target, halo_send.at[kind, r, 0], halo_recv.at[kind, r, 0], index + 1)

    def halo_left(kind, r, size):
        source = (tok_all, cot_all)[kind].at[r, :size]
        target = halos.at[kind, r, HALO : HALO + size]
        return seq_copy(source, target, halo_send.at[kind, r, 1], halo_recv.at[kind, r, 1], index - 1)

    def halo_start(kind, r):
        sized(to_right, lambda size: halo_right(kind, r, size).start())
        sized(to_left, lambda size: halo_left(kind, r, size).start())

    def halo_wait(kind, r):
        sized(from_left, lambda size: halo_right(kind, r, size).wait_recv())
        sized(from_right, lambda size: halo_left(kind, r, size).wait_recv())

    def side_left(kind, r, size):
        source = sides.at[kind, r, HALO - size : HALO]
        target = backs.at[kind, r, 2 * HALO - size :]
        return seq_copy(source, target, side_send.at[kind, r, 0], side_recv.at[kind, r, 0], index - 1)

    def side_right(kind, r, size):
        source = sides.at[kind, r, HALO : HALO + size]
        target = backs.at[kind, r, :size]
        return seq_copy(source, target, side_send.at[kind, r, 1], side_recv.at[kind, r, 1], index + 1)

    def side_start(kind, r):
        sized(from_left, lambda size: side_left(kind, r, size).start())
        sized(from_right, lambda size: side_right(kind, r, size).start())

    def side_merge(kind, r):
        sized(to_right, lambda size: side_left(kind, r, size).wait_recv())
        sized(to_left, lambda size: side_right(kind, r, size).wait_recv())
        result = (out, tgr)[kind]
        result[r, :HALO] = result[r, :HALO] + backs[kind, r, :HALO]
        result[r, span - HALO :] = result[r, span - HALO :] + backs[kind, r, HALO:]

    def flipped(place, step):
        return place + step - 2 * step * (place // step % 2)

    partners = tuple({"batch": flipped(group, k)} for k in (1, 2)) + tuple({"seq": flipped(index, k)} for k in (1, 2, 4))

    @pl.when(row == 0)
    def _():
        for k in range(4):
            weight(k).start()
        halos[...] = jnp.zeros_like(halos)
        backs[...] = jnp.zeros_like(backs)
        barrier = pltpu.get_barrier_semaphore()
        for device in partners:
            pl.semaphore_signal(barrier, inc=1, device_id=device, device_id_type=MESH)
        @pl.when(has_left)
        def _():
            pl.semaphore_signal(barrier, inc=1, device_id={"seq": index - 1}, device_id_type=MESH)
        @pl.when(has_right)
        def _():
            pl.semaphore_signal(barrier, inc=1, device_id={"seq": index + 1}, device_id_type=MESH)
        prom[...] = jnp.zeros_like(prom)
        prom[1 : PROMPTS + 1] = prompts[...]
        part[...] = jnp.zeros_like(part)
        pl.semaphore_wait(barrier, len(partners) + jnp.where(has_left, 1, 0) + jnp.where(has_right, 1, 0))
        halo_start(0, 0)

    slot = slot_map(ids[pl.ds(row, 1)], index, span)
    slots = lax.broadcasted_iota(jnp.int32, (SLOTS, span + 2 * HALO), 0)
    pick[...] = jnp.where(slots == slot, 1.0, 0.0).astype(bf)

    first_rows = lax.broadcasted_iota(jnp.int32, (64, 1), 0)
    is_prompt = (first_rows >= 1) & (first_rows <= PROMPTS)
    halo_wait(0, row)
    halo_start(1, row)
    for r in range(0, SLOTS, 64):
        x = dot(pick[r : r + 64, :span], tok[0]) + dot(pick[r : r + 64, span:], halos[0, row])
        if r == 0:
            x = jnp.where(is_prompt, prom[...], x)
        ins[r : r + 64] = x
        mean = jnp.mean(x, axis=-1, keepdims=True)
        c = x - mean
        inv = lax.rsqrt(jnp.mean(c * c, axis=-1, keepdims=True) + 1e-06)
        c = c * inv
        if r < KEYS:
            n1[r : r + 64] = c
            inv1[r : r + 64] = inv
        wide[r : r + 64] = (c * g1[...][None] + b1[...][None]).astype(bf)

    arrived(0)
    for c in range(0, width, 256):
        q = dot(wide[:KEYS], w_qkv[:, c : c + 256]) + b_qv[c : c + 256][None]
        qkv[:KEYS, c : c + 256] = (q * SCALE).astype(bf)
        k = dot(wide[:KEYS], w_qkv[:, width + c : width + c + 256])
        qkv[:KEYS, width + c : width + c + 256] = k.astype(bf)
        v = dot(wide[...], w_qkv[:, 2 * width + c : 2 * width + c + 256]) + b_qv[width + c : width + c + 256][None]
        qkv[:, 2 * width + c : 2 * width + c + 256] = v.astype(bf)

    lane = lax.broadcasted_iota(jnp.int32, (1, PAIR), 1)
    low_half = jnp.where(lane < HEAD_FEATURES, 1.0, 0.0).astype(bf)
    high_half = jnp.where(lane < HEAD_FEATURES, 0.0, 1.0).astype(bf)

    def both(x):
        return jnp.concatenate([x * low_half, x * high_half], axis=0)

    def own_halves(x):
        return x[:HEAD_FEATURES, :KEYS], x[HEAD_FEATURES:, KEYS:]

    tail_rows = lax.broadcasted_iota(jnp.int32, (16, 1), 0) + (KEYS - 16)
    for p in range(width // PAIR):
        at = p * PAIR
        qp = qkv[:KEYS, at : at + PAIR]
        kp = qkv[:KEYS, width + at : width + at + PAIR]
        vp = qkv[:KEYS, 2 * width + at : 2 * width + at + PAIR]
        st = dot_nt(kp, both(qp))
        upper, lower = st[: KEYS - 16], st[KEYS - 16 :]
        lower = jnp.where(tail_rows < IMAGE_TOKENS, lower, -1e30)
        top = jnp.maximum(jnp.max(upper, axis=0, keepdims=True), jnp.max(lower, axis=0, keepdims=True))
        upper = jnp.exp(upper - top)
        lower = jnp.exp(lower - top)
        total = jnp.sum(upper, axis=0, keepdims=True) + jnp.sum(lower, axis=0, keepdims=True)
        share = 1.0 / total
        probs[p, : KEYS - 16] = (upper * share).astype(bf)
        probs[p, KEYS - 16 :] = (lower * share).astype(bf)
        head0, head1 = own_halves(dot_tn(vp, probs[p]))
        turned[at : at + HEAD_FEATURES] = head0.astype(bf)
        turned[at + HEAD_FEATURES : at + PAIR] = head1.astype(bf)

    key_rows = lax.broadcasted_iota(jnp.int32, (KEYS, 1), 0)
    attended = turned[...].T
    wide[:KEYS] = jnp.where(key_rows < IMAGE_TOKENS, attended, qkv[:KEYS, 2 * width :])
    wide[KEYS:] = qkv[KEYS:, 2 * width :]
    arrived(1)
    for c in range(0, width, 256):
        hid[:, c : c + 256] = ins[:, c : c + 256] + dot(wide[...], w_out[:, c : c + 256]) + b_out[c : c + 256][None]

    for r in range(0, SLOTS, 64):
        x = hid[r : r + 64]
        mean = jnp.mean(x, axis=-1, keepdims=True)
        c = x - mean
        inv = lax.rsqrt(jnp.mean(c * c, axis=-1, keepdims=True) + 1e-06)
        c = c * inv
        if r < KEYS:
            n2[r : r + 64] = c
            inv2[r : r + 64] = inv
        wide[r : r + 64] = (c * g2[...][None] + b2[...][None]).astype(bf)
    halo_wait(1, row)
    pl.when(row < rows - 1)(lambda: halo_start(0, row + 1))
    for r in range(0, KEYS, 64):
        x = dot(pick[r : r + 64, :span], cot[0]) + dot(pick[r : r + 64, span:], halos[1, row])
        if r + 64 == KEYS:
            x = jnp.where(first_rows < IMAGE_TOKENS - r, x, 0.0)
        og[r : r + 64] = x.astype(bf)

    arrived(2)
    arrived(3)
    for c in range(0, ff, 256):
        upper = dot(wide[...], w_up[:, c : c + 256]) + b_up[c : c + 256][None]
        act_grad = dot_nt(og[...], w_down[c : c + 256, :])
        value, slope = gelu_parts(upper)
        act[:, c : c + 256] = value.astype(bf)
        upg[:, c : c + 256] = (act_grad * slope[:KEYS]).astype(bf)
    for c in range(0, width, 256):
        y = hid[:, c : c + 256] + dot(act[...], w_down[:, c : c + 256]) + b_down[c : c + 256][None]
        wide[:, c : c + 256] = y.astype(bf)
        grad[:, c : c + 256] = dot_nt(upg[...], w_up[c : c + 256, :])
    out[row] = dot_tn(pick[:, :span], wide[...]).astype(bf)
    sides[0, row] = dot_tn(pick[:, span:], wide[...]).astype(bf)

    for r in range(0, KEYS, 64):
        e = grad[r : r + 64] * g2[...][None]
        n = n2[r : r + 64]
        mean = jnp.mean(e, axis=-1, keepdims=True)
        lean = jnp.mean(e * n, axis=-1, keepdims=True)
        h = og[r : r + 64].astype(jnp.float32) + inv2[r : r + 64] * (e - mean - n * lean)
        hid[r : r + 64] = h
        wide[r : r + 64] = h.astype(bf)
    for c in range(0, width, 256):
        og[:, c : c + 256] = dot_nt(wide[:KEYS], w_out[c : c + 256, :]).astype(bf)

    side_start(0, row)

    for p in range(width // PAIR):
        at = p * PAIR
        qp = qkv[:KEYS, at : at + PAIR]
        kp = qkv[:KEYS, width + at : width + at + PAIR]
        vp = qkv[:KEYS, 2 * width + at : 2 * width + at + PAIR]
        two_grads = both(og[:, at : at + PAIR])
        dp = dot_nt(vp, two_grads)
        pt = probs[p]
        pf = pt.astype(jnp.float32)
        inner = jnp.sum(pf * dp, axis=0, keepdims=True)
        ds = (pf * (dp - inner)).astype(bf)
        qkv[:KEYS, 2 * width + at : 2 * width + at + PAIR] = dot(pt, two_grads).astype(bf)
        head0, head1 = own_halves(dot_tn(kp, ds))
        qkv[:KEYS, width + at : width + at + PAIR] = dot(ds, both(qp)).astype(bf)
        turned[at : at + HEAD_FEATURES] = (head0 * SCALE).astype(bf)
        turned[at + HEAD_FEATURES : at + PAIR] = (head1 * SCALE).astype(bf)
    qkv[:KEYS, :width] = turned[...].T

    for c in range(0, width, 256):
        grad[:, c : c + 256] = dot_nt(qkv[:KEYS], w_qkv[c : c + 256, :])
    for r in range(0, KEYS, 64):
        e = grad[r : r + 64] * g1[...][None]
        n = n1[r : r + 64]
        mean = jnp.mean(e, axis=-1, keepdims=True)
        lean = jnp.mean(e * n, axis=-1, keepdims=True)
        x = hid[r : r + 64] + inv1[r : r + 64] * (e - mean - n * lean)
        if r == 0:
            part[...] += x
            x = jnp.where(is_prompt, 0.0, x)
        wide[r : r + 64] = x.astype(bf)
    tgr[row] = dot_tn(pick[:KEYS, :span], wide[:KEYS]).astype(bf)
    sides[1, row] = dot_tn(pick[:KEYS, span:], wide[:KEYS]).astype(bf)

    @pl.when(row > 0)
    def _():
        side_merge(0, row - 1)
        side_merge(1, row - 1)

    side_start(1, row)

    @pl.when(row == rows - 1)
    def _():
        def exchange(stage, source, target):
            partner = partners[(0, 1, 2, 3, 4, 2, 1, 0)[stage]]
            copy = pltpu.make_async_remote_copy(
                source, target, part_send.at[stage], part_recv.at[stage], device_id=partner, device_id_type=MESH
            )
            copy.start()
            copy.wait()

        def rows_at(first, size):
            return pl.ds(pl.multiple_of(first, 8), size)

        first = 0
        size = part.shape[0]
        kept = []
        base = 0
        for stage, bit in enumerate((group % 2, group // 2, index % 2)):
            size = size // 2
            kept.append((first, size, bit))
            landed = part_in.at[base : base + size]
            exchange(stage, part.at[rows_at(first + (1 - bit) * size, size)], landed)
            first = first + bit * size
            part[rows_at(first, size)] += landed[...]
            base += size
        for stage in (3, 4):
            landed = part_in.at[base : base + size]
            exchange(stage, part.at[rows_at(first, size)], landed)
            part[rows_at(first, size)] += landed[...]
            base += size
        for stage in (5, 6, 7):
            before, size, bit = kept[7 - stage]
            landed = part_in.at[base : base + size]
            exchange(stage, part.at[rows_at(before + bit * size, size)], landed)
            part[rows_at(before + (1 - bit) * size, size)] = landed[...]
            base += size
        pgr[...] = part[1 : PROMPTS + 1]
        side_merge(0, row)
        side_merge(1, row)
        for r in range(rows):
            for kind in range(2):
                sized(to_right, lambda size: halo_right(kind, r, size).wait_send())
                sized(to_left, lambda size: halo_left(kind, r, size).wait_send())
                sized(from_left, lambda size: side_left(kind, r, size).wait_send())
                sized(from_right, lambda size: side_right(kind, r, size).wait_send())


def image_body(
    tokens, prompts, image_id, prompt_slot, ln1_gain, ln1_bias, w_qkv, bias_qv, w_out, bias_out,
    ln2_gain, ln2_bias, w_up, bias_up, w_down, bias_down, cotangent,
):
    rows, span, width = tokens.shape
    ff = w_up.shape[1]
    f32, bf = jnp.float32, jnp.bfloat16
    dma = pltpu.SemaphoreType.DMA

    per_row = pl.BlockSpec((1, span, width), lambda r: (r, 0, 0))
    in_place = pl.BlockSpec(memory_space=pl.ANY)

    def whole(array):
        return pl.BlockSpec(array.shape, lambda r: (0,) * len(array.shape), pipeline_mode=pl.Buffered(1))

    return pl.pallas_call(
        row_kernel,
        grid=(rows,),
        in_specs=[
            whole(image_id), per_row, per_row, in_place, in_place, whole(prompts), whole(ln1_gain), whole(ln1_bias),
            in_place, whole(bias_qv), in_place, whole(bias_out), whole(ln2_gain), whole(ln2_bias), in_place,
            whole(bias_up), in_place, whole(bias_down),
        ],
        out_specs=[
            pl.BlockSpec((rows, span, width), lambda r: (0, 0, 0)), pl.BlockSpec((rows, span, width), lambda r: (0, 0, 0)),
            pl.BlockSpec((PROMPTS, width), lambda r: (0, 0)),
        ],
        out_shape=[
            jax.ShapeDtypeStruct((rows, span, width), bf), jax.ShapeDtypeStruct((rows, span, width), bf),
            jax.ShapeDtypeStruct((PROMPTS, width), f32),
        ],
        scratch_shapes=[
            pltpu.VMEM(w_qkv.shape, bf), pltpu.VMEM(w_out.shape, bf), pltpu.VMEM(w_up.shape, bf),
            pltpu.VMEM(w_down.shape, bf), dma((4,)),
            pltpu.VMEM((64, width), f32), pltpu.VMEM((SLOTS, span + 2 * HALO), bf), pltpu.VMEM((SLOTS, width), f32),
            pltpu.VMEM((KEYS, width), f32), pltpu.VMEM((KEYS, 1), f32), pltpu.VMEM((SLOTS, width), bf),
            pltpu.VMEM((SLOTS, 3 * width), bf), pltpu.VMEM((width // PAIR, KEYS, 2 * KEYS), bf),
            pltpu.VMEM((width, KEYS), bf), pltpu.VMEM((SLOTS, width), f32), pltpu.VMEM((KEYS, width), f32),
            pltpu.VMEM((KEYS, 1), f32), pltpu.VMEM((SLOTS, ff), bf), pltpu.VMEM((KEYS, ff), bf),
            pltpu.VMEM((KEYS, width), bf), pltpu.VMEM((KEYS, width), f32),
            pltpu.VMEM((2, rows, 2 * HALO, width), bf), dma((2, rows, 2)), dma((2, rows, 2)),
            pltpu.VMEM((2, rows, 2 * HALO, width), bf), pltpu.VMEM((2, rows, 2 * HALO, width), bf),
            dma((2, rows, 2)), dma((2, rows, 2)),
            pltpu.VMEM((64, width), f32), pltpu.VMEM((128, width), f32), dma((8,)), dma((8,)),
        ],
        compiler_params=pltpu.CompilerParams(
            vmem_limit_bytes=62 << 20, dimension_semantics=("arbitrary",), collective_id=0, has_side_effects=True
        ),
        name="layer_rows",
    )(
        image_id, tokens, cotangent, tokens, cotangent, prompts, ln1_gain, ln1_bias, w_qkv, bias_qv, w_out, bias_out,
        ln2_gain, ln2_bias, w_up, bias_up, w_down, bias_down,
    )


def body(tokens, prompts, image_id, *rest):
    if lax.axis_size("seq") == IMAGES_PER_ROW and lax.axis_size("batch") == 4 and tokens.shape[1] == KEYS:
        return image_body(tokens, prompts, image_id, *rest)
    return general_body(tokens, prompts, image_id, *rest)


def solution(mesh):
    in_specs = (
        P("batch", "seq", None),
        P(),
        P("batch", None),
        P("batch", "seq"),
        P(),
        P(),
        P(),
        P(),
        P(),
        P(),
        P(),
        P(),
        P(),
        P(),
        P(),
        P(),
        P("batch", "seq", None),
    )
    out_specs = (P("batch", "seq", None), P("batch", "seq", None), P())
    return jax.shard_map(body, mesh=mesh, in_specs=in_specs, out_specs=out_specs, check_vma=False)
```

```python
import functools

import jax
import jax.numpy as jnp
from jax import lax
from jax.experimental import pallas as pl
from jax.experimental.pallas import tpu as pltpu
from jax.sharding import PartitionSpec as P

ATTENTION_HEADS = 12
HEAD_FEATURES = 64
PROMPTS = 50
IMAGES_PER_ROW = 8
IMAGE_TOKENS = 247


def passed_along(block, axis, distance):
    devices = range(lax.axis_size(axis))
    route = [(i - distance, i) for i in devices if i - distance in devices]
    return lax.ppermute(block, axis, route)


def normalize(value_rows):
    mean = jnp.mean(value_rows, axis=-1, keepdims=True)
    centered = value_rows - mean
    inverse = lax.rsqrt(jnp.mean(centered * centered, axis=-1, keepdims=True) + 1e-06)
    return (centered * inverse, inverse)


def norm_back(grad_in, normal_draws, inverse, gain):
    scaled = grad_in * gain
    return inverse * (
        scaled
        - jnp.mean(scaled, axis=-1, keepdims=True)
        - normal_draws * jnp.mean(scaled * normal_draws, axis=-1, keepdims=True)
    )


def block_rows(rows, span):
    group = min(rows, max(1, 512 // span))
    while rows % group:
        group = group - 1
    return group


def masked_scores(query_rows, key_rows, query_ids, key_ids, own_pos, key_pos):
    scores = jnp.einsum(
        "gqhd,gkhd->ghqk", query_rows, key_rows, preferred_element_type=jnp.float32
    ) * HEAD_FEATURES ** (-0.5)
    same_image = (query_ids[:, :, None] == key_ids[:, None, :]) & (query_ids < IMAGES_PER_ROW)[
        :, :, None
    ]
    permitted_mask = same_image | (own_pos[:, None] == key_pos[None, :])[None]
    return jnp.where(permitted_mask[:, None], scores, -1e30)


def general_body(
    tokens,
    prompts,
    image_id,
    prompt_slot,
    ln1_gain,
    ln1_bias,
    w_qkv,
    bias_qv,
    w_out,
    bias_out,
    ln2_gain,
    ln2_bias,
    w_up,
    bias_up,
    w_down,
    bias_down,
    cotangent,
):
    rows, span, width = tokens.shape
    length = image_id.shape[1]
    start = lax.axis_index("seq") * span
    own_ids = lax.dynamic_slice_in_dim(image_id, start, span, 1)
    own_pos = start + jnp.arange(span, dtype=jnp.int32)
    valid = (own_ids < IMAGES_PER_ROW).astype(jnp.float32)
    one_hot = (prompt_slot[..., None] == jnp.arange(PROMPTS, dtype=jnp.int32)).astype(jnp.float32)
    placed = jnp.einsum("rsn,nd->rsd", one_hot, prompts, precision=lax.Precision.HIGHEST)
    is_prompt = (prompt_slot < PROMPTS)[..., None]
    inserted = jnp.where(is_prompt, placed, tokens.astype(jnp.float32))
    normal1, inverse1 = normalize(inserted)
    normed1 = (normal1 * ln1_gain + ln1_bias).astype(jnp.bfloat16)
    bias_three = jnp.concatenate(
        [bias_qv[:width], jnp.zeros((width,), jnp.float32), bias_qv[width:]]
    )
    query_key_value = (
        jnp.einsum("rsd,de->rse", normed1, w_qkv, preferred_element_type=jnp.float32) + bias_three
    ).astype(jnp.bfloat16)
    query_rows = query_key_value[..., :width]
    key_own = query_key_value[..., width : 2 * width]
    value_own = query_key_value[..., 2 * width :]
    reach = (IMAGE_TOKENS - 2 + span) // span
    offsets = list(range(-reach, reach + 1))
    key_parts = []
    value_parts = []
    for offset in offsets:
        if offset == 0:
            fetched_key, fetched_value = (key_own, value_own)
        else:
            fetched_key, fetched_value = passed_along((key_own, value_own), "seq", -offset)
        key_parts.append(fetched_key)
        value_parts.append(fetched_value)
    key_rows = jnp.concatenate(key_parts, axis=1)
    value_rows = jnp.concatenate(value_parts, axis=1)
    raw_pos = jnp.concatenate(
        [start + offset * span + jnp.arange(span, dtype=jnp.int32) for offset in offsets]
    )
    in_row = (raw_pos >= 0) & (raw_pos < length)
    taken = jnp.take(image_id, jnp.clip(raw_pos, 0, length - 1), axis=1)
    key_ids = jnp.where(in_row[None, :], taken, -1)
    key_pos = jnp.where(in_row, raw_pos, -1)
    key_count = key_rows.shape[1]
    group = block_rows(rows, span)

    def grouped(array):
        return array.reshape((rows // group, group) + array.shape[1:])

    query_heads = grouped(query_rows.reshape(rows, span, ATTENTION_HEADS, HEAD_FEATURES))
    key_heads = grouped(key_rows.reshape(rows, key_count, ATTENTION_HEADS, HEAD_FEATURES))
    value_heads = grouped(value_rows.reshape(rows, key_count, ATTENTION_HEADS, HEAD_FEATURES))
    query_ids = grouped(own_ids)
    grouped_key_ids = grouped(key_ids)

    def forward_block(inputs):
        query_blk, key_blk, value_blk, qid_blk, kid_blk = inputs
        scores = masked_scores(query_blk, key_blk, qid_blk, kid_blk, own_pos, key_pos)
        row_top = jnp.max(scores, axis=-1, keepdims=True)
        total = jnp.sum(jnp.exp(scores - row_top), axis=-1, keepdims=True)
        log_total = row_top + jnp.log(total)
        attention_weights = jnp.exp(scores - log_total).astype(jnp.bfloat16)
        attention_output = jnp.einsum(
            "vbta,vabj->vtbj", attention_weights, value_blk, preferred_element_type=jnp.float32
        )
        return (attention_output.astype(jnp.bfloat16), log_total[..., 0])

    attention_output, log_totals = lax.map(
        forward_block, (query_heads, key_heads, value_heads, query_ids, grouped_key_ids)
    )
    attention_output = attention_output.reshape(rows, span, width)
    hidden1 = (
        inserted
        + jnp.einsum("rsd,de->rse", attention_output, w_out, preferred_element_type=jnp.float32)
        + bias_out
    )
    normal2, inverse2 = normalize(hidden1)
    normed2 = (normal2 * ln2_gain + ln2_bias).astype(jnp.bfloat16)
    upper = jnp.einsum("rsd,df->rsf", normed2, w_up, preferred_element_type=jnp.float32) + bias_up
    activated, gelu_pull = jax.vjp(lambda inner: jax.nn.gelu(inner, approximate=False), upper)
    activated = activated.astype(jnp.bfloat16)
    output = (
        hidden1
        + jnp.einsum("rsf,fd->rsd", activated, w_down, preferred_element_type=jnp.float32)
        + bias_down
    ).astype(jnp.bfloat16)
    out_grad = cotangent.astype(jnp.float32) * valid[..., None]
    act_grad = jnp.einsum(
        "rsd,fd->rsf", out_grad.astype(jnp.bfloat16), w_down, preferred_element_type=jnp.float32
    )
    upper_grad = gelu_pull(act_grad)[0].astype(jnp.bfloat16)
    normed2_grad = jnp.einsum("rsf,df->rsd", upper_grad, w_up, preferred_element_type=jnp.float32)
    hidden1_grad = out_grad + norm_back(normed2_grad, normal2, inverse2, ln2_gain)
    attended_grad = jnp.einsum(
        "rse,de->rsd", hidden1_grad.astype(jnp.bfloat16), w_out, preferred_element_type=jnp.float32
    ).astype(jnp.bfloat16)
    attended_grad = grouped(attended_grad.reshape(rows, span, ATTENTION_HEADS, HEAD_FEATURES))

    def backward_block(inputs):
        query_blk, key_blk, value_blk, qid_blk, kid_blk, total_blk, grad_blk = inputs
        scores = masked_scores(query_blk, key_blk, qid_blk, kid_blk, own_pos, key_pos)
        attention_weights = jnp.exp(scores - total_blk[..., None])
        value_grad = jnp.einsum(
            "ghqk,gqhd->gkhd",
            attention_weights.astype(jnp.bfloat16),
            grad_blk,
            preferred_element_type=jnp.float32,
        )
        prob_grad = jnp.einsum(
            "gqhd,gkhd->ghqk", grad_blk, value_blk, preferred_element_type=jnp.float32
        )
        inner = jnp.sum(attention_weights * prob_grad, axis=-1, keepdims=True)
        score_grad = (attention_weights * (prob_grad - inner)).astype(jnp.bfloat16)
        query_grad = jnp.einsum(
            "vbta,vabj->vtbj", score_grad, key_blk, preferred_element_type=jnp.float32
        ) * HEAD_FEATURES ** (-0.5)
        key_grad = jnp.einsum(
            "ghqk,gqhd->gkhd", score_grad, query_blk, preferred_element_type=jnp.float32
        ) * HEAD_FEATURES ** (-0.5)
        return (query_grad, key_grad, value_grad)

    query_grad, key_grad, value_grad = lax.map(
        backward_block,
        (
            query_heads,
            key_heads,
            value_heads,
            query_ids,
            grouped_key_ids,
            log_totals,
            attended_grad,
        ),
    )
    query_grad = query_grad.reshape(rows, span, width)
    key_grad = key_grad.reshape(rows, key_count, width)
    value_grad = value_grad.reshape(rows, key_count, width)
    key_total = key_grad[:, reach * span : (reach + 1) * span]
    value_total = value_grad[:, reach * span : (reach + 1) * span]
    for offset in range(-reach, reach + 1):
        if offset != 0:
            first = (offset + reach) * span
            back_key, back_value = (
                passed_along(
                    key_grad[:, first : first + span].astype(jnp.bfloat16), "seq", offset
                ).astype(jnp.float32),
                passed_along(
                    value_grad[:, first : first + span].astype(jnp.bfloat16), "seq", offset
                ).astype(jnp.float32),
            )
            key_total = key_total + back_key
            value_total = value_total + back_value
    qkv_grad = jnp.concatenate([query_grad, key_total, value_total], axis=-1).astype(jnp.bfloat16)
    normed1_grad = jnp.einsum("rse,de->rsd", qkv_grad, w_qkv, preferred_element_type=jnp.float32)
    inserted_grad = hidden1_grad + norm_back(normed1_grad, normal1, inverse1, ln1_gain)
    token_gradient = jnp.where(is_prompt, 0.0, inserted_grad).astype(jnp.bfloat16)
    prompt_part = jnp.einsum("rsn,rsd->nd", one_hot, inserted_grad, precision=lax.Precision.HIGHEST)
    prompt_gradient = lax.psum(prompt_part, ("batch", "seq"))
    return (output, token_gradient, prompt_gradient)


MESH = pl.DeviceIdType.MESH
HALO = 64
PADS = 80
KEYS = 256
PAIR = 2 * HEAD_FEATURES
SCALE = HEAD_FEATURES ** (-0.5)
ERFC_RATE = 0.39
ERFC_TERMS = (
    0.23532515356929604,
    0.09138882070894727,
    0.6495583974454544,
    -0.6353990518468564,
    0.8866636223583176,
    -0.22753694392981927,
)


def dot(a, b):
    return lax.dot_general(a, b, (((1,), (0,)), ((), ())), preferred_element_type=jnp.float32)


def dot_nt(a, b):
    return lax.dot_general(a, b, (((1,), (1,)), ((), ())), preferred_element_type=jnp.float32)


def dot_tn(a, b):
    return lax.dot_general(a, b, (((0,), (0,)), ((), ())), preferred_element_type=jnp.float32)


def gelu_parts(upper):
    size = jnp.abs(upper)
    t = 1.0 / (1.0 + (ERFC_RATE * 0.5**0.5) * size)
    tail = jnp.full_like(t, 0.5 * ERFC_TERMS[-1])
    for term in ERFC_TERMS[-2::-1]:
        tail = tail * t + 0.5 * term
    bell = jnp.exp(-0.5 * upper * upper)
    tail = tail * t * bell
    below = jnp.where(upper < 0, tail, 1.0 - tail)
    return upper * below, below + upper * (bell * 0.3989422804014327)


def slot_map(ids, index, span):
    lane = lax.broadcasted_iota(jnp.int32, ids.shape, 1)

    def first(image):
        return jnp.min(jnp.where(ids == image, lane, ids.shape[1] * 2), axis=1, keepdims=True)

    low = index * span
    start = first(index)
    end = start + IMAGE_TOKENS
    before = jnp.where(index == 0, low, jnp.maximum(first(index - 1) + IMAGE_TOKENS, low))
    after = jnp.where(
        index == IMAGES_PER_ROW - 1, low + span, jnp.minimum(first(index + 1), low + span)
    )
    spot = lax.broadcasted_iota(jnp.int32, (1, span + 2 * HALO), 1)
    place = low + jnp.where(
        spot < span, spot, jnp.where(spot < span + HALO, spot - span - HALO, spot - HALO)
    )
    slot = jnp.where((place >= start) & (place < end), place - start, -1)
    own = low + lax.broadcasted_iota(jnp.int32, (1, span), 1)
    lead = jnp.maximum(start - before, 0)
    pad = jnp.where((own >= end) & (own < after), lead + own - end, -1)
    pad = jnp.where((own >= before) & (own < start), own - before, pad)
    return slot, pad


def needed(tokens):
    return (tokens + 15) // 16 * 16


def sized(count, act):
    for size in range(16, HALO + 1, 16):
        pl.when(count == size)(functools.partial(act, size))


def row_kernel(
    ids, tok, cot, tok_all, cot_all, prompts, g1, b1, w_qkv_hbm, b_qv, w_out_hbm, b_out, g2, b2, w_up_hbm, b_up,
    w_down_hbm, b_down,
    out, tgr, pgr,
    w_qkv, w_out, w_up, w_down, w_sem,
    prom, pick, pad_pick, pad_tok, ins, n1, inv1, wide, qkv, probs, turned, hid, n2, inv2, act, upg, og, grad,
    halos, halo_send, halo_recv, sides, backs, side_send, side_recv,
    part, part_in, part_floor, summed, part_send, part_recv,
):
    index = lax.axis_index("seq")
    group = lax.axis_index("batch")
    row = pl.program_id(0)
    rows = tok_all.shape[0]
    span, width = tok.shape[1], tok.shape[2]
    ff = w_up.shape[1]
    bf = jnp.bfloat16
    last = IMAGES_PER_ROW - 1
    slack = span - IMAGE_TOKENS
    has_left, has_right = index > 0, index < last
    from_left = jnp.where(has_left, needed(slack * index), 0)
    from_right = jnp.where(has_right, needed(slack * (last - index)), 0)
    to_right = jnp.where(has_right, needed(slack * (index + 1)), 0)
    to_left = jnp.where(has_left, needed(slack * (IMAGES_PER_ROW - index)), 0)

    def weight(k):
        source = (w_qkv_hbm, w_out_hbm, w_up_hbm, w_down_hbm)[k]
        return pltpu.make_async_copy(source, (w_qkv, w_out, w_up, w_down)[k], w_sem.at[k])

    def arrived(k):
        pl.when(row == 0)(lambda: weight(k).wait())

    def seq_copy(source, target, send, recv, to):
        return pltpu.make_async_remote_copy(
            source, target, send, recv, device_id={"seq": to}, device_id_type=MESH
        )

    def halo_right(kind, r, size):
        source = (tok_all, cot_all)[kind].at[r, span - size :]
        target = halos.at[kind, r, HALO - size : HALO]
        return seq_copy(source, target, halo_send.at[kind, r, 0], halo_recv.at[kind, r, 0], index + 1)

    def halo_left(kind, r, size):
        source = (tok_all, cot_all)[kind].at[r, :size]
        target = halos.at[kind, r, HALO : HALO + size]
        return seq_copy(source, target, halo_send.at[kind, r, 1], halo_recv.at[kind, r, 1], index - 1)

    def halo_start(kind, r):
        sized(to_right, lambda size: halo_right(kind, r, size).start())
        sized(to_left, lambda size: halo_left(kind, r, size).start())

    def halo_wait(kind, r):
        sized(from_left, lambda size: halo_right(kind, r, size).wait_recv())
        sized(from_right, lambda size: halo_left(kind, r, size).wait_recv())

    def side_left(kind, r, size):
        source = sides.at[kind, r, HALO - size : HALO]
        target = backs.at[kind, r, 2 * HALO - size :]
        return seq_copy(source, target, side_send.at[kind, r, 0], side_recv.at[kind, r, 0], index - 1)

    def side_right(kind, r, size):
        source = sides.at[kind, r, HALO : HALO + size]
        target = backs.at[kind, r, :size]
        return seq_copy(source, target, side_send.at[kind, r, 1], side_recv.at[kind, r, 1], index + 1)

    def side_start(kind, r):
        sized(from_left, lambda size: side_left(kind, r, size).start())
        sized(from_right, lambda size: side_right(kind, r, size).start())

    def side_merge(kind, r):
        sized(to_right, lambda size: side_left(kind, r, size).wait_recv())
        sized(to_left, lambda size: side_right(kind, r, size).wait_recv())
        result = (out, tgr)[kind]
        result[r, :HALO] = result[r, :HALO] + backs[kind, r, :HALO]
        result[r, span - HALO :] = result[r, span - HALO :] + backs[kind, r, HALO:]

    down, deep = index // 2, index % 2
    piece = group * 2 + deep
    mates = []
    for k in range(1, 8):
        other = lax.rem(piece + k, 8)
        mates.append((other, {"batch": other // 2, "seq": down * 2 + lax.rem(other, 2)}))
    floors = [{"batch": group, "seq": lax.rem(down + k, 4) * 2 + deep} for k in range(1, 4)]

    def eight(place):
        return pl.ds(pl.multiple_of(place * 8, 8), 8)

    def part_copy(k, source, target, device):
        return pltpu.make_async_remote_copy(
            source, target, part_send.at[k], part_recv.at[k], device_id=device, device_id_type=MESH
        )

    spread = [
        part_copy(k, part.at[eight(other)], part_in.at[eight(piece)], device)
        for k, (other, device) in enumerate(mates)
    ]
    climb = [
        part_copy(7 + k, part_floor.at[eight(down)], part_floor.at[eight(down)], device)
        for k, device in enumerate(floors)
    ]
    hand = [
        part_copy(10 + k, summed.at[eight(piece)], summed.at[eight(piece)], device)
        for k, (_, device) in enumerate(mates)
    ]
    partners = [device for _, device in mates] + floors

    @pl.when(row == 0)
    def _():
        for k in range(4):
            weight(k).start()
        halos[...] = jnp.zeros_like(halos)
        backs[...] = jnp.zeros_like(backs)
        barrier = pltpu.get_barrier_semaphore()
        for device in partners:
            pl.semaphore_signal(barrier, inc=1, device_id=device, device_id_type=MESH)
        @pl.when(has_left)
        def _():
            pl.semaphore_signal(barrier, inc=1, device_id={"seq": index - 1}, device_id_type=MESH)
        @pl.when(has_right)
        def _():
            pl.semaphore_signal(barrier, inc=1, device_id={"seq": index + 1}, device_id_type=MESH)
        prom[...] = jnp.zeros_like(prom)
        prom[1 : PROMPTS + 1] = prompts[...]
        part[...] = jnp.zeros_like(part)
        pl.semaphore_wait(barrier, len(partners) + jnp.where(has_left, 1, 0) + jnp.where(has_right, 1, 0))
        halo_start(0, 0)

    slot, pad = slot_map(ids[pl.ds(row, 1)], index, span)
    slots = lax.broadcasted_iota(jnp.int32, (KEYS, span + 2 * HALO), 0)
    pick[...] = jnp.where(slots == slot, 1.0, 0.0).astype(bf)
    pads = lax.broadcasted_iota(jnp.int32, (PADS, span), 0)
    pad_pick[row] = jnp.where(pads == pad, 1.0, 0.0).astype(bf)
    pad_tok[row] = dot(pad_pick[row], tok[0]).astype(bf)

    first_rows = lax.broadcasted_iota(jnp.int32, (64, 1), 0)
    is_prompt = (first_rows >= 1) & (first_rows <= PROMPTS)
    halo_wait(0, row)
    halo_start(1, row)
    for r in range(0, KEYS, 64):
        x = dot(pick[r : r + 64, :span], tok[0]) + dot(pick[r : r + 64, span:], halos[0, row])
        if r == 0:
            x = jnp.where(is_prompt, prom[...], x)
        ins[r : r + 64] = x
        c, inv = normalize(x)
        n1[r : r + 64] = c
        inv1[r : r + 64] = inv
        wide[r : r + 64] = (c * g1[...][None] + b1[...][None]).astype(bf)

    arrived(0)
    for c in range(0, width, 256):
        q = dot(wide[:KEYS], w_qkv[:, c : c + 256]) + b_qv[c : c + 256][None]
        qkv[:KEYS, c : c + 256] = (q * SCALE).astype(bf)
        k = dot(wide[:KEYS], w_qkv[:, width + c : width + c + 256])
        qkv[:KEYS, width + c : width + c + 256] = k.astype(bf)
        v = dot(wide[:KEYS], w_qkv[:, 2 * width + c : 2 * width + c + 256]) + b_qv[width + c : width + c + 256][None]
        qkv[:, 2 * width + c : 2 * width + c + 256] = v.astype(bf)

    lane = lax.broadcasted_iota(jnp.int32, (1, PAIR), 1)
    low_half = jnp.where(lane < HEAD_FEATURES, 1.0, 0.0).astype(bf)
    high_half = jnp.where(lane < HEAD_FEATURES, 0.0, 1.0).astype(bf)

    def both(x):
        return jnp.concatenate([x * low_half, x * high_half], axis=0)

    def own_halves(x):
        return x[:HEAD_FEATURES, :KEYS], x[HEAD_FEATURES:, KEYS:]

    tail_rows = lax.broadcasted_iota(jnp.int32, (16, 1), 0) + (KEYS - 16)
    for p in range(width // PAIR):
        at = p * PAIR
        qp = qkv[:KEYS, at : at + PAIR]
        kp = qkv[:KEYS, width + at : width + at + PAIR]
        vp = qkv[:KEYS, 2 * width + at : 2 * width + at + PAIR]
        st = dot_nt(kp, both(qp))
        upper, lower = st[: KEYS - 16], st[KEYS - 16 :]
        lower = jnp.where(tail_rows < IMAGE_TOKENS, lower, -1e30)
        top = jnp.maximum(jnp.max(upper, axis=0, keepdims=True), jnp.max(lower, axis=0, keepdims=True))
        upper = jnp.exp(upper - top)
        lower = jnp.exp(lower - top)
        total = jnp.sum(upper, axis=0, keepdims=True) + jnp.sum(lower, axis=0, keepdims=True)
        share = 1.0 / total
        probs[p, : KEYS - 16] = (upper * share).astype(bf)
        probs[p, KEYS - 16 :] = (lower * share).astype(bf)
        head0, head1 = own_halves(dot_tn(vp, probs[p]))
        turned[at : at + HEAD_FEATURES] = head0.astype(bf)
        turned[at + HEAD_FEATURES : at + PAIR] = head1.astype(bf)

    wide[:KEYS] = turned[...].T
    arrived(1)
    for c in range(0, width, 256):
        hid[:KEYS, c : c + 256] = ins[:KEYS, c : c + 256] + dot(wide[:KEYS], w_out[:, c : c + 256]) + b_out[c : c + 256][None]

    for r in range(0, KEYS, 64):
        c, inv = normalize(hid[r : r + 64])
        n2[r : r + 64] = c
        inv2[r : r + 64] = inv
        wide[r : r + 64] = (c * g2[...][None] + b2[...][None]).astype(bf)
    halo_wait(1, row)
    pl.when(row < rows - 1)(lambda: halo_start(0, row + 1))
    for r in range(0, KEYS, 64):
        x = dot(pick[r : r + 64, :span], cot[0]) + dot(pick[r : r + 64, span:], halos[1, row])
        og[r : r + 64] = x.astype(bf)

    arrived(2)
    arrived(3)
    for c in range(0, ff, 256):
        upper = dot(wide[:KEYS], w_up[:, c : c + 256]) + b_up[c : c + 256][None]
        act_grad = dot_nt(og[...], w_down[c : c + 256, :])
        value, slope = gelu_parts(upper)
        act[:KEYS, c : c + 256] = value.astype(bf)
        upg[:, c : c + 256] = (act_grad * slope).astype(bf)
    for c in range(0, width, 256):
        y = hid[:KEYS, c : c + 256] + dot(act[:KEYS], w_down[:, c : c + 256]) + b_down[c : c + 256][None]
        wide[:KEYS, c : c + 256] = y.astype(bf)
        grad[:, c : c + 256] = dot_nt(upg[...], w_up[c : c + 256, :])
    out[row] = dot_tn(pick[:, :span], wide[:KEYS]).astype(bf)
    sides[0, row] = dot_tn(pick[:, span:], wide[:KEYS]).astype(bf)

    for r in range(0, KEYS, 64):
        e = grad[r : r + 64] * g2[...][None]
        n = n2[r : r + 64]
        mean = jnp.mean(e, axis=-1, keepdims=True)
        lean = jnp.mean(e * n, axis=-1, keepdims=True)
        h = og[r : r + 64].astype(jnp.float32) + inv2[r : r + 64] * (e - mean - n * lean)
        hid[r : r + 64] = h
        wide[r : r + 64] = h.astype(bf)
    for c in range(0, width, 256):
        og[:, c : c + 256] = dot_nt(wide[:KEYS], w_out[c : c + 256, :]).astype(bf)

    side_start(0, row)

    for p in range(width // PAIR):
        at = p * PAIR
        qp = qkv[:KEYS, at : at + PAIR]
        kp = qkv[:KEYS, width + at : width + at + PAIR]
        vp = qkv[:KEYS, 2 * width + at : 2 * width + at + PAIR]
        two_grads = both(og[:, at : at + PAIR])
        dp = dot_nt(vp, two_grads)
        pt = probs[p]
        pf = pt.astype(jnp.float32)
        inner = jnp.sum(pf * dp, axis=0, keepdims=True)
        ds = (pf * (dp - inner)).astype(bf)
        qkv[:KEYS, 2 * width + at : 2 * width + at + PAIR] = dot(pt, two_grads).astype(bf)
        head0, head1 = own_halves(dot_tn(kp, ds))
        qkv[:KEYS, width + at : width + at + PAIR] = dot(ds, both(qp)).astype(bf)
        turned[at : at + HEAD_FEATURES] = (head0 * SCALE).astype(bf)
        turned[at + HEAD_FEATURES : at + PAIR] = (head1 * SCALE).astype(bf)
    qkv[:KEYS, :width] = turned[...].T

    for c in range(0, width, 256):
        grad[:, c : c + 256] = dot_nt(qkv[:KEYS], w_qkv[c : c + 256, :])
    for r in range(0, KEYS, 64):
        e = grad[r : r + 64] * g1[...][None]
        n = n1[r : r + 64]
        mean = jnp.mean(e, axis=-1, keepdims=True)
        lean = jnp.mean(e * n, axis=-1, keepdims=True)
        x = hid[r : r + 64] + inv1[r : r + 64] * (e - mean - n * lean)
        if r == 0:
            part[...] += x

            @pl.when(row == rows - 1)
            def _():
                for copy in spread:
                    copy.start()

            x = jnp.where(is_prompt, 0.0, x)
        wide[r : r + 64] = x.astype(bf)
    tgr[row] = dot_tn(pick[:, :span], wide[:KEYS]).astype(bf)
    sides[1, row] = dot_tn(pick[:, span:], wide[:KEYS]).astype(bf)

    @pl.when(row > 0)
    def _():
        side_merge(0, row - 1)
        side_merge(1, row - 1)

    side_start(1, row)

    @pl.when(row == rows - 1)
    def _():
        many = rows * PADS
        for r in range(rows):
            ins[r * PADS : (r + 1) * PADS] = pad_tok[r].astype(jnp.float32)
        for r in range(0, many, 64):
            c, _ = normalize(ins[r : r + 64])
            wide[r : r + 64] = (c * g1[...][None] + b1[...][None]).astype(bf)
        for c in range(0, width, 256):
            v = dot(wide[...], w_qkv[:, 2 * width + c : 2 * width + c + 256])
            act[:, c : c + 256] = (v + b_qv[width + c : width + c + 256][None]).astype(bf)
        for c in range(0, width, 256):
            h = ins[:, c : c + 256] + dot(act[:, :width], w_out[:, c : c + 256])
            hid[:, c : c + 256] = h + b_out[c : c + 256][None]
        for r in range(0, many, 64):
            c, _ = normalize(hid[r : r + 64])
            wide[r : r + 64] = (c * g2[...][None] + b2[...][None]).astype(bf)

        for copy in spread:
            copy.wait_recv()
        part_in[eight(piece)] = part[eight(piece)]
        mine = part_in[0:8]
        for k in range(8, 64, 8):
            mine = mine + part_in[k : k + 8]
        part_floor[eight(down)] = mine
        for copy in climb:
            copy.start()

        for c in range(0, ff, 256):
            upper = dot(wide[...], w_up[:, c : c + 256]) + b_up[c : c + 256][None]
            act[:, c : c + 256] = gelu_parts(upper)[0].astype(bf)

        for copy in climb:
            copy.wait_recv()
        summed[eight(piece)] = (part_floor[0:8] + part_floor[8:16]) + (part_floor[16:24] + part_floor[24:32])
        for copy in hand:
            copy.start()

        for c in range(0, width, 256):
            y = hid[:, c : c + 256] + dot(act[...], w_down[:, c : c + 256]) + b_down[c : c + 256][None]
            wide[:, c : c + 256] = y.astype(bf)
        for r in range(rows):
            out[r] = out[r] + dot_tn(pad_pick[r], wide[r * PADS : (r + 1) * PADS]).astype(bf)

        side_merge(0, row)
        side_merge(1, row)
        for copy in hand:
            copy.wait_recv()
        pgr[...] = summed[1 : PROMPTS + 1]
        for copy in spread + climb + hand:
            copy.wait_send()
        for r in range(rows):
            for kind in range(2):
                sized(to_right, lambda size: halo_right(kind, r, size).wait_send())
                sized(to_left, lambda size: halo_left(kind, r, size).wait_send())
                sized(from_left, lambda size: side_left(kind, r, size).wait_send())
                sized(from_right, lambda size: side_right(kind, r, size).wait_send())


def image_body(
    tokens, prompts, image_id, prompt_slot, ln1_gain, ln1_bias, w_qkv, bias_qv, w_out, bias_out,
    ln2_gain, ln2_bias, w_up, bias_up, w_down, bias_down, cotangent,
):
    rows, span, width = tokens.shape
    ff = w_up.shape[1]
    f32, bf = jnp.float32, jnp.bfloat16
    dma = pltpu.SemaphoreType.DMA

    per_row = pl.BlockSpec((1, span, width), lambda r: (r, 0, 0))
    in_place = pl.BlockSpec(memory_space=pl.ANY)

    def whole(array):
        return pl.BlockSpec(array.shape, lambda r: (0,) * len(array.shape), pipeline_mode=pl.Buffered(1))

    return pl.pallas_call(
        row_kernel,
        grid=(rows,),
        in_specs=[
            whole(image_id), per_row, per_row, in_place, in_place, whole(prompts), whole(ln1_gain), whole(ln1_bias),
            in_place, whole(bias_qv), in_place, whole(bias_out), whole(ln2_gain), whole(ln2_bias), in_place,
            whole(bias_up), in_place, whole(bias_down),
        ],
        out_specs=[
            pl.BlockSpec((rows, span, width), lambda r: (0, 0, 0)), pl.BlockSpec((rows, span, width), lambda r: (0, 0, 0)),
            pl.BlockSpec((PROMPTS, width), lambda r: (0, 0)),
        ],
        out_shape=[
            jax.ShapeDtypeStruct((rows, span, width), bf), jax.ShapeDtypeStruct((rows, span, width), bf),
            jax.ShapeDtypeStruct((PROMPTS, width), f32),
        ],
        scratch_shapes=[
            pltpu.VMEM(w_qkv.shape, bf), pltpu.VMEM(w_out.shape, bf), pltpu.VMEM(w_up.shape, bf),
            pltpu.VMEM(w_down.shape, bf), dma((4,)),
            pltpu.VMEM((64, width), f32), pltpu.VMEM((KEYS, span + 2 * HALO), bf), pltpu.VMEM((rows, PADS, span), bf),
            pltpu.VMEM((rows, PADS, width), bf), pltpu.VMEM((rows * PADS, width), f32), pltpu.VMEM((KEYS, width), f32),
            pltpu.VMEM((KEYS, 1), f32), pltpu.VMEM((rows * PADS, width), bf), pltpu.VMEM((KEYS, 3 * width), bf),
            pltpu.VMEM((width // PAIR, KEYS, 2 * KEYS), bf), pltpu.VMEM((width, KEYS), bf),
            pltpu.VMEM((rows * PADS, width), f32), pltpu.VMEM((KEYS, width), f32), pltpu.VMEM((KEYS, 1), f32),
            pltpu.VMEM((rows * PADS, ff), bf), pltpu.VMEM((KEYS, ff), bf),
            pltpu.VMEM((KEYS, width), bf), pltpu.VMEM((KEYS, width), f32),
            pltpu.VMEM((2, rows, 2 * HALO, width), bf), dma((2, rows, 2)), dma((2, rows, 2)),
            pltpu.VMEM((2, rows, 2 * HALO, width), bf), pltpu.VMEM((2, rows, 2 * HALO, width), bf),
            dma((2, rows, 2)), dma((2, rows, 2)),
            pltpu.VMEM((64, width), f32), pltpu.VMEM((64, width), f32), pltpu.VMEM((32, width), f32),
            pltpu.VMEM((64, width), f32), dma((17,)), dma((17,)),
        ],
        compiler_params=pltpu.CompilerParams(
            vmem_limit_bytes=62 << 20, dimension_semantics=("arbitrary",), collective_id=0, has_side_effects=True
        ),
        name="layer_rows",
    )(
        image_id, tokens, cotangent, tokens, cotangent, prompts, ln1_gain, ln1_bias, w_qkv, bias_qv, w_out, bias_out,
        ln2_gain, ln2_bias, w_up, bias_up, w_down, bias_down,
    )


def body(tokens, prompts, image_id, *rest):
    if lax.axis_size("seq") == IMAGES_PER_ROW and lax.axis_size("batch") == 4 and tokens.shape[1] == KEYS:
        return image_body(tokens, prompts, image_id, *rest)
    return general_body(tokens, prompts, image_id, *rest)


def solution(mesh):
    in_specs = (
        P("batch", "seq", None),
        P(),
        P("batch", None),
        P("batch", "seq"),
        P(),
        P(),
        P(),
        P(),
        P(),
        P(),
        P(),
        P(),
        P(),
        P(),
        P(),
        P(),
        P("batch", "seq", None),
    )
    out_specs = (P("batch", "seq", None), P("batch", "seq", None), P())
    return jax.shard_map(body, mesh=mesh, in_specs=in_specs, out_specs=out_specs, check_vma=False)
```

```python
import functools

import jax
import jax.numpy as jnp
from jax import lax
from jax.experimental import pallas as pl
from jax.experimental.pallas import tpu as pltpu
from jax.sharding import PartitionSpec as P

ATTENTION_HEADS = 12
HEAD_FEATURES = 64
PROMPTS = 50
IMAGES_PER_ROW = 8
IMAGE_TOKENS = 247


def passed_along(block, axis, distance):
    devices = range(lax.axis_size(axis))
    route = [(i - distance, i) for i in devices if i - distance in devices]
    return lax.ppermute(block, axis, route)


def normalize(value_rows):
    mean = jnp.mean(value_rows, axis=-1, keepdims=True)
    centered = value_rows - mean
    inverse = lax.rsqrt(jnp.mean(centered * centered, axis=-1, keepdims=True) + 1e-06)
    return (centered * inverse, inverse)


def norm_back(grad_in, normal_draws, inverse, gain):
    scaled = grad_in * gain
    return inverse * (
        scaled
        - jnp.mean(scaled, axis=-1, keepdims=True)
        - normal_draws * jnp.mean(scaled * normal_draws, axis=-1, keepdims=True)
    )


def block_rows(rows, span):
    group = min(rows, max(1, 512 // span))
    while rows % group:
        group = group - 1
    return group


def masked_scores(query_rows, key_rows, query_ids, key_ids, own_pos, key_pos):
    scores = jnp.einsum(
        "gqhd,gkhd->ghqk", query_rows, key_rows, preferred_element_type=jnp.float32
    ) * HEAD_FEATURES ** (-0.5)
    same_image = (query_ids[:, :, None] == key_ids[:, None, :]) & (query_ids < IMAGES_PER_ROW)[
        :, :, None
    ]
    permitted_mask = same_image | (own_pos[:, None] == key_pos[None, :])[None]
    return jnp.where(permitted_mask[:, None], scores, -1e30)


def general_body(
    tokens,
    prompts,
    image_id,
    prompt_slot,
    ln1_gain,
    ln1_bias,
    w_qkv,
    bias_qv,
    w_out,
    bias_out,
    ln2_gain,
    ln2_bias,
    w_up,
    bias_up,
    w_down,
    bias_down,
    cotangent,
):
    rows, span, width = tokens.shape
    length = image_id.shape[1]
    start = lax.axis_index("seq") * span
    own_ids = lax.dynamic_slice_in_dim(image_id, start, span, 1)
    own_pos = start + jnp.arange(span, dtype=jnp.int32)
    valid = (own_ids < IMAGES_PER_ROW).astype(jnp.float32)
    one_hot = (prompt_slot[..., None] == jnp.arange(PROMPTS, dtype=jnp.int32)).astype(jnp.float32)
    placed = jnp.einsum("rsn,nd->rsd", one_hot, prompts, precision=lax.Precision.HIGHEST)
    is_prompt = (prompt_slot < PROMPTS)[..., None]
    inserted = jnp.where(is_prompt, placed, tokens.astype(jnp.float32))
    normal1, inverse1 = normalize(inserted)
    normed1 = (normal1 * ln1_gain + ln1_bias).astype(jnp.bfloat16)
    bias_three = jnp.concatenate(
        [bias_qv[:width], jnp.zeros((width,), jnp.float32), bias_qv[width:]]
    )
    query_key_value = (
        jnp.einsum("rsd,de->rse", normed1, w_qkv, preferred_element_type=jnp.float32) + bias_three
    ).astype(jnp.bfloat16)
    query_rows = query_key_value[..., :width]
    key_own = query_key_value[..., width : 2 * width]
    value_own = query_key_value[..., 2 * width :]
    reach = (IMAGE_TOKENS - 2 + span) // span
    offsets = list(range(-reach, reach + 1))
    key_parts = []
    value_parts = []
    for offset in offsets:
        if offset == 0:
            fetched_key, fetched_value = (key_own, value_own)
        else:
            fetched_key, fetched_value = passed_along((key_own, value_own), "seq", -offset)
        key_parts.append(fetched_key)
        value_parts.append(fetched_value)
    key_rows = jnp.concatenate(key_parts, axis=1)
    value_rows = jnp.concatenate(value_parts, axis=1)
    raw_pos = jnp.concatenate(
        [start + offset * span + jnp.arange(span, dtype=jnp.int32) for offset in offsets]
    )
    in_row = (raw_pos >= 0) & (raw_pos < length)
    taken = jnp.take(image_id, jnp.clip(raw_pos, 0, length - 1), axis=1)
    key_ids = jnp.where(in_row[None, :], taken, -1)
    key_pos = jnp.where(in_row, raw_pos, -1)
    key_count = key_rows.shape[1]
    group = block_rows(rows, span)

    def grouped(array):
        return array.reshape((rows // group, group) + array.shape[1:])

    query_heads = grouped(query_rows.reshape(rows, span, ATTENTION_HEADS, HEAD_FEATURES))
    key_heads = grouped(key_rows.reshape(rows, key_count, ATTENTION_HEADS, HEAD_FEATURES))
    value_heads = grouped(value_rows.reshape(rows, key_count, ATTENTION_HEADS, HEAD_FEATURES))
    query_ids = grouped(own_ids)
    grouped_key_ids = grouped(key_ids)

    def forward_block(inputs):
        query_blk, key_blk, value_blk, qid_blk, kid_blk = inputs
        scores = masked_scores(query_blk, key_blk, qid_blk, kid_blk, own_pos, key_pos)
        row_top = jnp.max(scores, axis=-1, keepdims=True)
        total = jnp.sum(jnp.exp(scores - row_top), axis=-1, keepdims=True)
        log_total = row_top + jnp.log(total)
        attention_weights = jnp.exp(scores - log_total).astype(jnp.bfloat16)
        attention_output = jnp.einsum(
            "vbta,vabj->vtbj", attention_weights, value_blk, preferred_element_type=jnp.float32
        )
        return (attention_output.astype(jnp.bfloat16), log_total[..., 0])

    attention_output, log_totals = lax.map(
        forward_block, (query_heads, key_heads, value_heads, query_ids, grouped_key_ids)
    )
    attention_output = attention_output.reshape(rows, span, width)
    hidden1 = (
        inserted
        + jnp.einsum("rsd,de->rse", attention_output, w_out, preferred_element_type=jnp.float32)
        + bias_out
    )
    normal2, inverse2 = normalize(hidden1)
    normed2 = (normal2 * ln2_gain + ln2_bias).astype(jnp.bfloat16)
    upper = jnp.einsum("rsd,df->rsf", normed2, w_up, preferred_element_type=jnp.float32) + bias_up
    activated, gelu_pull = jax.vjp(lambda inner: jax.nn.gelu(inner, approximate=False), upper)
    activated = activated.astype(jnp.bfloat16)
    output = (
        hidden1
        + jnp.einsum("rsf,fd->rsd", activated, w_down, preferred_element_type=jnp.float32)
        + bias_down
    ).astype(jnp.bfloat16)
    out_grad = cotangent.astype(jnp.float32) * valid[..., None]
    act_grad = jnp.einsum(
        "rsd,fd->rsf", out_grad.astype(jnp.bfloat16), w_down, preferred_element_type=jnp.float32
    )
    upper_grad = gelu_pull(act_grad)[0].astype(jnp.bfloat16)
    normed2_grad = jnp.einsum("rsf,df->rsd", upper_grad, w_up, preferred_element_type=jnp.float32)
    hidden1_grad = out_grad + norm_back(normed2_grad, normal2, inverse2, ln2_gain)
    attended_grad = jnp.einsum(
        "rse,de->rsd", hidden1_grad.astype(jnp.bfloat16), w_out, preferred_element_type=jnp.float32
    ).astype(jnp.bfloat16)
    attended_grad = grouped(attended_grad.reshape(rows, span, ATTENTION_HEADS, HEAD_FEATURES))

    def backward_block(inputs):
        query_blk, key_blk, value_blk, qid_blk, kid_blk, total_blk, grad_blk = inputs
        scores = masked_scores(query_blk, key_blk, qid_blk, kid_blk, own_pos, key_pos)
        attention_weights = jnp.exp(scores - total_blk[..., None])
        value_grad = jnp.einsum(
            "ghqk,gqhd->gkhd",
            attention_weights.astype(jnp.bfloat16),
            grad_blk,
            preferred_element_type=jnp.float32,
        )
        prob_grad = jnp.einsum(
            "gqhd,gkhd->ghqk", grad_blk, value_blk, preferred_element_type=jnp.float32
        )
        inner = jnp.sum(attention_weights * prob_grad, axis=-1, keepdims=True)
        score_grad = (attention_weights * (prob_grad - inner)).astype(jnp.bfloat16)
        query_grad = jnp.einsum(
            "vbta,vabj->vtbj", score_grad, key_blk, preferred_element_type=jnp.float32
        ) * HEAD_FEATURES ** (-0.5)
        key_grad = jnp.einsum(
            "ghqk,gqhd->gkhd", score_grad, query_blk, preferred_element_type=jnp.float32
        ) * HEAD_FEATURES ** (-0.5)
        return (query_grad, key_grad, value_grad)

    query_grad, key_grad, value_grad = lax.map(
        backward_block,
        (
            query_heads,
            key_heads,
            value_heads,
            query_ids,
            grouped_key_ids,
            log_totals,
            attended_grad,
        ),
    )
    query_grad = query_grad.reshape(rows, span, width)
    key_grad = key_grad.reshape(rows, key_count, width)
    value_grad = value_grad.reshape(rows, key_count, width)
    key_total = key_grad[:, reach * span : (reach + 1) * span]
    value_total = value_grad[:, reach * span : (reach + 1) * span]
    for offset in range(-reach, reach + 1):
        if offset != 0:
            first = (offset + reach) * span
            back_key, back_value = (
                passed_along(
                    key_grad[:, first : first + span].astype(jnp.bfloat16), "seq", offset
                ).astype(jnp.float32),
                passed_along(
                    value_grad[:, first : first + span].astype(jnp.bfloat16), "seq", offset
                ).astype(jnp.float32),
            )
            key_total = key_total + back_key
            value_total = value_total + back_value
    qkv_grad = jnp.concatenate([query_grad, key_total, value_total], axis=-1).astype(jnp.bfloat16)
    normed1_grad = jnp.einsum("rse,de->rsd", qkv_grad, w_qkv, preferred_element_type=jnp.float32)
    inserted_grad = hidden1_grad + norm_back(normed1_grad, normal1, inverse1, ln1_gain)
    token_gradient = jnp.where(is_prompt, 0.0, inserted_grad).astype(jnp.bfloat16)
    prompt_part = jnp.einsum("rsn,rsd->nd", one_hot, inserted_grad, precision=lax.Precision.HIGHEST)
    prompt_gradient = lax.psum(prompt_part, ("batch", "seq"))
    return (output, token_gradient, prompt_gradient)


MESH = pl.DeviceIdType.MESH
HALO = 64
PADS = 80
CUTS = (4, 8)
KEYS = 256
PAIR = 2 * HEAD_FEATURES
SCALE = HEAD_FEATURES ** (-0.5)
ERFC_RATE = 0.39
ERFC_TERMS = (
    0.23532515356929604,
    0.09138882070894727,
    0.6495583974454544,
    -0.6353990518468564,
    0.8866636223583176,
    -0.22753694392981927,
)


def dot(a, b):
    return lax.dot_general(a, b, (((1,), (0,)), ((), ())), preferred_element_type=jnp.float32)


def dot_nt(a, b):
    return lax.dot_general(a, b, (((1,), (1,)), ((), ())), preferred_element_type=jnp.float32)


def dot_tn(a, b):
    return lax.dot_general(a, b, (((0,), (0,)), ((), ())), preferred_element_type=jnp.float32)


def gelu_parts(upper):
    size = jnp.abs(upper)
    t = 1.0 / (1.0 + (ERFC_RATE * 0.5**0.5) * size)
    tail = jnp.full_like(t, 0.5 * ERFC_TERMS[-1])
    for term in ERFC_TERMS[-2::-1]:
        tail = tail * t + 0.5 * term
    bell = jnp.exp(-0.5 * upper * upper)
    tail = tail * t * bell
    below = jnp.where(upper < 0, tail, 1.0 - tail)
    return upper * below, below + upper * (bell * 0.3989422804014327)


def slot_map(ids, index, span):
    lane = lax.broadcasted_iota(jnp.int32, ids.shape, 1)

    def first(image):
        return jnp.min(jnp.where(ids == image, lane, ids.shape[1] * 2), axis=1, keepdims=True)

    low = index * span
    start = first(index)
    end = start + IMAGE_TOKENS
    before = jnp.where(index == 0, low, jnp.maximum(first(index - 1) + IMAGE_TOKENS, low))
    after = jnp.where(
        index == IMAGES_PER_ROW - 1, low + span, jnp.minimum(first(index + 1), low + span)
    )
    spot = lax.broadcasted_iota(jnp.int32, (1, span + 2 * HALO), 1)
    place = low + jnp.where(
        spot < span, spot, jnp.where(spot < span + HALO, spot - span - HALO, spot - HALO)
    )
    slot = jnp.where((place >= start) & (place < end), place - start, -1)
    own = low + lax.broadcasted_iota(jnp.int32, (1, span), 1)
    lead = jnp.maximum(start - before, 0)
    pad = jnp.where((own >= end) & (own < after), lead + own - end, -1)
    pad = jnp.where((own >= before) & (own < start), own - before, pad)
    return slot, pad


def needed(tokens):
    return (tokens + 15) // 16 * 16


def sized(count, act):
    for size in range(16, HALO + 1, 16):
        pl.when(count == size)(functools.partial(act, size))


def row_kernel(
    ids, tok, cot, tok_all, cot_all, prompts, g1, b1, w_qkv_hbm, b_qv, w_out_hbm, b_out, g2, b2, w_up_hbm, b_up,
    w_down_hbm, b_down,
    out, tgr, pgr,
    w_qkv, w_out, w_up, w_down, w_sem,
    prom, pick, pad_pick, pad_wide, pad_hid, ins, n1, inv1, wide, qkv, probs, turned, hid, n2, inv2, act, upg, og, grad,
    halos, halo_send, halo_recv, sides, backs, side_send, side_recv,
    part, part_in, part_floor, summed, part_send, part_recv,
):
    index = lax.axis_index("seq")
    group = lax.axis_index("batch")
    row = pl.program_id(0)
    rows = tok_all.shape[0]
    span, width = tok.shape[1], tok.shape[2]
    ff = w_up.shape[1]
    bf = jnp.bfloat16
    last = IMAGES_PER_ROW - 1
    slack = span - IMAGE_TOKENS
    has_left, has_right = index > 0, index < last
    from_left = jnp.where(has_left, needed(slack * index), 0)
    from_right = jnp.where(has_right, needed(slack * (last - index)), 0)
    to_right = jnp.where(has_right, needed(slack * (index + 1)), 0)
    to_left = jnp.where(has_left, needed(slack * (IMAGES_PER_ROW - index)), 0)

    def weight(k):
        source = (w_qkv_hbm, w_out_hbm, w_up_hbm, w_down_hbm)[k]
        return pltpu.make_async_copy(source, (w_qkv, w_out, w_up, w_down)[k], w_sem.at[k])

    def seq_copy(source, target, send, recv, to):
        return pltpu.make_async_remote_copy(
            source, target, send, recv, device_id={"seq": to}, device_id_type=MESH
        )

    def halo_right(kind, r, size):
        source = (tok_all, cot_all)[kind].at[r, span - size :]
        target = halos.at[kind, r, HALO - size : HALO]
        return seq_copy(source, target, halo_send.at[kind, r, 0], halo_recv.at[kind, r, 0], index + 1)

    def halo_left(kind, r, size):
        source = (tok_all, cot_all)[kind].at[r, :size]
        target = halos.at[kind, r, HALO : HALO + size]
        return seq_copy(source, target, halo_send.at[kind, r, 1], halo_recv.at[kind, r, 1], index - 1)

    def halo_start(kind, r):
        sized(to_right, lambda size: halo_right(kind, r, size).start())
        sized(to_left, lambda size: halo_left(kind, r, size).start())

    def halo_wait(kind, r):
        sized(from_left, lambda size: halo_right(kind, r, size).wait_recv())
        sized(from_right, lambda size: halo_left(kind, r, size).wait_recv())

    def side_left(kind, r, size):
        source = sides.at[kind, r, HALO - size : HALO]
        target = backs.at[kind, r, 2 * HALO - size :]
        return seq_copy(source, target, side_send.at[kind, r, 0], side_recv.at[kind, r, 0], index - 1)

    def side_right(kind, r, size):
        source = sides.at[kind, r, HALO : HALO + size]
        target = backs.at[kind, r, :size]
        return seq_copy(source, target, side_send.at[kind, r, 1], side_recv.at[kind, r, 1], index + 1)

    def side_start(kind, r):
        sized(from_left, lambda size: side_left(kind, r, size).start())
        sized(from_right, lambda size: side_right(kind, r, size).start())

    def side_merge(kind, r):
        sized(to_right, lambda size: side_left(kind, r, size).wait_recv())
        sized(to_left, lambda size: side_right(kind, r, size).wait_recv())
        result = (out, tgr)[kind]
        result[r, :HALO] = result[r, :HALO] + backs[kind, r, :HALO]
        result[r, span - HALO :] = result[r, span - HALO :] + backs[kind, r, HALO:]

    down, deep = index // 2, index % 2
    piece = group * 2 + deep
    mates = []
    for k in range(1, 8):
        other = lax.rem(piece + k, 8)
        mates.append((other, {"batch": other // 2, "seq": down * 2 + lax.rem(other, 2)}))
    floors = [{"batch": group, "seq": lax.rem(down + k, 4) * 2 + deep} for k in range(1, 4)]

    def eight(place):
        return pl.ds(pl.multiple_of(place * 8, 8), 8)

    def part_copy(k, source, target, device):
        return pltpu.make_async_remote_copy(
            source, target, part_send.at[k], part_recv.at[k], device_id=device, device_id_type=MESH
        )

    pieces = PROMPTS // 8 + 1
    spread = [
        (other, part_copy(k, part.at[eight(other)], part_in.at[eight(piece)], device))
        for k, (other, device) in enumerate(mates)
    ]
    climb = [
        part_copy(7 + k, part_floor.at[eight(down)], part_floor.at[eight(down)], device)
        for k, device in enumerate(floors)
    ]
    hand = [
        part_copy(10 + k, summed.at[eight(piece)], summed.at[eight(piece)], device)
        for k, (_, device) in enumerate(mates)
    ]
    partners = [device for _, device in mates] + floors
    senders = [lax.rem(piece + 8 - k, 8) for k in range(1, 8)]

    @pl.when(row == 0)
    def _():
        for k in range(2):
            weight(k).start()
        halos[...] = jnp.zeros_like(halos)
        backs[...] = jnp.zeros_like(backs)
        barrier = pltpu.get_barrier_semaphore()
        for device in partners:
            pl.semaphore_signal(barrier, inc=1, device_id=device, device_id_type=MESH)
        @pl.when(has_left)
        def _():
            pl.semaphore_signal(barrier, inc=1, device_id={"seq": index - 1}, device_id_type=MESH)
        @pl.when(has_right)
        def _():
            pl.semaphore_signal(barrier, inc=1, device_id={"seq": index + 1}, device_id_type=MESH)
        prom[...] = jnp.zeros_like(prom)
        prom[1 : PROMPTS + 1] = prompts[...]
        part[...] = jnp.zeros_like(part)
        pl.semaphore_wait(barrier, len(partners) + jnp.where(has_left, 1, 0) + jnp.where(has_right, 1, 0))
        halo_start(0, 0)
        halo_start(1, 0)
        many = rows * PADS
        for r in range(rows):
            pads = lax.broadcasted_iota(jnp.int32, (PADS, span), 0)
            pad_pick[r] = jnp.where(pads == slot_map(ids[r : r + 1], index, span)[1], 1.0, 0.0).astype(bf)
            ins[r * PADS : (r + 1) * PADS] = dot(pad_pick[r], tok[r])
        for r in range(0, many, 64):
            c, _ = normalize(ins[r : r + 64])
            wide[r : r + 64] = (c * g1[...][None] + b1[...][None]).astype(bf)
        weight(0).wait()
        for c in range(0, width, 256):
            v = dot(wide[...], w_qkv[:, 2 * width + c : 2 * width + c + 256])
            act[:, c : c + 256] = (v + b_qv[width + c : width + c + 256][None]).astype(bf)
        weight(1).wait()
        for k in range(2, 4):
            weight(k).start()
        for c in range(0, width, 256):
            h = ins[:, c : c + 256] + dot(act[:, :width], w_out[:, c : c + 256])
            pad_hid[:, c : c + 256] = h + b_out[c : c + 256][None]
        for r in range(0, many, 64):
            c, _ = normalize(pad_hid[r : r + 64])
            pad_wide[r : r + 64] = (c * g2[...][None] + b2[...][None]).astype(bf)
        for k in range(2, 4):
            weight(k).wait()

    halo_wait(0, row)
    halo_wait(1, row)

    @pl.when(row < rows - 1)
    def _():
        halo_start(0, row + 1)
        halo_start(1, row + 1)

    @pl.when(row > 0)
    def _():
        side_start(0, row - 1)
        side_start(1, row - 1)

    @pl.when(row > 1)
    def _():
        side_merge(0, row - 2)
        side_merge(1, row - 2)

    slot, _ = slot_map(ids[pl.ds(row, 1)], index, span)
    slots = lax.broadcasted_iota(jnp.int32, (KEYS, span + 2 * HALO), 0)
    pick[...] = jnp.where(slots == slot, 1.0, 0.0).astype(bf)

    first_rows = lax.broadcasted_iota(jnp.int32, (64, 1), 0)
    is_prompt = (first_rows >= 1) & (first_rows <= PROMPTS)
    for r in range(0, KEYS, 64):
        x = dot(pick[r : r + 64, :span], tok[row]) + dot(pick[r : r + 64, span:], halos[0, row])
        if r == 0:
            x = jnp.where(is_prompt, prom[...], x)
        ins[r : r + 64] = x
        c, inv = normalize(x)
        n1[r : r + 64] = c
        inv1[r : r + 64] = inv
        wide[r : r + 64] = (c * g1[...][None] + b1[...][None]).astype(bf)

    for c in range(0, width, 256):
        q = dot(wide[:KEYS], w_qkv[:, c : c + 256]) + b_qv[c : c + 256][None]
        qkv[:KEYS, c : c + 256] = (q * SCALE).astype(bf)
        k = dot(wide[:KEYS], w_qkv[:, width + c : width + c + 256])
        qkv[:KEYS, width + c : width + c + 256] = k.astype(bf)
        v = dot(wide[:KEYS], w_qkv[:, 2 * width + c : 2 * width + c + 256]) + b_qv[width + c : width + c + 256][None]
        qkv[:, 2 * width + c : 2 * width + c + 256] = v.astype(bf)

    lane = lax.broadcasted_iota(jnp.int32, (1, PAIR), 1)
    low_half = jnp.where(lane < HEAD_FEATURES, 1.0, 0.0).astype(bf)
    high_half = jnp.where(lane < HEAD_FEATURES, 0.0, 1.0).astype(bf)

    def both(x):
        return jnp.concatenate([x * low_half, x * high_half], axis=0)

    def own_halves(x):
        return x[:HEAD_FEATURES, :KEYS], x[HEAD_FEATURES:, KEYS:]

    tail_rows = lax.broadcasted_iota(jnp.int32, (16, 1), 0) + (KEYS - 16)
    for p in range(width // PAIR):
        at = p * PAIR
        qp = qkv[:KEYS, at : at + PAIR]
        kp = qkv[:KEYS, width + at : width + at + PAIR]
        vp = qkv[:KEYS, 2 * width + at : 2 * width + at + PAIR]
        st = dot_nt(kp, both(qp))
        upper, lower = st[: KEYS - 16], st[KEYS - 16 :]
        lower = jnp.where(tail_rows < IMAGE_TOKENS, lower, -1e30)
        top = jnp.maximum(jnp.max(upper, axis=0, keepdims=True), jnp.max(lower, axis=0, keepdims=True))
        upper = jnp.exp(upper - top)
        lower = jnp.exp(lower - top)
        total = jnp.sum(upper, axis=0, keepdims=True) + jnp.sum(lower, axis=0, keepdims=True)
        share = 1.0 / total
        probs[p, : KEYS - 16] = (upper * share).astype(bf)
        probs[p, KEYS - 16 :] = (lower * share).astype(bf)
        head0, head1 = own_halves(dot_tn(vp, probs[p]))
        turned[at : at + HEAD_FEATURES] = head0.astype(bf)
        turned[at + HEAD_FEATURES : at + PAIR] = head1.astype(bf)

    wide[:KEYS] = turned[...].T
    for c in range(0, width, 256):
        hid[:KEYS, c : c + 256] = ins[:KEYS, c : c + 256] + dot(wide[:KEYS], w_out[:, c : c + 256]) + b_out[c : c + 256][None]

    for r in range(0, KEYS, 64):
        c, inv = normalize(hid[r : r + 64])
        n2[r : r + 64] = c
        inv2[r : r + 64] = inv
        wide[r : r + 64] = (c * g2[...][None] + b2[...][None]).astype(bf)
    for r in range(0, KEYS, 64):
        x = dot(pick[r : r + 64, :span], cot[0]) + dot(pick[r : r + 64, span:], halos[1, row])
        og[r : r + 64] = x.astype(bf)

    for c in range(0, ff, 256):
        upper = dot(wide[:KEYS], w_up[:, c : c + 256]) + b_up[c : c + 256][None]
        act_grad = dot_nt(og[...], w_down[c : c + 256, :])
        value, slope = gelu_parts(upper)
        act[:KEYS, c : c + 256] = value.astype(bf)
        upg[:, c : c + 256] = (act_grad * slope).astype(bf)
    for c in range(0, width, 256):
        y = hid[:KEYS, c : c + 256] + dot(act[:KEYS], w_down[:, c : c + 256]) + b_down[c : c + 256][None]
        wide[:KEYS, c : c + 256] = y.astype(bf)
        grad[:, c : c + 256] = dot_nt(upg[...], w_up[c : c + 256, :])
    out[row] = dot_tn(pick[:, :span], wide[:KEYS]).astype(bf)
    sides[0, row] = dot_tn(pick[:, span:], wide[:KEYS]).astype(bf)

    for r in range(0, KEYS, 64):
        e = grad[r : r + 64] * g2[...][None]
        n = n2[r : r + 64]
        mean = jnp.mean(e, axis=-1, keepdims=True)
        lean = jnp.mean(e * n, axis=-1, keepdims=True)
        h = og[r : r + 64].astype(jnp.float32) + inv2[r : r + 64] * (e - mean - n * lean)
        hid[r : r + 64] = h
        wide[r : r + 64] = h.astype(bf)
    for c in range(0, width, 256):
        og[:, c : c + 256] = dot_nt(wide[:KEYS], w_out[c : c + 256, :]).astype(bf)

    for p in range(width // PAIR):
        at = p * PAIR
        qp = qkv[:KEYS, at : at + PAIR]
        kp = qkv[:KEYS, width + at : width + at + PAIR]
        vp = qkv[:KEYS, 2 * width + at : 2 * width + at + PAIR]
        two_grads = both(og[:, at : at + PAIR])
        dp = dot_nt(vp, two_grads)
        pt = probs[p]
        pf = pt.astype(jnp.float32)
        inner = jnp.sum(pf * dp, axis=0, keepdims=True)
        ds = (pf * (dp - inner)).astype(bf)
        qkv[:KEYS, 2 * width + at : 2 * width + at + PAIR] = dot(pt, two_grads).astype(bf)
        head0, head1 = own_halves(dot_tn(kp, ds))
        qkv[:KEYS, width + at : width + at + PAIR] = dot(ds, both(qp)).astype(bf)
        turned[at : at + HEAD_FEATURES] = (head0 * SCALE).astype(bf)
        turned[at + HEAD_FEATURES : at + PAIR] = (head1 * SCALE).astype(bf)
    qkv[:KEYS, :width] = turned[...].T

    for c in range(0, width, 256):
        grad[:, c : c + 256] = dot_nt(qkv[:KEYS], w_qkv[c : c + 256, :])
    for r in range(0, KEYS, 64):
        e = grad[r : r + 64] * g1[...][None]
        n = n1[r : r + 64]
        mean = jnp.mean(e, axis=-1, keepdims=True)
        lean = jnp.mean(e * n, axis=-1, keepdims=True)
        x = hid[r : r + 64] + inv1[r : r + 64] * (e - mean - n * lean)
        if r == 0:
            part[...] += x
            x = jnp.where(is_prompt, 0.0, x)
        wide[r : r + 64] = x.astype(bf)
    @pl.when(row == rows - 1)
    def _():
        for other, copy in spread:
            pl.when(other < pieces)(copy.start)

    tgr[row] = dot_tn(pick[:, :span], wide[:KEYS]).astype(bf)
    sides[1, row] = dot_tn(pick[:, span:], wide[:KEYS]).astype(bf)

    @pl.when(row == rows - 1)
    def _():
        side_start(0, row)
        side_start(1, row)

        def pad_up(first, last):
            for c in range(first * 256, last * 256, 256):
                upper = dot(pad_wide[...], w_up[:, c : c + 256]) + b_up[c : c + 256][None]
                act[:, c : c + 256] = gelu_parts(upper)[0].astype(bf)

        chunks = ff // 256
        pad_up(0, chunks * CUTS[0] // 12)
        @pl.when(piece < pieces)
        def _():
            for _, copy in spread:
                copy.wait_recv()
            part_in[eight(piece)] = part[eight(piece)]
            mine = part_in[0:8]
            for k in range(8, 64, 8):
                mine = mine + part_in[k : k + 8]
            part_floor[eight(down)] = mine
            for copy in climb:
                copy.start()

        pad_up(chunks * CUTS[0] // 12, chunks * CUTS[1] // 12)
        @pl.when(piece < pieces)
        def _():
            for copy in climb:
                copy.wait_recv()
            summed[eight(piece)] = (part_floor[0:8] + part_floor[8:16]) + (part_floor[16:24] + part_floor[24:32])
            for copy in hand:
                copy.start()

        pad_up(chunks * CUTS[1] // 12, chunks)
        for c in range(0, width, 256):
            y = pad_hid[:, c : c + 256] + dot(act[...], w_down[:, c : c + 256]) + b_down[c : c + 256][None]
            wide[:, c : c + 256] = y.astype(bf)
        for r in range(rows):
            out[r] = out[r] + dot_tn(pad_pick[r], wide[r * PADS : (r + 1) * PADS]).astype(bf)

        for r in (rows - 2, rows - 1):
            side_merge(0, r)
            side_merge(1, r)
        for back, copy in zip(senders, hand):
            pl.when(back < pieces)(copy.wait_recv)
        pgr[...] = summed[1 : PROMPTS + 1]
        for other, copy in spread:
            pl.when(other < pieces)(copy.wait_send)

        @pl.when(piece < pieces)
        def _():
            for copy in climb + hand:
                copy.wait_send()

        for r in range(rows):
            for kind in range(2):
                sized(to_right, lambda size: halo_right(kind, r, size).wait_send())
                sized(to_left, lambda size: halo_left(kind, r, size).wait_send())
                sized(from_left, lambda size: side_left(kind, r, size).wait_send())
                sized(from_right, lambda size: side_right(kind, r, size).wait_send())


def image_body(
    tokens, prompts, image_id, prompt_slot, ln1_gain, ln1_bias, w_qkv, bias_qv, w_out, bias_out,
    ln2_gain, ln2_bias, w_up, bias_up, w_down, bias_down, cotangent,
):
    rows, span, width = tokens.shape
    ff = w_up.shape[1]
    f32, bf = jnp.float32, jnp.bfloat16
    dma = pltpu.SemaphoreType.DMA

    per_row = pl.BlockSpec((1, span, width), lambda r: (r, 0, 0))
    in_place = pl.BlockSpec(memory_space=pl.ANY)

    def whole(array):
        return pl.BlockSpec(array.shape, lambda r: (0,) * len(array.shape), pipeline_mode=pl.Buffered(1))

    return pl.pallas_call(
        row_kernel,
        grid=(rows,),
        in_specs=[
            whole(image_id), whole(tokens), per_row, in_place, in_place, whole(prompts), whole(ln1_gain), whole(ln1_bias),
            in_place, whole(bias_qv), in_place, whole(bias_out), whole(ln2_gain), whole(ln2_bias), in_place,
            whole(bias_up), in_place, whole(bias_down),
        ],
        out_specs=[pl.BlockSpec(memory_space=pltpu.VMEM)] * 3,
        out_shape=[
            pltpu.VMEM((rows, span, width), bf), pltpu.VMEM((rows, span, width), bf), pltpu.VMEM((PROMPTS, width), f32),
        ],
        scratch_shapes=[
            pltpu.VMEM(w_qkv.shape, bf), pltpu.VMEM(w_out.shape, bf), pltpu.VMEM(w_up.shape, bf),
            pltpu.VMEM(w_down.shape, bf), dma((4,)),
            pltpu.VMEM((64, width), f32), pltpu.VMEM((KEYS, span + 2 * HALO), bf), pltpu.VMEM((rows, PADS, span), bf),
            pltpu.VMEM((rows * PADS, width), bf), pltpu.VMEM((rows * PADS, width), f32), pltpu.VMEM((rows * PADS, width), f32), pltpu.VMEM((KEYS, width), f32),
            pltpu.VMEM((KEYS, 1), f32), pltpu.VMEM((rows * PADS, width), bf), pltpu.VMEM((KEYS, 3 * width), bf),
            pltpu.VMEM((width // PAIR, KEYS, 2 * KEYS), bf), pltpu.VMEM((width, KEYS), bf),
            pltpu.VMEM((rows * PADS, width), f32), pltpu.VMEM((KEYS, width), f32), pltpu.VMEM((KEYS, 1), f32),
            pltpu.VMEM((rows * PADS, ff), bf), pltpu.VMEM((KEYS, ff), bf),
            pltpu.VMEM((KEYS, width), bf), pltpu.VMEM((KEYS, width), f32),
            pltpu.VMEM((2, rows, 2 * HALO, width), bf), dma((2, rows, 2)), dma((2, rows, 2)),
            pltpu.VMEM((2, rows, 2 * HALO, width), bf), pltpu.VMEM((2, rows, 2 * HALO, width), bf),
            dma((2, rows, 2)), dma((2, rows, 2)),
            pltpu.VMEM((64, width), f32), pltpu.VMEM((64, width), f32), pltpu.VMEM((32, width), f32),
            pltpu.VMEM((64, width), f32), dma((17,)), dma((17,)),
        ],
        compiler_params=pltpu.CompilerParams(
            vmem_limit_bytes=56 << 20, dimension_semantics=("arbitrary",), collective_id=0, has_side_effects=True
        ),
        name="layer_rows",
    )(
        image_id, tokens, cotangent, tokens, cotangent, prompts, ln1_gain, ln1_bias, w_qkv, bias_qv, w_out, bias_out,
        ln2_gain, ln2_bias, w_up, bias_up, w_down, bias_down,
    )


def body(tokens, prompts, image_id, *rest):
    if lax.axis_size("seq") == IMAGES_PER_ROW and lax.axis_size("batch") == 4 and tokens.shape[1] == KEYS:
        return image_body(tokens, prompts, image_id, *rest)
    return general_body(tokens, prompts, image_id, *rest)


def solution(mesh):
    in_specs = (
        P("batch", "seq", None),
        P(),
        P("batch", None),
        P("batch", "seq"),
        P(),
        P(),
        P(),
        P(),
        P(),
        P(),
        P(),
        P(),
        P(),
        P(),
        P(),
        P(),
        P("batch", "seq", None),
    )
    out_specs = (P("batch", "seq", None), P("batch", "seq", None), P())
    return jax.shard_map(body, mesh=mesh, in_specs=in_specs, out_specs=out_specs, check_vma=False)
```

```python
import functools

import jax
import jax.numpy as jnp
from jax import lax
from jax.experimental import pallas as pl
from jax.experimental.pallas import tpu as pltpu
from jax.sharding import PartitionSpec as P

ATTENTION_HEADS = 12
HEAD_FEATURES = 64
PROMPTS = 50
IMAGES_PER_ROW = 8
IMAGE_TOKENS = 247


def passed_along(block, axis, distance):
    devices = range(lax.axis_size(axis))
    route = [(i - distance, i) for i in devices if i - distance in devices]
    return lax.ppermute(block, axis, route)


def normalize(value_rows):
    mean = jnp.mean(value_rows, axis=-1, keepdims=True)
    centered = value_rows - mean
    inverse = lax.rsqrt(jnp.mean(centered * centered, axis=-1, keepdims=True) + 1e-06)
    return (centered * inverse, inverse)


def norm_back(grad_in, normal_draws, inverse, gain):
    scaled = grad_in * gain
    return inverse * (
        scaled
        - jnp.mean(scaled, axis=-1, keepdims=True)
        - normal_draws * jnp.mean(scaled * normal_draws, axis=-1, keepdims=True)
    )


def block_rows(rows, span):
    group = min(rows, max(1, 512 // span))
    while rows % group:
        group = group - 1
    return group


def masked_scores(query_rows, key_rows, query_ids, key_ids, own_pos, key_pos):
    scores = jnp.einsum(
        "gqhd,gkhd->ghqk", query_rows, key_rows, preferred_element_type=jnp.float32
    ) * HEAD_FEATURES ** (-0.5)
    same_image = (query_ids[:, :, None] == key_ids[:, None, :]) & (query_ids < IMAGES_PER_ROW)[
        :, :, None
    ]
    permitted_mask = same_image | (own_pos[:, None] == key_pos[None, :])[None]
    return jnp.where(permitted_mask[:, None], scores, -1e30)


def general_body(
    tokens,
    prompts,
    image_id,
    prompt_slot,
    ln1_gain,
    ln1_bias,
    w_qkv,
    bias_qv,
    w_out,
    bias_out,
    ln2_gain,
    ln2_bias,
    w_up,
    bias_up,
    w_down,
    bias_down,
    cotangent,
):
    rows, span, width = tokens.shape
    length = image_id.shape[1]
    start = lax.axis_index("seq") * span
    own_ids = lax.dynamic_slice_in_dim(image_id, start, span, 1)
    own_pos = start + jnp.arange(span, dtype=jnp.int32)
    valid = (own_ids < IMAGES_PER_ROW).astype(jnp.float32)
    one_hot = (prompt_slot[..., None] == jnp.arange(PROMPTS, dtype=jnp.int32)).astype(jnp.float32)
    placed = jnp.einsum("rsn,nd->rsd", one_hot, prompts, precision=lax.Precision.HIGHEST)
    is_prompt = (prompt_slot < PROMPTS)[..., None]
    inserted = jnp.where(is_prompt, placed, tokens.astype(jnp.float32))
    normal1, inverse1 = normalize(inserted)
    normed1 = (normal1 * ln1_gain + ln1_bias).astype(jnp.bfloat16)
    bias_three = jnp.concatenate(
        [bias_qv[:width], jnp.zeros((width,), jnp.float32), bias_qv[width:]]
    )
    query_key_value = (
        jnp.einsum("rsd,de->rse", normed1, w_qkv, preferred_element_type=jnp.float32) + bias_three
    ).astype(jnp.bfloat16)
    query_rows = query_key_value[..., :width]
    key_own = query_key_value[..., width : 2 * width]
    value_own = query_key_value[..., 2 * width :]
    reach = (IMAGE_TOKENS - 2 + span) // span
    offsets = list(range(-reach, reach + 1))
    key_parts = []
    value_parts = []
    for offset in offsets:
        if offset == 0:
            fetched_key, fetched_value = (key_own, value_own)
        else:
            fetched_key, fetched_value = passed_along((key_own, value_own), "seq", -offset)
        key_parts.append(fetched_key)
        value_parts.append(fetched_value)
    key_rows = jnp.concatenate(key_parts, axis=1)
    value_rows = jnp.concatenate(value_parts, axis=1)
    raw_pos = jnp.concatenate(
        [start + offset * span + jnp.arange(span, dtype=jnp.int32) for offset in offsets]
    )
    in_row = (raw_pos >= 0) & (raw_pos < length)
    taken = jnp.take(image_id, jnp.clip(raw_pos, 0, length - 1), axis=1)
    key_ids = jnp.where(in_row[None, :], taken, -1)
    key_pos = jnp.where(in_row, raw_pos, -1)
    key_count = key_rows.shape[1]
    group = block_rows(rows, span)

    def grouped(array):
        return array.reshape((rows // group, group) + array.shape[1:])

    query_heads = grouped(query_rows.reshape(rows, span, ATTENTION_HEADS, HEAD_FEATURES))
    key_heads = grouped(key_rows.reshape(rows, key_count, ATTENTION_HEADS, HEAD_FEATURES))
    value_heads = grouped(value_rows.reshape(rows, key_count, ATTENTION_HEADS, HEAD_FEATURES))
    query_ids = grouped(own_ids)
    grouped_key_ids = grouped(key_ids)

    def forward_block(inputs):
        query_blk, key_blk, value_blk, qid_blk, kid_blk = inputs
        scores = masked_scores(query_blk, key_blk, qid_blk, kid_blk, own_pos, key_pos)
        row_top = jnp.max(scores, axis=-1, keepdims=True)
        total = jnp.sum(jnp.exp(scores - row_top), axis=-1, keepdims=True)
        log_total = row_top + jnp.log(total)
        attention_weights = jnp.exp(scores - log_total).astype(jnp.bfloat16)
        attention_output = jnp.einsum(
            "vbta,vabj->vtbj", attention_weights, value_blk, preferred_element_type=jnp.float32
        )
        return (attention_output.astype(jnp.bfloat16), log_total[..., 0])

    attention_output, log_totals = lax.map(
        forward_block, (query_heads, key_heads, value_heads, query_ids, grouped_key_ids)
    )
    attention_output = attention_output.reshape(rows, span, width)
    hidden1 = (
        inserted
        + jnp.einsum("rsd,de->rse", attention_output, w_out, preferred_element_type=jnp.float32)
        + bias_out
    )
    normal2, inverse2 = normalize(hidden1)
    normed2 = (normal2 * ln2_gain + ln2_bias).astype(jnp.bfloat16)
    upper = jnp.einsum("rsd,df->rsf", normed2, w_up, preferred_element_type=jnp.float32) + bias_up
    activated, gelu_pull = jax.vjp(lambda inner: jax.nn.gelu(inner, approximate=False), upper)
    activated = activated.astype(jnp.bfloat16)
    output = (
        hidden1
        + jnp.einsum("rsf,fd->rsd", activated, w_down, preferred_element_type=jnp.float32)
        + bias_down
    ).astype(jnp.bfloat16)
    out_grad = cotangent.astype(jnp.float32) * valid[..., None]
    act_grad = jnp.einsum(
        "rsd,fd->rsf", out_grad.astype(jnp.bfloat16), w_down, preferred_element_type=jnp.float32
    )
    upper_grad = gelu_pull(act_grad)[0].astype(jnp.bfloat16)
    normed2_grad = jnp.einsum("rsf,df->rsd", upper_grad, w_up, preferred_element_type=jnp.float32)
    hidden1_grad = out_grad + norm_back(normed2_grad, normal2, inverse2, ln2_gain)
    attended_grad = jnp.einsum(
        "rse,de->rsd", hidden1_grad.astype(jnp.bfloat16), w_out, preferred_element_type=jnp.float32
    ).astype(jnp.bfloat16)
    attended_grad = grouped(attended_grad.reshape(rows, span, ATTENTION_HEADS, HEAD_FEATURES))

    def backward_block(inputs):
        query_blk, key_blk, value_blk, qid_blk, kid_blk, total_blk, grad_blk = inputs
        scores = masked_scores(query_blk, key_blk, qid_blk, kid_blk, own_pos, key_pos)
        attention_weights = jnp.exp(scores - total_blk[..., None])
        value_grad = jnp.einsum(
            "ghqk,gqhd->gkhd",
            attention_weights.astype(jnp.bfloat16),
            grad_blk,
            preferred_element_type=jnp.float32,
        )
        prob_grad = jnp.einsum(
            "gqhd,gkhd->ghqk", grad_blk, value_blk, preferred_element_type=jnp.float32
        )
        inner = jnp.sum(attention_weights * prob_grad, axis=-1, keepdims=True)
        score_grad = (attention_weights * (prob_grad - inner)).astype(jnp.bfloat16)
        query_grad = jnp.einsum(
            "vbta,vabj->vtbj", score_grad, key_blk, preferred_element_type=jnp.float32
        ) * HEAD_FEATURES ** (-0.5)
        key_grad = jnp.einsum(
            "ghqk,gqhd->gkhd", score_grad, query_blk, preferred_element_type=jnp.float32
        ) * HEAD_FEATURES ** (-0.5)
        return (query_grad, key_grad, value_grad)

    query_grad, key_grad, value_grad = lax.map(
        backward_block,
        (
            query_heads,
            key_heads,
            value_heads,
            query_ids,
            grouped_key_ids,
            log_totals,
            attended_grad,
        ),
    )
    query_grad = query_grad.reshape(rows, span, width)
    key_grad = key_grad.reshape(rows, key_count, width)
    value_grad = value_grad.reshape(rows, key_count, width)
    key_total = key_grad[:, reach * span : (reach + 1) * span]
    value_total = value_grad[:, reach * span : (reach + 1) * span]
    for offset in range(-reach, reach + 1):
        if offset != 0:
            first = (offset + reach) * span
            back_key, back_value = (
                passed_along(
                    key_grad[:, first : first + span].astype(jnp.bfloat16), "seq", offset
                ).astype(jnp.float32),
                passed_along(
                    value_grad[:, first : first + span].astype(jnp.bfloat16), "seq", offset
                ).astype(jnp.float32),
            )
            key_total = key_total + back_key
            value_total = value_total + back_value
    qkv_grad = jnp.concatenate([query_grad, key_total, value_total], axis=-1).astype(jnp.bfloat16)
    normed1_grad = jnp.einsum("rse,de->rsd", qkv_grad, w_qkv, preferred_element_type=jnp.float32)
    inserted_grad = hidden1_grad + norm_back(normed1_grad, normal1, inverse1, ln1_gain)
    token_gradient = jnp.where(is_prompt, 0.0, inserted_grad).astype(jnp.bfloat16)
    prompt_part = jnp.einsum("rsn,rsd->nd", one_hot, inserted_grad, precision=lax.Precision.HIGHEST)
    prompt_gradient = lax.psum(prompt_part, ("batch", "seq"))
    return (output, token_gradient, prompt_gradient)


MESH = pl.DeviceIdType.MESH
HALO = 64
PADS = 80
CUTS = (4, 8)
KEYS = 256
PAIR = 2 * HEAD_FEATURES
SCALE = HEAD_FEATURES ** (-0.5)
ERFC_RATE = 0.39
ERFC_TERMS = (
    0.23532515356929604,
    0.09138882070894727,
    0.6495583974454544,
    -0.6353990518468564,
    0.8866636223583176,
    -0.22753694392981927,
)


def dot(a, b):
    return lax.dot_general(a, b, (((1,), (0,)), ((), ())), preferred_element_type=jnp.float32)


def dot_nt(a, b):
    return lax.dot_general(a, b, (((1,), (1,)), ((), ())), preferred_element_type=jnp.float32)


def dot_tn(a, b):
    return lax.dot_general(a, b, (((0,), (0,)), ((), ())), preferred_element_type=jnp.float32)


def gelu_parts(upper):
    size = jnp.abs(upper)
    t = 1.0 / (1.0 + (ERFC_RATE * 0.5**0.5) * size)
    tail = jnp.full_like(t, 0.5 * ERFC_TERMS[-1])
    for term in ERFC_TERMS[-2::-1]:
        tail = tail * t + 0.5 * term
    bell = jnp.exp(-0.5 * upper * upper)
    tail = tail * t * bell
    below = jnp.where(upper < 0, tail, 1.0 - tail)
    return upper * below, below + upper * (bell * 0.3989422804014327)


def slot_map(ids, index, span):
    lane = lax.broadcasted_iota(jnp.int32, ids.shape, 1)

    def first(image):
        return jnp.min(jnp.where(ids == image, lane, ids.shape[1] * 2), axis=1, keepdims=True)

    low = index * span
    start = first(index)
    end = start + IMAGE_TOKENS
    before = jnp.where(index == 0, low, jnp.maximum(first(index - 1) + IMAGE_TOKENS, low))
    after = jnp.where(
        index == IMAGES_PER_ROW - 1, low + span, jnp.minimum(first(index + 1), low + span)
    )
    spot = lax.broadcasted_iota(jnp.int32, (1, span + 2 * HALO), 1)
    place = low + jnp.where(
        spot < span, spot, jnp.where(spot < span + HALO, spot - span - HALO, spot - HALO)
    )
    slot = jnp.where((place >= start) & (place < end), place - start, -1)
    own = low + lax.broadcasted_iota(jnp.int32, (1, span), 1)
    lead = jnp.maximum(start - before, 0)
    pad = jnp.where((own >= end) & (own < after), lead + own - end, -1)
    pad = jnp.where((own >= before) & (own < start), own - before, pad)
    return slot, pad


def needed(tokens):
    return (tokens + 15) // 16 * 16


def sized(count, act):
    for size in range(16, HALO + 1, 16):
        pl.when(count == size)(functools.partial(act, size))


def row_kernel(
    ids, tok, cot, tok_all, cot_all, prompts, g1, b1, w_qkv_hbm, b_qv, w_out_hbm, b_out, g2, b2, w_up_hbm, b_up,
    w_down_hbm, b_down,
    out, tgr, pgr,
    w_qkv, w_out, w_up, w_down, w_sem,
    prom, pick, pad_pick, pad_wide, pad_hid, ins, n1, inv1, wide, qkv, probs, turned, hid, n2, inv2, act, upg, og, grad,
    halos, halo_send, halo_recv, sides, backs, side_send, side_recv,
    part, part_low, part_in, part_floor, summed, part_send, part_recv,
):
    index = lax.axis_index("seq")
    group = lax.axis_index("batch")
    row = pl.program_id(0)
    rows = tok_all.shape[0]
    span, width = tok.shape[1], tok.shape[2]
    ff = w_up.shape[1]
    bf = jnp.bfloat16
    last = IMAGES_PER_ROW - 1
    slack = span - IMAGE_TOKENS
    has_left, has_right = index > 0, index < last
    from_left = jnp.where(has_left, needed(slack * index), 0)
    from_right = jnp.where(has_right, needed(slack * (last - index)), 0)
    to_right = jnp.where(has_right, needed(slack * (index + 1)), 0)
    to_left = jnp.where(has_left, needed(slack * (IMAGES_PER_ROW - index)), 0)

    def weight(k):
        source = (w_qkv_hbm, w_out_hbm, w_up_hbm, w_down_hbm)[k]
        return pltpu.make_async_copy(source, (w_qkv, w_out, w_up, w_down)[k], w_sem.at[k])

    def seq_copy(source, target, send, recv, to):
        return pltpu.make_async_remote_copy(
            source, target, send, recv, device_id={"seq": to}, device_id_type=MESH
        )

    def halo_right(kind, r, size):
        source = (tok_all, cot_all)[kind].at[r, span - size :]
        target = halos.at[kind, r, HALO - size : HALO]
        return seq_copy(source, target, halo_send.at[kind, r, 0], halo_recv.at[kind, r, 0], index + 1)

    def halo_left(kind, r, size):
        source = (tok_all, cot_all)[kind].at[r, :size]
        target = halos.at[kind, r, HALO : HALO + size]
        return seq_copy(source, target, halo_send.at[kind, r, 1], halo_recv.at[kind, r, 1], index - 1)

    def halo_start(kind, r):
        sized(to_right, lambda size: halo_right(kind, r, size).start())
        sized(to_left, lambda size: halo_left(kind, r, size).start())

    def halo_wait(kind, r):
        sized(from_left, lambda size: halo_right(kind, r, size).wait_recv())
        sized(from_right, lambda size: halo_left(kind, r, size).wait_recv())

    def side_left(kind, r, size):
        source = sides.at[kind, r, HALO - size : HALO]
        target = backs.at[kind, r, 2 * HALO - size :]
        return seq_copy(source, target, side_send.at[kind, r, 0], side_recv.at[kind, r, 0], index - 1)

    def side_right(kind, r, size):
        source = sides.at[kind, r, HALO : HALO + size]
        target = backs.at[kind, r, :size]
        return seq_copy(source, target, side_send.at[kind, r, 1], side_recv.at[kind, r, 1], index + 1)

    def side_start(kind, r):
        sized(from_left, lambda size: side_left(kind, r, size).start())
        sized(from_right, lambda size: side_right(kind, r, size).start())

    def side_merge(kind, r):
        sized(to_right, lambda size: side_left(kind, r, size).wait_recv())
        sized(to_left, lambda size: side_right(kind, r, size).wait_recv())
        result = (out, tgr)[kind]
        result[r, :HALO] = result[r, :HALO] + backs[kind, r, :HALO]
        result[r, span - HALO :] = result[r, span - HALO :] + backs[kind, r, HALO:]

    down, deep = index // 2, index % 2
    piece = group * 2 + deep
    mates = []
    for k in range(1, 8):
        other = lax.rem(piece + k, 8)
        mates.append((other, {"batch": other // 2, "seq": down * 2 + lax.rem(other, 2)}))
    floors = [{"batch": group, "seq": lax.rem(down + k, 4) * 2 + deep} for k in range(1, 4)]

    def eight(place):
        return pl.ds(pl.multiple_of(place * 8, 8), 8)

    def part_copy(k, source, target, device):
        return pltpu.make_async_remote_copy(
            source, target, part_send.at[k], part_recv.at[k], device_id=device, device_id_type=MESH
        )

    pieces = PROMPTS // 8 + 1
    spread = [
        (other, part_copy(k, part_low.at[other], part_in.at[piece], device))
        for k, (other, device) in enumerate(mates)
    ]
    climb = [
        part_copy(7 + k, part_floor.at[down], part_floor.at[down], device)
        for k, device in enumerate(floors)
    ]
    hand = [
        part_copy(10 + k, summed.at[piece], summed.at[piece], device)
        for k, (_, device) in enumerate(mates)
    ]
    partners = [device for _, device in mates] + floors
    senders = [lax.rem(piece + 8 - k, 8) for k in range(1, 8)]

    @pl.when(row == 0)
    def _():
        for k in range(2):
            weight(k).start()
        halos[...] = jnp.zeros_like(halos)
        backs[...] = jnp.zeros_like(backs)
        barrier = pltpu.get_barrier_semaphore()
        for device in partners:
            pl.semaphore_signal(barrier, inc=1, device_id=device, device_id_type=MESH)
        @pl.when(has_left)
        def _():
            pl.semaphore_signal(barrier, inc=1, device_id={"seq": index - 1}, device_id_type=MESH)
        @pl.when(has_right)
        def _():
            pl.semaphore_signal(barrier, inc=1, device_id={"seq": index + 1}, device_id_type=MESH)
        prom[...] = jnp.zeros_like(prom)
        prom[1 : PROMPTS + 1] = prompts[...]
        part[...] = jnp.zeros_like(part)
        pl.semaphore_wait(barrier, len(partners) + jnp.where(has_left, 1, 0) + jnp.where(has_right, 1, 0))
        halo_start(0, 0)
        halo_start(1, 0)
        many = rows * PADS
        for r in range(rows):
            pads = lax.broadcasted_iota(jnp.int32, (PADS, span), 0)
            pad_pick[r] = jnp.where(pads == slot_map(ids[r : r + 1], index, span)[1], 1.0, 0.0).astype(bf)
            ins[r * PADS : (r + 1) * PADS] = dot(pad_pick[r], tok[r])
        for r in range(0, many, 64):
            c, _ = normalize(ins[r : r + 64])
            wide[r : r + 64] = (c * g1[...][None] + b1[...][None]).astype(bf)
        weight(0).wait()
        for c in range(0, width, 256):
            v = dot(wide[...], w_qkv[:, 2 * width + c : 2 * width + c + 256])
            act[:, c : c + 256] = (v + b_qv[width + c : width + c + 256][None]).astype(bf)
        weight(1).wait()
        for k in range(2, 4):
            weight(k).start()
        for c in range(0, width, 256):
            h = ins[:, c : c + 256] + dot(act[:, :width], w_out[:, c : c + 256])
            pad_hid[:, c : c + 256] = h + b_out[c : c + 256][None]
        for r in range(0, many, 64):
            c, _ = normalize(pad_hid[r : r + 64])
            pad_wide[r : r + 64] = (c * g2[...][None] + b2[...][None]).astype(bf)
        for k in range(2, 4):
            weight(k).wait()

    halo_wait(0, row)
    pl.when(row > 0)(lambda: halo_wait(1, row))

    @pl.when(row < rows - 1)
    def _():
        halo_start(0, row + 1)
        halo_start(1, row + 1)

    @pl.when(row > 0)
    def _():
        side_start(0, row - 1)
        side_start(1, row - 1)

    @pl.when(row > 1)
    def _():
        side_merge(0, row - 2)
        side_merge(1, row - 2)

    slot, _ = slot_map(ids[pl.ds(row, 1)], index, span)
    slots = lax.broadcasted_iota(jnp.int32, (KEYS, span + 2 * HALO), 0)
    pick[...] = jnp.where(slots == slot, 1.0, 0.0).astype(bf)

    first_rows = lax.broadcasted_iota(jnp.int32, (64, 1), 0)
    is_prompt = (first_rows >= 1) & (first_rows <= PROMPTS)
    for r in range(0, KEYS, 64):
        x = dot(pick[r : r + 64, :span], tok[row]) + dot(pick[r : r + 64, span:], halos[0, row])
        if r == 0:
            x = jnp.where(is_prompt, prom[...], x)
        ins[r : r + 64] = x
        c, inv = normalize(x)
        n1[r : r + 64] = c
        inv1[r : r + 64] = inv
        wide[r : r + 64] = (c * g1[...][None] + b1[...][None]).astype(bf)

    for c in range(0, width, 256):
        q = dot(wide[:KEYS], w_qkv[:, c : c + 256]) + b_qv[c : c + 256][None]
        qkv[:KEYS, c : c + 256] = (q * SCALE).astype(bf)
        k = dot(wide[:KEYS], w_qkv[:, width + c : width + c + 256])
        qkv[:KEYS, width + c : width + c + 256] = k.astype(bf)
        v = dot(wide[:KEYS], w_qkv[:, 2 * width + c : 2 * width + c + 256]) + b_qv[width + c : width + c + 256][None]
        qkv[:, 2 * width + c : 2 * width + c + 256] = v.astype(bf)

    lane = lax.broadcasted_iota(jnp.int32, (1, PAIR), 1)
    low_half = jnp.where(lane < HEAD_FEATURES, 1.0, 0.0).astype(bf)
    high_half = jnp.where(lane < HEAD_FEATURES, 0.0, 1.0).astype(bf)

    def both(x):
        return jnp.concatenate([x * low_half, x * high_half], axis=0)

    def own_halves(x):
        return x[:HEAD_FEATURES, :KEYS], x[HEAD_FEATURES:, KEYS:]

    tail_rows = lax.broadcasted_iota(jnp.int32, (16, 1), 0) + (KEYS - 16)
    for p in range(width // PAIR):
        at = p * PAIR
        qp = qkv[:KEYS, at : at + PAIR]
        kp = qkv[:KEYS, width + at : width + at + PAIR]
        vp = qkv[:KEYS, 2 * width + at : 2 * width + at + PAIR]
        st = dot_nt(kp, both(qp))
        upper, lower = st[: KEYS - 16], st[KEYS - 16 :]
        lower = jnp.where(tail_rows < IMAGE_TOKENS, lower, -1e30)
        top = jnp.maximum(jnp.max(upper, axis=0, keepdims=True), jnp.max(lower, axis=0, keepdims=True))
        upper = jnp.exp(upper - top)
        lower = jnp.exp(lower - top)
        total = jnp.sum(upper, axis=0, keepdims=True) + jnp.sum(lower, axis=0, keepdims=True)
        share = 1.0 / total
        probs[p, : KEYS - 16] = (upper * share).astype(bf)
        probs[p, KEYS - 16 :] = (lower * share).astype(bf)
        head0, head1 = own_halves(dot_tn(vp, probs[p]))
        turned[at : at + HEAD_FEATURES] = head0.astype(bf)
        turned[at + HEAD_FEATURES : at + PAIR] = head1.astype(bf)

    wide[:KEYS] = turned[...].T
    for c in range(0, width, 256):
        hid[:KEYS, c : c + 256] = ins[:KEYS, c : c + 256] + dot(wide[:KEYS], w_out[:, c : c + 256]) + b_out[c : c + 256][None]

    for r in range(0, KEYS, 64):
        c, inv = normalize(hid[r : r + 64])
        n2[r : r + 64] = c
        inv2[r : r + 64] = inv
        wide[r : r + 64] = (c * g2[...][None] + b2[...][None]).astype(bf)
    pl.when(row == 0)(lambda: halo_wait(1, row))
    for r in range(0, KEYS, 64):
        x = dot(pick[r : r + 64, :span], cot[0]) + dot(pick[r : r + 64, span:], halos[1, row])
        og[r : r + 64] = x.astype(bf)

    for c in range(0, ff, 256):
        upper = dot(wide[:KEYS], w_up[:, c : c + 256]) + b_up[c : c + 256][None]
        act_grad = dot_nt(og[...], w_down[c : c + 256, :])
        value, slope = gelu_parts(upper)
        act[:KEYS, c : c + 256] = value.astype(bf)
        upg[:, c : c + 256] = (act_grad * slope).astype(bf)
    for c in range(0, width, 256):
        y = hid[:KEYS, c : c + 256] + dot(act[:KEYS], w_down[:, c : c + 256]) + b_down[c : c + 256][None]
        wide[:KEYS, c : c + 256] = y.astype(bf)
        grad[:, c : c + 256] = dot_nt(upg[...], w_up[c : c + 256, :])
    out[row] = dot_tn(pick[:, :span], wide[:KEYS]).astype(bf)
    sides[0, row] = dot_tn(pick[:, span:], wide[:KEYS]).astype(bf)

    for r in range(0, KEYS, 64):
        e = grad[r : r + 64] * g2[...][None]
        n = n2[r : r + 64]
        mean = jnp.mean(e, axis=-1, keepdims=True)
        lean = jnp.mean(e * n, axis=-1, keepdims=True)
        h = og[r : r + 64].astype(jnp.float32) + inv2[r : r + 64] * (e - mean - n * lean)
        hid[r : r + 64] = h
        wide[r : r + 64] = h.astype(bf)
    for c in range(0, width, 256):
        og[:, c : c + 256] = dot_nt(wide[:KEYS], w_out[c : c + 256, :]).astype(bf)

    for p in range(width // PAIR):
        at = p * PAIR
        qp = qkv[:KEYS, at : at + PAIR]
        kp = qkv[:KEYS, width + at : width + at + PAIR]
        vp = qkv[:KEYS, 2 * width + at : 2 * width + at + PAIR]
        two_grads = both(og[:, at : at + PAIR])
        dp = dot_nt(vp, two_grads)
        pt = probs[p]
        pf = pt.astype(jnp.float32)
        inner = jnp.sum(pf * dp, axis=0, keepdims=True)
        ds = (pf * (dp - inner)).astype(bf)
        qkv[:KEYS, 2 * width + at : 2 * width + at + PAIR] = dot(pt, two_grads).astype(bf)
        head0, head1 = own_halves(dot_tn(kp, ds))
        qkv[:KEYS, width + at : width + at + PAIR] = dot(ds, both(qp)).astype(bf)
        turned[at : at + HEAD_FEATURES] = (head0 * SCALE).astype(bf)
        turned[at + HEAD_FEATURES : at + PAIR] = (head1 * SCALE).astype(bf)
    qkv[:KEYS, :width] = turned[...].T

    for c in range(0, width, 256):
        grad[:, c : c + 256] = dot_nt(qkv[:KEYS], w_qkv[c : c + 256, :])
    for r in range(0, KEYS, 64):
        e = grad[r : r + 64] * g1[...][None]
        n = n1[r : r + 64]
        mean = jnp.mean(e, axis=-1, keepdims=True)
        lean = jnp.mean(e * n, axis=-1, keepdims=True)
        x = hid[r : r + 64] + inv1[r : r + 64] * (e - mean - n * lean)
        if r == 0:
            part[...] += x
            x = jnp.where(is_prompt, 0.0, x)
        wide[r : r + 64] = x.astype(bf)
    @pl.when(row == rows - 1)
    def _():
        for k in range(8):
            part_low[k] = part[8 * k : 8 * k + 8].astype(bf)
        for other, copy in spread:
            pl.when(other < pieces)(copy.start)

    tgr[row] = dot_tn(pick[:, :span], wide[:KEYS]).astype(bf)
    sides[1, row] = dot_tn(pick[:, span:], wide[:KEYS]).astype(bf)

    @pl.when(row == rows - 1)
    def _():
        side_start(0, row)
        side_start(1, row)

        def pad_up(first, last):
            for c in range(first * 256, last * 256, 256):
                upper = dot(pad_wide[...], w_up[:, c : c + 256]) + b_up[c : c + 256][None]
                act[:, c : c + 256] = gelu_parts(upper)[0].astype(bf)

        chunks = ff // 256
        pad_up(0, chunks * CUTS[0] // 12)
        @pl.when(piece < pieces)
        def _():
            for _, copy in spread:
                copy.wait_recv()
            part_in[piece] = jnp.zeros_like(part_in[piece])
            mine = part[eight(piece)]
            for k in range(8):
                mine = mine + part_in[k].astype(jnp.float32)
            part_floor[down] = mine.astype(bf)
            for copy in climb:
                copy.start()

        pad_up(chunks * CUTS[0] // 12, chunks * CUTS[1] // 12)
        @pl.when(piece < pieces)
        def _():
            for copy in climb:
                copy.wait_recv()
            level = [part_floor[k].astype(jnp.float32) for k in range(4)]
            summed[piece] = ((level[0] + level[1]) + (level[2] + level[3])).astype(bf)
            for copy in hand:
                copy.start()

        pad_up(chunks * CUTS[1] // 12, chunks)
        for c in range(0, width, 256):
            y = pad_hid[:, c : c + 256] + dot(act[...], w_down[:, c : c + 256]) + b_down[c : c + 256][None]
            wide[:, c : c + 256] = y.astype(bf)
        for r in range(rows):
            out[r] = out[r] + dot_tn(pad_pick[r], wide[r * PADS : (r + 1) * PADS]).astype(bf)

        for r in (rows - 2, rows - 1):
            side_merge(0, r)
            side_merge(1, r)
        for back, copy in zip(senders, hand):
            pl.when(back < pieces)(copy.wait_recv)
        for k in range(pieces):
            part[8 * k : 8 * k + 8] = summed[k].astype(jnp.float32)
        pgr[...] = part[1 : PROMPTS + 1]
        for other, copy in spread:
            pl.when(other < pieces)(copy.wait_send)

        @pl.when(piece < pieces)
        def _():
            for copy in climb + hand:
                copy.wait_send()

        for r in range(rows):
            for kind in range(2):
                sized(to_right, lambda size: halo_right(kind, r, size).wait_send())
                sized(to_left, lambda size: halo_left(kind, r, size).wait_send())
                sized(from_left, lambda size: side_left(kind, r, size).wait_send())
                sized(from_right, lambda size: side_right(kind, r, size).wait_send())


def image_body(
    tokens, prompts, image_id, prompt_slot, ln1_gain, ln1_bias, w_qkv, bias_qv, w_out, bias_out,
    ln2_gain, ln2_bias, w_up, bias_up, w_down, bias_down, cotangent,
):
    rows, span, width = tokens.shape
    ff = w_up.shape[1]
    f32, bf = jnp.float32, jnp.bfloat16
    dma = pltpu.SemaphoreType.DMA

    per_row = pl.BlockSpec((1, span, width), lambda r: (r, 0, 0))
    in_place = pl.BlockSpec(memory_space=pl.ANY)

    def whole(array):
        return pl.BlockSpec(array.shape, lambda r: (0,) * len(array.shape), pipeline_mode=pl.Buffered(1))

    return pl.pallas_call(
        row_kernel,
        grid=(rows,),
        in_specs=[
            whole(image_id), whole(tokens), per_row, in_place, in_place, whole(prompts), whole(ln1_gain), whole(ln1_bias),
            in_place, whole(bias_qv), in_place, whole(bias_out), whole(ln2_gain), whole(ln2_bias), in_place,
            whole(bias_up), in_place, whole(bias_down),
        ],
        out_specs=[pl.BlockSpec(memory_space=pltpu.VMEM)] * 3,
        out_shape=[
            pltpu.VMEM((rows, span, width), bf), pltpu.VMEM((rows, span, width), bf), pltpu.VMEM((PROMPTS, width), f32),
        ],
        scratch_shapes=[
            pltpu.VMEM(w_qkv.shape, bf), pltpu.VMEM(w_out.shape, bf), pltpu.VMEM(w_up.shape, bf),
            pltpu.VMEM(w_down.shape, bf), dma((4,)),
            pltpu.VMEM((64, width), f32), pltpu.VMEM((KEYS, span + 2 * HALO), bf), pltpu.VMEM((rows, PADS, span), bf),
            pltpu.VMEM((rows * PADS, width), bf), pltpu.VMEM((rows * PADS, width), f32), pltpu.VMEM((rows * PADS, width), f32), pltpu.VMEM((KEYS, width), f32),
            pltpu.VMEM((KEYS, 1), f32), pltpu.VMEM((rows * PADS, width), bf), pltpu.VMEM((KEYS, 3 * width), bf),
            pltpu.VMEM((width // PAIR, KEYS, 2 * KEYS), bf), pltpu.VMEM((width, KEYS), bf),
            pltpu.VMEM((rows * PADS, width), f32), pltpu.VMEM((KEYS, width), f32), pltpu.VMEM((KEYS, 1), f32),
            pltpu.VMEM((rows * PADS, ff), bf), pltpu.VMEM((KEYS, ff), bf),
            pltpu.VMEM((KEYS, width), bf), pltpu.VMEM((KEYS, width), f32),
            pltpu.VMEM((2, rows, 2 * HALO, width), bf), dma((2, rows, 2)), dma((2, rows, 2)),
            pltpu.VMEM((2, rows, 2 * HALO, width), bf), pltpu.VMEM((2, rows, 2 * HALO, width), bf),
            dma((2, rows, 2)), dma((2, rows, 2)),
            pltpu.VMEM((64, width), f32), pltpu.VMEM((8, 8, width), bf), pltpu.VMEM((8, 8, width), bf),
            pltpu.VMEM((4, 8, width), bf), pltpu.VMEM((8, 8, width), bf), dma((17,)), dma((17,)),
        ],
        compiler_params=pltpu.CompilerParams(
            vmem_limit_bytes=56 << 20, dimension_semantics=("arbitrary",), collective_id=0, has_side_effects=True
        ),
        name="layer_rows",
    )(
        image_id, tokens, cotangent, tokens, cotangent, prompts, ln1_gain, ln1_bias, w_qkv, bias_qv, w_out, bias_out,
        ln2_gain, ln2_bias, w_up, bias_up, w_down, bias_down,
    )


def body(tokens, prompts, image_id, *rest):
    if lax.axis_size("seq") == IMAGES_PER_ROW and lax.axis_size("batch") == 4 and tokens.shape[1] == KEYS:
        return image_body(tokens, prompts, image_id, *rest)
    return general_body(tokens, prompts, image_id, *rest)


def solution(mesh):
    in_specs = (
        P("batch", "seq", None),
        P(),
        P("batch", None),
        P("batch", "seq"),
        P(),
        P(),
        P(),
        P(),
        P(),
        P(),
        P(),
        P(),
        P(),
        P(),
        P(),
        P(),
        P("batch", "seq", None),
    )
    out_specs = (P("batch", "seq", None), P("batch", "seq", None), P())
    return jax.shard_map(body, mesh=mesh, in_specs=in_specs, out_specs=out_specs, check_vma=False)
```
